32 devices in a mesh: fsdp: 4 (over z), context: 2 (over x), tensor: 4 (over y, core).
Axes of the slice: x: 2, y: 2, z: 4, core: 2. Of those that a mesh axis runs over, the one named last changes fastest.
Arguments:
- tokens: bfloat16 [8, 1024, 768], P('fsdp', 'context'), may hold values from -6 to 6
- cotangent: bfloat16 [8, 1024, 768], P('fsdp', 'context'), may hold values from -6 to 6
- segment_ids: int32 [8, 1024], P('fsdp', 'context'), may hold values from 0 to 15, never falling along the last dimension, each value on 1 to 512 neighbouring positions
- owner: int32 [4], replicated, may hold values from 0 to 1, as said below
- qkv_weight: float32 [768, 3, 768], P('fsdp', None, 'tensor'), may hold values from -0.21875 to 0.21875
- out_weight: float32 [768, 768], P('tensor', 'fsdp'), may hold values from -1.25 to 1.25
- gate_up_weight: float32 [768, 2, 3072], P('fsdp', None, 'tensor'), may hold values from -0.21875 to 0.21875
- down_weight: float32 [3072, 768], P('tensor', 'fsdp'), may hold values from -0.109375 to 0.109375
- norm_gains: float32 [2, 768], replicated, may hold values from 0.5 to 1.5
- norm_biases: float32 [2, 768], replicated, may hold values from -2 to 2
- qkv_moment: float32 [2, 768, 3, 768], P('context', 'fsdp', None, 'tensor'), may hold values from -32 to 32
- qkv_square: float32 [2, 768, 3, 768], P('context', 'fsdp', None, 'tensor'), may hold values from 1 to 10
- out_moment: float32 [2, 768, 768], P('context', 'tensor', 'fsdp'), may hold values from -32 to 32
- out_square: float32 [2, 768, 768], P('context', 'tensor', 'fsdp'), may hold values from 1 to 10
- gate_moment: float32 [2, 768, 2, 3072], P('context', 'fsdp', None, 'tensor'), may hold values from -32 to 32
- gate_square: float32 [2, 768, 2, 3072], P('context', 'fsdp', None, 'tensor'), may hold values from 1 to 10
- down_moment: float32 [2, 3072, 768], P('context', 'tensor', 'fsdp'), may hold values from -32 to 32
- down_square: float32 [2, 3072, 768], P('context', 'tensor', 'fsdp'), may hold values from 1 to 10
- norm_moment: float32 [4, 768], replicated, may hold values from -32 to 32
- norm_square: float32 [4, 768], replicated, may hold values from 1 to 10
Outputs:
- layer_out: bfloat16 [8, 1024, 768], P('fsdp', ('context', 'tensor'))
- input_grad: float32 [8, 1024, 768], P('fsdp', ('context', 'tensor'))
- qkv_grad: float32 [768, 3, 768], P('fsdp', None, 'tensor')
- out_grad: float32 [768, 768], P('tensor', 'fsdp')
- gate_up_grad: float32 [768, 2, 3072], P('fsdp', None, 'tensor')
- down_grad: float32 [3072, 768], P('tensor', 'fsdp')
- norm_grad: float32 [4, 768], replicated
- qkv_state: float32 [2, 768, 3, 768], P(None, 'fsdp', None, 'tensor')
- out_state: float32 [2, 768, 768], P(None, 'tensor', 'fsdp')
- gate_up_state: float32 [2, 768, 2, 3072], P(None, 'fsdp', None, 'tensor')
- down_state: float32 [2, 3072, 768], P(None, 'tensor', 'fsdp')
- norm_state: float32 [2, 4, 768], replicated
- weight_updates: float32 [4, 4, 590016], P('fsdp', 'tensor')
The draws below stay inside these ranges and needn't reach their ends.
Inputs may be any that keep to these rules, and one draw needn't show every extreme that they name: `segment_ids`: within each sequence the ids never fall; each of 0 to 15 names one document of 1 to 512 tokens, and one document has exactly 512. Some matrix has owner 0 and some other has owner 2 - 1.
All inputs are finite; a program needn't handle non-finite values.
Results may differ from the reference program's by a relative error of at most 0.03.
Values may be sent and summed in bfloat16 or wider, within the bound.
A program may use at most 192 MiB of HBM per device.

```python
import math
import jax
import jax.numpy as jnp
import numpy as np
from jax import lax

D = 768
HEADS = 12
HD = 64
FF = 3072
DOCS = 16
LEN = 1024
SEQS = 8
MOST_DOC = 512
N_FSDP = 4
N_CONTEXT = 2
N_TENSOR = 4


def draw_owner(key, part):
    first_key, second_key, third_key = jax.random.split(key, 3)
    owners_drawn = jax.random.randint(first_key, (4,), 0, N_CONTEXT)
    high_place = jax.random.randint(second_key, (), 0, 4)
    low_place = (high_place + 1 + jax.random.randint(third_key, (), 0, 3)) % 4
    places_all = jnp.arange(4)
    owners_drawn = jnp.where(places_all == high_place, N_CONTEXT - 1, owners_drawn)
    owners_drawn = jnp.where(places_all == low_place, 0, owners_drawn)
    return owners_drawn.astype(jnp.int32)


def block_scale(stream_key, dims, cuts, smallest, largest):
    level = 1.0
    for position, blocks in cuts:
        draws = jax.random.uniform(jax.random.fold_in(jax.random.fold_in(stream_key, 6), position), (blocks,), jnp.float32, smallest / len(cuts), largest / len(cuts))
        level = level * jnp.repeat(jnp.exp(draws), dims[position] // blocks).reshape((-1,) + (1,) * (len(dims) - 1 - position))
    return level


def length_profile(amount, total, most, lean):
    portions = [(1 << 20) // math.isqrt(rank ** lean) + 1 for rank in range(2, amount + 1)]
    surplus, given = total - most - (amount - 1), [1] * (amount - 1)
    while surplus > 0:
        free = [i for i in range(amount - 1) if given[i] < most]
        pool, budget = sum([portions[i] for i in free]), surplus
        for i in free:
            more = min(most - given[i], max(1, budget * portions[i] // pool), surplus)
            given[i] = given[i] + more
            surplus = surplus - more
    return np.array([most] + given)


def uneven_parts(stream_key, count, total, limit, skew):
    if count == 2:
        one = jax.random.randint(stream_key, (), max(1, total - limit), min(limit, total - 1) + 1)
        return jnp.stack([one, total - one])
    lengths = jnp.asarray(length_profile(count, total, limit, skew), jnp.int32)
    couples = (count - 1) // 2
    donor, taker = lengths[1:1 + 2 * couples:2], lengths[2:2 + 2 * couples:2]
    margin = jnp.minimum(donor - 1, limit - taker)
    shifted = jax.random.randint(jax.random.fold_in(stream_key, 1), (couples,), 0, 1 << 20) % (margin + 1)
    lengths = lengths.at[1:1 + 2 * couples:2].set(donor - shifted).at[2:2 + 2 * couples:2].set(taker + shifted)
    return lengths[jax.random.permutation(jax.random.fold_in(stream_key, 2), count)]


def normal_values(stream_key, extent, scale, reach, shards=(), kind=jnp.bfloat16):
    result = scale * jax.random.normal(stream_key, extent, jnp.float32)
    if shards:
        result = result * block_scale(stream_key, extent, shards, -0.22, 0.18)
    return jnp.clip(result, -reach, reach).astype(kind)


def setup_inputs(seed: int = 0) -> dict:
    keys = jax.random.split(jax.random.key(seed), 21)
    return {
        "tokens": normal_values(keys[0], (SEQS, LEN, D), 1.0, 6.0, ((0, 4), (1, 2))),
        "cotangent": normal_values(keys[1], (SEQS, LEN, D), 1.0, 6.0, ((0, 4), (1, 2))),
        "segment_ids": jax.vmap(lambda own: jnp.searchsorted(jnp.cumsum(uneven_parts(own, DOCS, LEN, MOST_DOC, 2)), jnp.arange(LEN), side="right"))(jax.random.split(keys[2], SEQS)).reshape((SEQS, LEN)).astype(jnp.int32),
        "owner": draw_owner(jax.random.fold_in(keys[20], 71), 0),
        "qkv_weight": normal_values(keys[4], (D, 3, D), D ** -0.5, 0.21875, ((0, 4), (2, 4)), jnp.float32),
        "out_weight": normal_values(keys[5], (D, D), (D // 32) ** -0.5, 1.25, ((0, 4), (1, 4)), jnp.float32),
        "gate_up_weight": normal_values(keys[6], (D, 2, FF), D ** -0.5, 0.21875, ((0, 4), (2, 4)), jnp.float32),
        "down_weight": normal_values(keys[7], (FF, D), FF ** -0.5, 0.109375, ((0, 4), (1, 4)), jnp.float32),
        "norm_gains": jnp.clip(1.0 + 0.1 * jax.random.normal(keys[8], (2, D), jnp.float32), 0.5, 1.5),
        "norm_biases": normal_values(keys[9], (2, D), 0.3, 2.0, (), jnp.float32),
        "qkv_moment": normal_values(keys[10], (N_CONTEXT, D, 3, D), ((SEQS * LEN) ** 0.5 // 16), 32.0, ((0, 2), (1, 4), (3, 4)), jnp.float32),
        "qkv_square": jnp.clip(jnp.exp(math.log(10.0) - 2.3025851 * jax.random.uniform(keys[11], (N_CONTEXT, D, 3, D), jnp.float32) ** block_scale(keys[11], (N_CONTEXT, D, 3, D), ((0, 2), (1, 4), (3, 4)), -0.2, 0.2)), 1.0, 10.0),
        "out_moment": normal_values(keys[12], (N_CONTEXT, D, D), ((SEQS * LEN) ** 0.5 // 16), 32.0, ((0, 2), (1, 4), (2, 4)), jnp.float32),
        "out_square": jnp.clip(jnp.exp(math.log(10.0) - 2.3025851 * jax.random.uniform(keys[13], (N_CONTEXT, D, D), jnp.float32) ** block_scale(keys[13], (N_CONTEXT, D, D), ((0, 2), (1, 4), (2, 4)), -0.2, 0.2)), 1.0, 10.0),
        "gate_moment": normal_values(keys[14], (N_CONTEXT, D, 2, FF), ((SEQS * LEN) ** 0.5 // 16), 32.0, ((0, 2), (1, 4), (3, 4)), jnp.float32),
        "gate_square": jnp.clip(jnp.exp(math.log(10.0) - 2.3025851 * jax.random.uniform(keys[15], (N_CONTEXT, D, 2, FF), jnp.float32) ** block_scale(keys[15], (N_CONTEXT, D, 2, FF), ((0, 2), (1, 4), (3, 4)), -0.2, 0.2)), 1.0, 10.0),
        "down_moment": normal_values(keys[16], (N_CONTEXT, FF, D), ((SEQS * LEN) ** 0.5 // 16), 32.0, ((0, 2), (1, 4), (2, 4)), jnp.float32),
        "down_square": jnp.clip(jnp.exp(math.log(10.0) - 2.3025851 * jax.random.uniform(keys[17], (N_CONTEXT, FF, D), jnp.float32) ** block_scale(keys[17], (N_CONTEXT, FF, D), ((0, 2), (1, 4), (2, 4)), -0.2, 0.2)), 1.0, 10.0),
        "norm_moment": normal_values(keys[18], (4, D), ((SEQS * LEN) ** 0.5 // 16), 32.0, (), jnp.float32),
        "norm_square": jnp.clip(jnp.exp(jax.random.uniform(keys[19], (4, D), jnp.float32, math.log(1.0), math.log(10.0))), 1.0, 10.0),
    }


NEGATIVE = -1e+30
EPSILON = 1e-05
ROPE_BASE = 1000.0
BETA_ONE = 0.9
BETA_TWO = 0.999
ADAM_EPS = 1e-08
ADAM_STEP = 3.0
RATE = 0.03
DECAY = 0.1
HIGHEST = lax.Precision.HIGHEST

@jax.custom_vjp
def low(v):
    return lax.optimization_barrier(v.astype(jnp.bfloat16)).astype(jnp.float32)

@jax.custom_vjp
def low_back(v):
    return v

def low_keep(v):
    return (low(v), None)

def low_pass(kept, grad):
    return (grad,)

def back_keep(v):
    return (v, None)

def back_low(kept, grad):
    return (low(grad),)
low.defvjp(low_keep, low_pass)
low_back.defvjp(back_keep, back_low)

def rotary_tables(positions, head_size):
    frequency = jnp.power(jnp.float32(ROPE_BASE), -jnp.arange(0, head_size, 2, dtype=jnp.float32) / head_size)
    angles = positions[:, None] * frequency[None, :]
    return (jnp.cos(angles), jnp.sin(angles))

def rotate(vectors, cosine, sine_rows):
    half_size = vectors.shape[-1] // 2
    first_half = vectors[..., :half_size]
    second_half = vectors[..., half_size:]
    cosine = cosine[:, None, :]
    sine_rows = sine_rows[:, None, :]
    return jnp.concatenate([first_half * cosine - second_half * sine_rows, second_half * cosine + first_half * sine_rows], axis=-1)

def normalize(values, gain_row, bias_row):
    center = values - lax.optimization_barrier(jnp.mean(values, axis=-1, keepdims=True))
    variance = lax.optimization_barrier(jnp.mean(center * center, axis=-1, keepdims=True))
    return center * lax.rsqrt(variance + EPSILON) * gain_row + bias_row

def attend_block(queries, query_ids, key_rows, value_rows, key_ids):
    scores = jnp.einsum('qhd,khd->hqk', queries, key_rows, precision=HIGHEST) * HD ** (-0.5)
    scores = low_back(scores)
    scores = jnp.where(query_ids[None, :, None] == key_ids[None, None, :], scores, NEGATIVE)
    row_total = jax.nn.logsumexp(scores, axis=-1, keepdims=True)
    probability = low(jnp.exp(scores - row_total))
    return jnp.einsum('hqk,khd->qhd', probability, value_rows, precision=HIGHEST)

def forward_sequence(inputs, seq_ids, qkv_low, out_low, gate_low, down_low, norm_gains, norm_biases):
    query_block = min(512, LEN)
    projected = jnp.dot(inputs, qkv_low.reshape(D, 3 * D), precision=HIGHEST)
    projected = low_back(projected).reshape(LEN, 3, HEADS, HD)
    cosine, sine_rows = rotary_tables(jnp.arange(LEN, dtype=jnp.float32), HD)
    queries = low(rotate(projected[:, 0], cosine, sine_rows))
    key_rows = low(rotate(projected[:, 1], cosine, sine_rows))
    value_rows = low(projected[:, 2])
    checked = jax.checkpoint(attend_block)

    def one_block(packed):
        return checked(packed[0], packed[1], key_rows, value_rows, seq_ids)
    attended = lax.map(one_block, (queries.reshape(LEN // query_block, query_block, HEADS, HD), seq_ids.reshape(LEN // query_block, query_block)))
    attended = low(low_back(attended.reshape(LEN, D)))
    branch_attn = low_back(jnp.dot(attended, out_low, precision=HIGHEST))
    normed_first = normalize(inputs + branch_attn, norm_gains[0], norm_biases[0])
    gate_up = jnp.dot(low(normed_first), gate_low.reshape(D, 2 * FF), precision=HIGHEST)
    gate_up = low_back(gate_up).reshape(LEN, 2, FF)
    hidden = low(jax.nn.silu(gate_up[:, 0]) * gate_up[:, 1])
    branch_ffn = low_back(jnp.dot(hidden, down_low, precision=HIGHEST))
    return normalize(normed_first + branch_ffn, norm_gains[1], norm_biases[1])

def adam_update(gradient, master, moment, square, decay_rate):
    moment_new = BETA_ONE * moment + (1.0 - BETA_ONE) * gradient
    square_new = BETA_TWO * square + (1.0 - BETA_TWO) * gradient * gradient
    corrected = moment_new / (1.0 - BETA_ONE ** ADAM_STEP)
    scaled = square_new / (1.0 - BETA_TWO ** ADAM_STEP)
    update = -RATE * (corrected / (jnp.sqrt(scaled) + ADAM_EPS) + decay_rate * master)
    return (jnp.stack([moment_new, square_new]), update)

def owned_slot(stack, owner_index):
    return lax.dynamic_index_in_dim(stack, owner_index, 0, keepdims=False)

def flat_updates(qkv_update, out_update, gate_update, down_update, norm_update):
    qkv_blocks = jnp.transpose(qkv_update.reshape(N_FSDP, D // N_FSDP, 3, N_TENSOR, D // N_TENSOR), (0, 3, 1, 2, 4)).reshape(N_FSDP, N_TENSOR, -1)
    out_blocks = jnp.transpose(out_update.reshape(N_TENSOR, D // N_TENSOR, N_FSDP, D // N_FSDP), (2, 0, 1, 3)).reshape(N_FSDP, N_TENSOR, -1)
    gate_blocks = jnp.transpose(gate_update.reshape(N_FSDP, D // N_FSDP, 2, N_TENSOR, FF // N_TENSOR), (0, 3, 1, 2, 4)).reshape(N_FSDP, N_TENSOR, -1)
    down_blocks = jnp.transpose(down_update.reshape(N_TENSOR, FF // N_TENSOR, N_FSDP, D // N_FSDP), (2, 0, 1, 3)).reshape(N_FSDP, N_TENSOR, -1)
    norm_blocks = norm_update.reshape(N_FSDP, N_TENSOR, -1)
    return jnp.concatenate([qkv_blocks, out_blocks, gate_blocks, down_blocks, norm_blocks], axis=2)

def reference(tokens, cotangent, segment_ids, owner, qkv_weight, out_weight, gate_up_weight, down_weight, norm_gains, norm_biases, qkv_moment, qkv_square, out_moment, out_square, gate_moment, gate_square, down_moment, down_square, norm_moment, norm_square):

    def whole(inputs, qkv_matrix, out_matrix, gate_matrix, down_matrix, gains_all, biases_all):
        qkv_low = low(qkv_matrix)
        out_low = low(out_matrix)
        gate_low = low(gate_matrix)
        down_low = low(down_matrix)

        def one_sequence(packed):
            return forward_sequence(packed[0], packed[1], qkv_low, out_low, gate_low, down_low, gains_all, biases_all)
        return lax.map(one_sequence, (inputs, segment_ids))
    outputs, pullback = jax.vjp(whole, tokens.astype(jnp.float32), qkv_weight, out_weight, gate_up_weight, down_weight, norm_gains, norm_biases)
    grad_input, qkv_grad, out_grad, gate_grad, down_grad, gain_grad, bias_grad = pullback(cotangent.astype(jnp.float32))
    norm_grad = jnp.concatenate([gain_grad, bias_grad], axis=0)
    qkv_state, qkv_update = adam_update(qkv_grad, qkv_weight, owned_slot(qkv_moment, owner[0]), owned_slot(qkv_square, owner[0]), DECAY)
    out_state, out_update = adam_update(out_grad, out_weight, owned_slot(out_moment, owner[1]), owned_slot(out_square, owner[1]), DECAY)
    gate_state, gate_update = adam_update(gate_grad, gate_up_weight, owned_slot(gate_moment, owner[2]), owned_slot(gate_square, owner[2]), DECAY)
    down_state, down_update = adam_update(down_grad, down_weight, owned_slot(down_moment, owner[3]), owned_slot(down_square, owner[3]), DECAY)
    norm_state, norm_update = adam_update(norm_grad, jnp.concatenate([norm_gains, norm_biases], axis=0), norm_moment, norm_square, 0.0)
    weight_updates = flat_updates(qkv_update, out_update, gate_update, down_update, norm_update)
    return (outputs.astype(jnp.bfloat16), grad_input, qkv_grad, out_grad, gate_grad, down_grad, norm_grad, qkv_state, out_state, gate_state, down_state, norm_state, weight_updates)
```

```python
import functools

import jax
import jax.numpy as jnp
from jax import lax
from jax.experimental import pallas as pl
from jax.experimental.pallas import tpu as pltpu
from jax.sharding import PartitionSpec as P

HD = 64

NEGATIVE = -1e30
EPSILON = 1e-05
ROPE_BASE = 1000.0
BETA_ONE = 0.9
BETA_TWO = 0.999
ADAM_EPS = 1e-08
ADAM_STEP = 3.0
RATE = 0.03
DECAY = 0.1

F32 = jnp.float32
BF16 = jnp.bfloat16
MESH = pl.DeviceIdType.MESH
NN = (((1,), (0,)), ((), ()))
NT = (((1,), (1,)), ((), ()))
TN = (((0,), (0,)), ((), ()))


def mm(left, right, dims):
    return lax.dot_general(left, right, dims, preferred_element_type=F32)


def swap_halves(values):
    lane = lax.broadcasted_iota(jnp.int32, values.shape, 1)
    low_half = lane % HD < HD // 2
    return jnp.where(
        low_half,
        pltpu.roll(values, 128 - HD // 2, 1),
        pltpu.roll(values, HD // 2, 1),
    )


def mean_of(values):
    return jnp.sum(values, axis=-1, keepdims=True) * (1.0 / values.shape[-1])


def normalize(values, gain_row, bias_row):
    center = values - mean_of(values)
    inverse_std = lax.rsqrt(mean_of(center * center) + EPSILON)
    unit = center * inverse_std
    return unit * gain_row + bias_row, unit, inverse_std


def norm_back(gradient, unit, inverse_std, gain_row):
    scaled = gradient * gain_row
    return inverse_std * (scaled - mean_of(scaled) - unit * mean_of(scaled * unit))


class Pack:
    pass


def layer_kernel(dims, *refs):
    S, T, D, C, F, NF, NC, NT4 = dims
    TS = T // NT4
    DB = D // NF
    QW, KW = 256, 384
    H = C // HD
    KS = min(max(NC - 1, 1), 2)
    scale = HD ** (-0.5)
    (
        tok, cot, ids_in, wq_in, wo_in, wg_in, wd_in, gains, biases, cos_t, sin_t,
        layer_out, input_grad, gq_out, go_out, gg_out, gd_out, norm_out,
        wq, wo, wg, wd, ids_all, q_ref, kv, att, tot, am, al, acc, bias_ref, vt,
        rsend, rsb, rs2, rs2r, ag1, ag2, ag3, hid, gb,
        n1, unit1, inv1, datt, dlt, dqt, dk, dv, kvg_s, kvg_r, kv_own, qb,
        gsq, gso, gsg, gsd, grq, gro, grg, grd, xq, xo, xg, xd, nsum_t, nsum_c, nsum_f, cot_v,
        w_ss, w_rs, kv_ss, kv_rs, id_ss, id_rs, rs_ss, rs_rs, ag_ss, ag_rs,
        kvg_ss, kvg_rs, gr_ss, gr_rs, x_ss, x_rs, n_ss, n_rs, loc_sem,
    ) = refs

    z, x, t = lax.axis_index("fsdp"), lax.axis_index("context"), lax.axis_index("tensor")
    core, yy = t % 2, t // 2
    t_core = yy * 2 + (1 - core)
    t_y = (1 - yy) * 2 + core
    t_diag = (1 - yy) * 2 + (1 - core)

    def remote(src, dst, ssem, rsem, axis, index):
        return pltpu.make_async_remote_copy(
            src_ref=src, dst_ref=dst, send_sem=ssem, recv_sem=rsem,
            device_id={axis: index}, device_id_type=MESH,
        )

    barrier = pltpu.get_barrier_semaphore()
    for d in range(1, NF):
        pl.semaphore_signal(barrier, inc=1, device_id={"fsdp": (z + d) % NF}, device_id_type=MESH)
    for d in range(1, NC):
        pl.semaphore_signal(barrier, inc=1, device_id={"context": (x + d) % NC}, device_id_type=MESH)
    for d in range(1, NT4):
        pl.semaphore_signal(barrier, inc=1, device_id={"tensor": (t + d) % NT4}, device_id_type=MESH)

    cot_copy = pltpu.make_async_copy(
        cot.at[:, pl.ds(pl.multiple_of(t * TS, TS), TS), :], cot_v, loc_sem.at[0]
    )
    cot_copy.start()

    def own_rows(index):
        return pl.ds(pl.multiple_of(index * DB, DB), DB)

    def pad_cols(values, left, right):
        parts = []
        if left:
            parts.append(jnp.zeros((values.shape[0], left), values.dtype))
        parts.append(values)
        if right:
            parts.append(jnp.zeros((values.shape[0], right), values.dtype))
        return jnp.concatenate(parts, axis=1)

    wq[own_rows(z), :] = jnp.concatenate(
        [
            pad_cols(wq_in[:, 0, :], 0, QW - C),
            jnp.concatenate([wq_in[:, 1, :], wq_in[:, 2, :]], axis=1),
        ],
        axis=1,
    ).astype(BF16)

    pl.semaphore_wait(barrier, NF - 1 + NC - 1 + NT4 - 1)

    def gather(buffer, slot):
        copies = []
        for d in range(1, NF):
            copies.append(
                remote(
                    buffer.at[own_rows(z), :], buffer.at[own_rows(z), :],
                    w_ss.at[slot, d - 1], w_rs.at[slot, d - 1], "fsdp", (z + d) % NF,
                )
            )
        for c in copies:
            c.start()
        return copies

    def wait_recv(copies):
        for c in copies:
            c.wait_recv()

    def wait_send(copies):
        for c in copies:
            c.wait_send()

    wq_copies = gather(wq, 0)

    ids_all[x] = ids_in[...]
    id_copies = []
    for d in range(1, NC):
        c = remote(
            ids_all.at[x], ids_all.at[x], id_ss.at[d - 1], id_rs.at[d - 1],
            "context", (x + d) % NC,
        )
        c.start()
        id_copies.append(c)

    def eye(n):
        return (
            lax.broadcasted_iota(jnp.int32, (n, n), 0)
            == lax.broadcasted_iota(jnp.int32, (n, n), 1)
        ).astype(F32).astype(BF16)

    wo_t = jnp.transpose(wo_in[...])
    wo[own_rows(z), :] = pad_cols(wo_t, HD, 0).astype(BF16)
    wd[own_rows(z), :] = jnp.transpose(wd_in[...]).astype(BF16)
    wg[own_rows(z), 0:F] = wg_in[:, 0, :].astype(BF16)
    wg[own_rows(z), F : 2 * F] = wg_in[:, 1, :].astype(BF16)

    wait_recv(wq_copies)
    wo_copies = gather(wo, 1)

    def rotate_pair(values, rows, sign):
        cosine, sine_rows = cos_t[rows, :], sin_t[rows, :] * sign
        lane = lax.broadcasted_iota(jnp.int32, cosine.shape, 1)
        head = lane < HD
        first, second = values[:, 0:128], values[:, 128:256]
        first = first * cosine + swap_halves(first) * sine_rows
        second = second * jnp.where(head, cosine, 1.0) + swap_halves(second) * jnp.where(
            head, sine_rows, 0.0
        )
        return first, second

    TR = min(256, T)

    def project(s):
        def tile(i, carry):
            rows = pl.ds(pl.multiple_of(i * TR, TR), TR)
            p = mm(tok[s, rows, :], wq[...], NN)
            q0, q1 = rotate_pair(p[:, 0:QW], rows, 1.0)
            q_ref[s, rows, 0:128] = q0.astype(BF16)
            q_ref[s, rows, 128:256] = q1.astype(BF16)
            k0, k1 = rotate_pair(p[:, QW : QW + 256], rows, 1.0)
            kv[x, s, rows, 0:128] = k0.astype(BF16)
            kv[x, s, rows, 128:256] = k1.astype(BF16)
            kv[x, s, rows, 256:384] = p[:, QW + 256 : QW + 384].astype(BF16)
            return carry

        lax.fori_loop(0, T // TR, tile, 0)
        for d in range(1, NC):
            kv_copy(s, d).start()

    def kv_copy(s, d):
        return remote(
            kv.at[x, s], kv.at[x, s], kv_ss.at[s, d - 1], kv_rs.at[s, d - 1],
            "context", (x + d) % NC,
        )

    def head_mask(h, offset):
        lane = lax.broadcasted_iota(jnp.int32, (1, 256), 1)
        return jnp.logical_and(lane >= offset + h * HD, lane < offset + (h + 1) * HD)

    def keep(values, mask):
        return jnp.where(mask, values, jnp.zeros_like(values))

    def doc_bias(j, s):
        key_ids = jnp.broadcast_to(ids_all[j, pl.ds(s, 1), :].astype(F32), (128, T))
        key_col = jnp.transpose(key_ids)[:, 0:1]
        query_row = ids_all[x, pl.ds(s, 1), :].astype(F32)
        bias_ref[...] = jnp.where(key_col == query_row, 0.0, NEGATIVE)

    eye256 = eye(256)

    def attend(s):
        am[...] = jnp.full(am.shape, NEGATIVE, F32)
        al[...] = jnp.zeros(al.shape, F32)
        acc[...] = jnp.zeros(acc.shape, F32)

        def block(d, carry):
            j = (x + NC - d) % NC
            doc_bias(j, s)
            vt[...] = mm(eye256, kv[j, s, :, 128:384], NT).astype(BF16)

            def head(h, inner):
                keys = keep(kv[j, s, :, 0:256], head_mask(h, 0))
                scores = mm(keys, q_ref[s], NT) * scale + bias_ref[...]
                row = pl.ds(h, 1)
                before = am[row, :]
                newest = jnp.maximum(before, jnp.max(scores, axis=0, keepdims=True))
                shrink = jnp.exp(before - newest)
                weights = jnp.exp(scores - newest)
                al[row, :] = al[row, :] * shrink + jnp.sum(weights, axis=0, keepdims=True)
                am[row, :] = newest
                rows = pl.ds(pl.multiple_of(h * HD, HD), HD)
                vrows = pl.ds(pl.multiple_of(HD + h * HD, HD), HD)
                acc[vrows, :] = acc[vrows, :] * shrink + mm(
                    vt[vrows, :], weights.astype(BF16), NN
                )
                return inner

            lax.fori_loop(0, H, head, 0)
            return carry

        block(0, 0)
        if NC > 1:
            for d in range(1, NC):
                kv_copy(s, d).wait_recv()
            if s == 0:
                wait_recv(id_copies)
            lax.fori_loop(1, NC, block, 0)
        for h in range(H):
            rows = slice(HD + h * HD, HD + (h + 1) * HD)
            acc[rows, :] = acc[rows, :] / al[h : h + 1, :]
        tot[s] = am[...] + jnp.log(jnp.maximum(al[...], 1e-37))
        att[s] = jnp.transpose(acc[...]).astype(BF16)

    def rs_copy(rnd, s, part):
        if part < 2:
            chip = 1 - yy if part == 0 else yy
            return remote(
                rsend.at[s, chip, 1 - core], rsb.at[s, chip],
                rs_ss.at[rnd, s, part], rs_rs.at[rnd, s, part], "tensor", t_core,
            )
        return remote(
            rs2.at[s], rs2r.at[s], rs_ss.at[rnd, s, 2], rs_rs.at[rnd, s, 2], "tensor", t_y
        )

    def rs_produce(rnd, s, product):
        if rnd > 0:
            for part in range(3):
                rs_copy(rnd - 1, s, part).wait_send()

        def tile(i, carry):
            chip = jnp.where(i < 2, 1 - yy, yy)
            other = jnp.where(i % 2 == 0, 1 - core, core)
            start = pl.multiple_of((chip * 2 + other) * TS, TS)
            rsend[s, chip, other] = product(s, pl.ds(start, TS)).astype(BF16)
            return carry

        lax.fori_loop(0, 2, tile, 0)
        rs_copy(rnd, s, 0).start()
        lax.fori_loop(2, 4, tile, 0)
        rs_copy(rnd, s, 1).start()

    def rs_middle(rnd, s):
        rs_copy(rnd, s, 0).wait_recv()
        rs2[s] = (
            rsend[s, 1 - yy, core].astype(F32) + rsb[s, 1 - yy].astype(F32)
        ).astype(BF16)
        rs_copy(rnd, s, 2).start()

    def rs_finish(rnd, s):
        rs_copy(rnd, s, 1).wait_recv()
        rs_copy(rnd, s, 2).wait_recv()
        return rsend[s, yy, core].astype(F32) + rsb[s, yy].astype(F32) + rs2r[s].astype(F32)

    def ag_copy(rnd, buffer, s, part):
        if part == 0:
            return remote(
                buffer.at[s, t], buffer.at[s, t],
                ag_ss.at[rnd, s, 0], ag_rs.at[rnd, s, 0], "tensor", t_core,
            )
        if part == 1:
            return remote(
                buffer.at[s, t], buffer.at[s, t],
                ag_ss.at[rnd, s, 1], ag_rs.at[rnd, s, 1], "tensor", t_y,
            )
        return remote(
            buffer.at[s, t_y], buffer.at[s, t_y],
            ag_ss.at[rnd, s, 2], ag_rs.at[rnd, s, 2], "tensor", t_core,
        )

    def ag_start(rnd, buffer, s):
        ag_copy(rnd, buffer, s, 1).start()
        ag_copy(rnd, buffer, s, 0).start()

    def ag_middle(rnd, buffer, s):
        ag_copy(rnd, buffer, s, 1).wait_recv()
        ag_copy(rnd, buffer, s, 2).start()

    def ag_finish(rnd, buffer, s):
        ag_copy(rnd, buffer, s, 0).wait_recv()
        ag_copy(rnd, buffer, s, 2).wait_recv()

    def out_product(s, rows):
        return mm(att[s, rows, :], wo[...], NT)

    def first_norm(s):
        share = pl.ds(pl.multiple_of(t * TS, TS), TS)
        values = tok[s, share, :].astype(F32) + rs_finish(0, s)
        normed, unit, inverse = normalize(values, gains[0:1, :], biases[0:1, :])
        n1[s] = normed
        unit1[s] = unit
        inv1[s] = jnp.broadcast_to(inverse, (TS, 128))
        ag1[s, t] = normed.astype(BF16)
        ag_start(0, ag1, s)

    def sigmoid(v):
        return 1.0 / (1.0 + jnp.exp(-v))

    def gate_up(s):
        def tile(i, carry):
            rows = pl.ds(pl.multiple_of(i * TS, TS), TS)
            both = mm(ag1[s, i], wg[...], NN)
            gate, up = both[:, 0:F], both[:, F : 2 * F]
            gb[s, rows, 0:F] = gate.astype(BF16)
            gb[s, rows, F : 2 * F] = up.astype(BF16)
            hid[s, rows, :] = (gate * sigmoid(gate) * up).astype(BF16)
            return carry

        lax.fori_loop(0, NT4, tile, 0)

    def down_product(s, rows):
        return mm(hid[s, rows, :], wd[...], NT)

    def second_norm(s):
        values = n1[s] + rs_finish(1, s)
        out, unit, inverse = normalize(values, gains[1:2, :], biases[1:2, :])
        layer_out[s] = out.astype(BF16)
        grad = cot_v[s].astype(F32)
        sums = (jnp.sum(grad * unit, axis=0, keepdims=True), jnp.sum(grad, axis=0, keepdims=True))
        add_sums(s, 1, sums)
        back = norm_back(grad, unit, inverse, gains[1:2, :])
        n1[s] = back
        ag2[s, t] = back.astype(BF16)
        ag_start(1, ag2, s)

    def add_sums(s, row, sums):
        for k in range(2):
            at = slice(row + 2 * k, row + 2 * k + 1)
            if s == 0:
                nsum_t[t, at, :] = sums[k]
            else:
                nsum_t[t, at, :] = nsum_t[t, at, :] + sums[k]

    def hidden_back(s):
        def tile(i, carry):
            rows = pl.ds(pl.multiple_of(i * TS, TS), TS)
            grad = mm(ag2[s, i], wd[...], NN)
            gate = gb[s, rows, 0:F].astype(F32)
            up = gb[s, rows, F : 2 * F].astype(F32)
            sig = sigmoid(gate)
            act = gate * sig
            gb[s, rows, 0:F] = (grad * up * (sig + act * (1.0 - sig))).astype(BF16)
            gb[s, rows, F : 2 * F] = (grad * act).astype(BF16)
            return carry

        lax.fori_loop(0, NT4, tile, 0)

    def gate_product(s, rows):
        return mm(gb[s, rows, :], wg[...], NT)

    def first_norm_back(s):
        grad = n1[s] + rs_finish(2, s)
        unit = unit1[s]
        sums = (jnp.sum(grad * unit, axis=0, keepdims=True), jnp.sum(grad, axis=0, keepdims=True))
        add_sums(s, 0, sums)
        back = norm_back(grad, unit, inv1[s, :, 0:1], gains[0:1, :])
        n1[s] = back
        ag3[s, t] = back.astype(BF16)
        ag_start(2, ag3, s)

    def weight_grad(dest, left_of, right):
        def tile(i, carry):
            columns = pl.ds(pl.multiple_of(i * 128, 128), 128)
            dest[columns, :] = mm(left_of(columns), right, TN).astype(BF16)
            return carry

        lax.fori_loop(0, D // 128, tile, 0)

    def reduce_start(slot, source, landing):
        for d in range(1, NF):
            reduce_copy(slot, source, landing, d).start()

    def reduce_copy(slot, source, landing, d):
        to = (z + d) % NF
        return remote(
            source.at[own_rows(to), :], landing.at[d - 1],
            gr_ss.at[slot, d - 1], gr_rs.at[slot, d - 1], "fsdp", to,
        )

    def reduce_middle(slot, source, landing, crossing):
        for d in range(1, NF):
            reduce_copy(slot, source, landing, d).wait_recv()
        total = source[own_rows(z), :].astype(F32)
        for d in range(1, NF):
            total = total + landing[d - 1].astype(F32)
        crossing[x] = total.astype(BF16)
        for d in range(1, NC):
            cross_copy(slot, crossing, d).start()

    def cross_copy(slot, crossing, d):
        return remote(
            crossing.at[x], crossing.at[x],
            x_ss.at[slot, d - 1], x_rs.at[slot, d - 1], "context", (x + d) % NC,
        )

    def reduce_finish(slot, source, landing, crossing, out):
        for d in range(1, NC):
            cross_copy(slot, crossing, d).wait_recv()
        total = crossing[0].astype(F32)
        for i in range(1, NC):
            total = total + crossing[i].astype(F32)
        out[...] = total
        for d in range(1, NC):
            cross_copy(slot, crossing, d).wait_send()
        for d in range(1, NF):
            reduce_copy(slot, source, landing, d).wait_send()

    def norm_copy(buffer, axis, me, count, base, d):
        return remote(
            buffer.at[me], buffer.at[me], n_ss.at[base + d - 1], n_rs.at[base + d - 1],
            axis, (me + d) % count,
        )

    norm_levels = (
        (nsum_t, "tensor", t, NT4, 0),
        (nsum_c, "context", x, NC, NT4 - 1),
        (nsum_f, "fsdp", z, NF, NT4 - 1 + NC - 1),
    )

    def norm_start(level):
        for d in range(1, norm_levels[level][3]):
            norm_copy(*norm_levels[level], d).start()

    def norm_total(level):
        buffer, count = norm_levels[level][0], norm_levels[level][3]
        for d in range(1, count):
            norm_copy(*norm_levels[level], d).wait_recv()
        total = buffer[0]
        for i in range(1, count):
            total = total + buffer[i]
        return total

    def attended_back(s):
        def tile(i, carry):
            rows = pl.ds(pl.multiple_of(i * TS, TS), TS)
            datt[s, rows, :] = mm(ag3[s, i], wo[...], NN).astype(BF16)
            return carry

        lax.fori_loop(0, NT4, tile, 0)
        both = datt[s].astype(F32) * att[s].astype(F32)
        head_row = lax.broadcasted_iota(jnp.int32, (8, 256), 0)
        lane = lax.broadcasted_iota(jnp.int32, (8, 256), 1)
        chooser = (lane // HD == head_row + 1).astype(F32)
        dlt[s] = lax.dot_general(
            chooser, both, NT, precision=lax.Precision.HIGHEST, preferred_element_type=F32
        )

    def kvg_copy(s, d):
        return remote(
            kvg_s.at[(d - 1) % KS, s], kvg_r.at[d - 1, s],
            kvg_ss.at[d - 1, s], kvg_rs.at[d - 1, s], "context", (x + NC - d) % NC,
        )

    def attend_back(s):
        dqt[...] = jnp.zeros(dqt.shape, F32)

        def block(d):
            j = (x + NC - d) % NC
            doc_bias(j, s)
            vt[...] = mm(eye256, kv[j, s, :, 0:256], NT).astype(BF16)
            dk[...] = jnp.zeros(dk.shape, F32)
            dv[...] = jnp.zeros(dv.shape, F32)

            def head(h, inner):
                key_mask, value_mask = head_mask(h, 0), head_mask(h, HD)
                keys = keep(kv[j, s, :, 0:256], key_mask)
                row = pl.ds(h, 1)
                scores = mm(keys, q_ref[s], NT) * scale + bias_ref[...]
                probs = jnp.exp(scores - tot[s, row, :])
                dv[...] += mm(probs.astype(BF16), keep(datt[s], value_mask), NN)
                grad_probs = mm(keep(kv[j, s, :, 128:384], value_mask), datt[s], NT)
                grads = (probs * (grad_probs - dlt[s, row, :])).astype(BF16)
                dk[...] += mm(grads, keep(q_ref[s], key_mask), NN)
                rows = pl.ds(pl.multiple_of(h * HD, HD), HD)
                dqt[rows, :] += mm(vt[rows, :], grads, NN)
                return inner

            lax.fori_loop(0, H, head, 0)
            first = dk[:, 0:128] * scale
            second = dk[:, 128:256] * scale + dv[:, 0:128]
            return first, second, dv[:, 128:256]

        def far(d, carry):
            parts = block(d)
            if NC - 1 > KS:

                @pl.when(d > KS)
                def _():
                    kvg_copy(s, d - KS).wait_send()

            for k in range(3):
                kvg_s[(d - 1) % KS, s, :, k * 128 : (k + 1) * 128] = parts[k].astype(BF16)
            kvg_copy(s, d).start()
            return carry

        if NC > 1:
            lax.fori_loop(1, NC, far, 0)
        parts = block(0)
        for k in range(3):
            kv_own[s, :, k * 128 : (k + 1) * 128] = parts[k]
        grad = jnp.transpose(dqt[...]) * scale
        q0, q1 = rotate_pair(grad, slice(0, T), -1.0)
        qb[s, :, 0:128] = q0.astype(BF16)
        qb[s, :, 128:256] = q1.astype(BF16)

    def keys_back(s):
        for d in range(1, NC):
            kvg_copy(s, d).wait_recv()

        def column(k):
            cols = slice(k * 128, (k + 1) * 128)
            total = kv_own[s, :, cols]
            for d in range(1, NC):
                total = total + kvg_r[d - 1, s, :, cols].astype(F32)
            return total

        k0, k1 = rotate_pair(
            jnp.concatenate([column(0), column(1)], axis=1), slice(0, T), -1.0
        )
        qb[s, :, QW : QW + 128] = k0.astype(BF16)
        qb[s, :, QW + 128 : QW + 256] = k1.astype(BF16)
        qb[s, :, QW + 256 : QW + 384] = column(2).astype(BF16)

    def input_product(s, rows):
        return mm(qb[s, rows, :], wq[...], NT)

    def input_out(s):
        input_grad[s] = n1[s] + rs_finish(3, s)

    seqs = range(S)
    R = S * T

    for s in seqs:
        project(s)
    wait_recv(wo_copies)
    wg_copies = gather(wg, 2)
    wd_copies = gather(wd, 3)
    for s in seqs:
        attend(s)
        if s > 0:
            rs_middle(0, s - 1)
        rs_produce(0, s, out_product)
        if s > 0:
            first_norm(s - 1)
    rs_middle(0, S - 1)
    first_norm(S - 1)
    wait_recv(wg_copies)
    for s in seqs:
        ag_middle(0, ag1, s)
    for s in seqs:
        ag_finish(0, ag1, s)
        gate_up(s)
        if s == 0:
            wait_recv(wd_copies)
        rs_produce(1, s, down_product)
        if s > 0:
            rs_middle(1, s - 1)
    rs_middle(1, S - 1)
    cot_copy.wait()
    nsum_t[t] = jnp.zeros(nsum_t.shape[1:], F32)
    for s in seqs:
        second_norm(s)
    for s in seqs:
        ag_middle(1, ag2, s)
    for s in seqs:
        ag_finish(1, ag2, s)
        hidden_back(s)
        rs_produce(2, s, gate_product)
        if s > 0:
            rs_middle(2, s - 1)
    rs_middle(2, S - 1)
    flat_hid = hid[...].reshape(R, F)
    weight_grad(gsd, lambda c: ag2[:, :, :, c].reshape(R, 128), flat_hid)
    reduce_start(3, gsd, grd)
    for s in seqs:
        first_norm_back(s)
    norm_start(0)
    weight_grad(gsg, lambda c: ag1[:, :, :, c].reshape(R, 128), gb[...].reshape(R, 2 * F))
    reduce_start(2, gsg, grg)
    for s in seqs:
        ag_middle(2, ag3, s)
    for s in seqs:
        ag_finish(2, ag3, s)
        attended_back(s)
        if s == 0:
            nsum_c[x] = norm_total(0)
            norm_start(1)
        attend_back(s)
    nsum_f[z] = norm_total(1)
    norm_start(2)
    weight_grad(gso, lambda c: ag3[:, :, :, c].reshape(R, 128), att[...].reshape(R, 256))
    reduce_start(1, gso, gro)
    for s in seqs:
        keys_back(s)
        rs_produce(3, s, input_product)
        if s > 0:
            rs_middle(3, s - 1)
    rs_middle(3, S - 1)
    weight_grad(gsq, lambda c: tok[:, :, c].reshape(R, 128), qb[...].reshape(R, QW + KW))
    reduce_start(0, gsq, grq)
    norm_out[...] = norm_total(2)
    reduce_middle(3, gsd, grd, xd)
    reduce_middle(2, gsg, grg, xg)
    reduce_middle(1, gso, gro, xo)
    for s in seqs:
        input_out(s)
    reduce_middle(0, gsq, grq, xq)
    reduce_finish(3, gsd, grd, xd, gd_out)
    reduce_finish(2, gsg, grg, xg, gg_out)
    reduce_finish(1, gso, gro, xo, go_out)
    reduce_finish(0, gsq, grq, xq, gq_out)

    for copies in (wq_copies, wo_copies, wg_copies, wd_copies, id_copies):
        wait_send(copies)
    for s in seqs:
        for d in range(1, NC):
            kv_copy(s, d).wait_send()
            if d > NC - 1 - KS:
                kvg_copy(s, d).wait_send()
        for part in range(3):
            rs_copy(3, s, part).wait_send()
        for rnd, buffer in ((0, ag1), (1, ag2), (2, ag3)):
            for part in range(3):
                ag_copy(rnd, buffer, s, part).wait_send()
    for level in range(3):
        for d in range(1, norm_levels[level][3]):
            norm_copy(*norm_levels[level], d).wait_send()


def run_layer(tokens, cotangent, segment_ids, weights, norm_gains, norm_biases, cosine, sine_rows):
    qkv_weight, out_weight, gate_up_weight, down_weight = weights
    S, T, D = tokens.shape
    C, F = qkv_weight.shape[2], gate_up_weight.shape[2]
    NF, NC, NT4 = lax.axis_size("fsdp"), lax.axis_size("context"), lax.axis_size("tensor")
    TS, DB, KW, W = T // NT4, D // NF, 384, 640
    assert NT4 == 4 and C == 192
    vmem = pl.BlockSpec(memory_space=pltpu.VMEM)
    far = pl.BlockSpec(memory_space=pl.ANY)
    VM = pltpu.VMEM
    DMA = pltpu.SemaphoreType.DMA
    NX = max(NC - 1, 1)
    scratch = [
        VM((D, W), BF16), VM((D, 256), BF16), VM((D, 2 * F), BF16), VM((D, F), BF16),
        VM((NC, S, T), jnp.int32), VM((S, T, 256), BF16), VM((NC, S, T, KW), BF16),
        VM((S, T, 256), BF16), VM((S, 8, T), F32), VM((8, T), F32), VM((8, T), F32),
        VM((256, T), F32), VM((T, T), F32), VM((256, T), BF16),
        VM((S, 2, 2, TS, D), BF16), VM((S, 2, TS, D), BF16), VM((S, TS, D), BF16), VM((S, TS, D), BF16),
        VM((S, 4, TS, D), BF16), VM((S, 4, TS, D), BF16), VM((S, 4, TS, D), BF16),
        VM((S, T, F), BF16), VM((S, T, 2 * F), BF16),
        VM((S, TS, D), F32), VM((S, TS, D), F32), VM((S, TS, 128), F32),
        VM((S, T, 256), BF16), VM((S, 8, T), F32), VM((256, T), F32),
        VM((T, 256), F32), VM((T, 256), F32), VM((min(NX, 2), S, T, KW), BF16), VM((NX, S, T, KW), BF16),
        VM((S, T, KW), F32), VM((S, T, W), BF16),
        VM((D, W), BF16), VM((D, 256), BF16), VM((D, 2 * F), BF16), VM((D, F), BF16),
        VM((NF - 1, DB, W), BF16), VM((NF - 1, DB, 256), BF16), VM((NF - 1, DB, 2 * F), BF16),
        VM((NF - 1, DB, F), BF16),
        VM((NC, DB, W), BF16), VM((NC, DB, 256), BF16), VM((NC, DB, 2 * F), BF16), VM((NC, DB, F), BF16),
        VM((NT4, 8, D), F32), VM((NC, 8, D), F32), VM((NF, 8, D), F32), VM((S, TS, D), BF16),
        DMA((4, NF - 1)), DMA((4, NF - 1)), DMA((S, NX)), DMA((S, NX)), DMA((NX,)), DMA((NX,)),
        DMA((4, S, 3)), DMA((4, S, 3)), DMA((3, S, 3)), DMA((3, S, 3)),
        DMA((NX, S)), DMA((NX, S)), DMA((4, NF - 1)), DMA((4, NF - 1)), DMA((4, NX)), DMA((4, NX)),
        DMA((NT4 + NC + NF,)), DMA((NT4 + NC + NF,)), DMA((1,)),
    ]
    outs = (
        jax.ShapeDtypeStruct((S, TS, D), BF16),
        jax.ShapeDtypeStruct((S, TS, D), F32),
        jax.ShapeDtypeStruct((DB, W), F32),
        jax.ShapeDtypeStruct((DB, 256), F32),
        jax.ShapeDtypeStruct((DB, 2 * F), F32),
        jax.ShapeDtypeStruct((DB, F), F32),
        jax.ShapeDtypeStruct((8, D), F32),
    )
    return pl.pallas_call(
        functools.partial(layer_kernel, (S, T, D, C, F, NF, NC, NT4)),
        out_shape=outs,
        in_specs=[vmem, far] + [vmem] * 9,
        out_specs=[vmem] * len(outs),
        scratch_shapes=scratch,
        compiler_params=pltpu.CompilerParams(
            collective_id=0, has_side_effects=True, vmem_limit_bytes=67043328
        ),
        name="layer",
    )(
        tokens, cotangent, segment_ids, qkv_weight, out_weight, gate_up_weight, down_weight,
        norm_gains, norm_biases, cosine, sine_rows,
    )


def from_root(block, axis, owner):
    block = jnp.where(lax.axis_index(axis) == owner, block, jnp.zeros_like(block))
    return lax.psum(block, axis)


def moment_pair(gradient, moment, square):
    moment_new = BETA_ONE * moment + (1.0 - BETA_ONE) * gradient
    square_new = BETA_TWO * square + (1.0 - BETA_TWO) * gradient * gradient
    return jnp.stack([moment_new, square_new])


def step_of(pair_new, master, decay_rate):
    corrected = pair_new[0] / (1.0 - BETA_ONE**ADAM_STEP)
    scaled = pair_new[1] / (1.0 - BETA_TWO**ADAM_STEP)
    return -RATE * (corrected / (jnp.sqrt(scaled) + ADAM_EPS) + decay_rate * master)


def shards(
    tokens, cotangent, segment_ids, owner, qkv_weight, out_weight, gate_up_weight, down_weight,
    norm_gains, norm_biases, qkv_moment, qkv_square, out_moment, out_square, gate_moment,
    gate_square, down_moment, down_square, norm_moment, norm_square,
):
    seqs_here, tok_here, model_width = tokens.shape
    head_cols = qkv_weight.shape[2]
    hidden_here = gate_up_weight.shape[2]
    tensor_size, fsdp_size = lax.axis_size("tensor"), lax.axis_size("fsdp")
    masters = (qkv_weight, out_weight, gate_up_weight, down_weight)
    moments = (
        (qkv_moment, qkv_square), (out_moment, out_square),
        (gate_moment, gate_square), (down_moment, down_square),
    )
    owned = [
        [
            from_root(slot[0].astype(BF16), "context", owner[k]).astype(F32)
            for slot in moments[k]
        ]
        for k in range(4)
    ]
    positions = (
        lax.axis_index("context") * tok_here + jnp.arange(tok_here, dtype=jnp.int32)
    ).astype(F32)
    frequency = jnp.power(F32(ROPE_BASE), -jnp.arange(0, HD, 2, dtype=F32) / HD)
    angles = positions[:, None] * frequency[None, :]
    cosine, sine_rows = jnp.cos(angles), jnp.sin(angles)
    cosine = jnp.concatenate([cosine] * 4, axis=1)
    sine_rows = jnp.concatenate([-sine_rows, sine_rows] * 2, axis=1)

    layer_out, input_grad, grad_q, grad_o, grad_g, grad_d, norm_sums = run_layer(
        tokens, cotangent, segment_ids, masters, norm_gains, norm_biases, cosine, sine_rows
    )
    rows = qkv_weight.shape[0]
    weight_grads = (
        jnp.concatenate([grad_q[:, :head_cols], grad_q[:, 256:]], axis=1).reshape(rows, 3, head_cols),
        jnp.transpose(grad_o[:, HD:]),
        grad_g.reshape(rows, 2, hidden_here),
        jnp.transpose(grad_d),
    )
    norm_grad = norm_sums[:4]
    new_pairs = [moment_pair(weight_grads[k], owned[k][0], owned[k][1]) for k in range(4)]
    new_steps = [step_of(new_pairs[k], masters[k], DECAY) for k in range(4)]
    norm_master = jnp.concatenate([norm_gains, norm_biases], axis=0)
    norm_state = moment_pair(norm_grad, norm_moment, norm_square)
    norm_step = step_of(norm_state, norm_master, 0.0).reshape(-1)
    piece = norm_step.shape[0] // (fsdp_size * tensor_size)
    start = (lax.axis_index("fsdp") * tensor_size + lax.axis_index("tensor")) * piece
    norm_piece = lax.dynamic_slice_in_dim(norm_step, start, piece, 0)
    weight_updates = jnp.concatenate(
        [value.reshape(-1) for value in new_steps] + [norm_piece], axis=0
    ).reshape(1, 1, -1)
    return (
        layer_out, input_grad, *weight_grads, norm_grad, *new_pairs, norm_state, weight_updates
    )


def solution(mesh):
    return jax.shard_map(
        shards,
        mesh=mesh,
        in_specs=(
            P("fsdp", "context", None),
            P("fsdp", "context", None),
            P("fsdp", "context"),
            P(),
            P("fsdp", None, "tensor"),
            P("tensor", "fsdp"),
            P("fsdp", None, "tensor"),
            P("tensor", "fsdp"),
            P(),
            P(),
            P("context", "fsdp", None, "tensor"),
            P("context", "fsdp", None, "tensor"),
            P("context", "tensor", "fsdp"),
            P("context", "tensor", "fsdp"),
            P("context", "fsdp", None, "tensor"),
            P("context", "fsdp", None, "tensor"),
            P("context", "tensor", "fsdp"),
            P("context", "tensor", "fsdp"),
            P(),
            P(),
        ),
        out_specs=(
            P("fsdp", ("context", "tensor"), None),
            P("fsdp", ("context", "tensor"), None),
            P("fsdp", None, "tensor"),
            P("tensor", "fsdp"),
            P("fsdp", None, "tensor"),
            P("tensor", "fsdp"),
            P(),
            P(None, "fsdp", None, "tensor"),
            P(None, "tensor", "fsdp"),
            P(None, "fsdp", None, "tensor"),
            P(None, "tensor", "fsdp"),
            P(),
            P("fsdp", "tensor", None),
        ),
        check_vma=False,
    )
```

```python
import functools
import math

import jax
import jax.numpy as jnp
from jax import lax
from jax.experimental import pallas as pl
from jax.experimental.pallas import tpu as pltpu
from jax.sharding import PartitionSpec as P

HD = 64

NEGATIVE = -1e30
EPSILON = 1e-05
ROPE_BASE = 1000.0
BETA_ONE = 0.9
BETA_TWO = 0.999
ADAM_EPS = 1e-08
ADAM_STEP = 3.0
RATE = 0.03
DECAY = 0.1

F32 = jnp.float32
BF16 = jnp.bfloat16
MESH = pl.DeviceIdType.MESH
NN = (((1,), (0,)), ((), ()))
NT = (((1,), (1,)), ((), ()))
TN = (((0,), (0,)), ((), ()))


def mm(left, right, dims):
    return lax.dot_general(left, right, dims, preferred_element_type=F32)


def swap_halves(values):
    lane = lax.broadcasted_iota(jnp.int32, values.shape, 1)
    low_half = lane % HD < HD // 2
    return jnp.where(
        low_half,
        pltpu.roll(values, 128 - HD // 2, 1),
        pltpu.roll(values, HD // 2, 1),
    )


def mean_of(values):
    return jnp.sum(values, axis=-1, keepdims=True) * (1.0 / values.shape[-1])


def normalize(values, gain_row, bias_row):
    center = values - mean_of(values)
    inverse_std = lax.rsqrt(mean_of(center * center) + EPSILON)
    unit = center * inverse_std
    return unit * gain_row + bias_row, unit, inverse_std


def norm_back(gradient, unit, inverse_std, gain_row):
    scaled = gradient * gain_row
    return inverse_std * (scaled - mean_of(scaled) - unit * mean_of(scaled * unit))


class Pack:
    pass


def layer_kernel(dims, *refs):
    S, T, D, C, F, NF, NC, NT4 = dims
    adam = NC == 2
    refs = list(refs)
    TS = T // NT4
    DB = D // NF
    QW, KW = 256, 384
    H = C // HD
    KS = min(max(NC - 1, 1), 2)
    scale = HD ** (-0.5)
    def take(count):
        taken, refs[:] = refs[:count], refs[count:]
        return taken

    tok, cot, ids_in, wq_in, wo_in, wg_in, wd_in, gains, biases, cos_t, sin_t = take(11)
    if adam:
        moments = take(8)
    layer_out, input_grad = take(2)
    own_out, crosses = take(4), take(4)
    norm_out = take(1)[0]
    if adam:
        lands = take(4)
    wq, wo, wg, wd, ids_all, q_ref, kv, att, tot, am, al, acc, bias_ref, vt = take(14)
    rsend, rsb, rs2, rs2r, ag1, ag2, ag3, hid, gb = take(9)
    n1, unit1, inv1, datt, dlt, dk, dv, kvg_s, kvg_r, kv_own, qb = take(11)
    dqt = acc
    gsq, gso, gsg, gsd, grq, gro, grg, grd = take(8)
    xq, xo, xg, xd = crosses
    nsum_t, nsum_c, nsum_f, cot_v = take(4)
    w_ss, w_rs, kv_ss, kv_rs, id_ss, id_rs, rs_ss, rs_rs, ag_ss, ag_rs = take(10)
    kvg_ss, kvg_rs, gr_ss, gr_rs, x_ss, x_rs, n_ss, n_rs, loc_sem = take(9)
    own_sem = take(1)[0]
    if adam:
        stages, sends = take(4), take(4)
        m_ss, m_rs, in_sem = take(3)

    z, x, t = lax.axis_index("fsdp"), lax.axis_index("context"), lax.axis_index("tensor")
    core, yy = t % 2, t // 2
    t_core = yy * 2 + (1 - core)
    t_y = (1 - yy) * 2 + core
    t_diag = (1 - yy) * 2 + (1 - core)

    def remote(src, dst, ssem, rsem, axis, index):
        return pltpu.make_async_remote_copy(
            src_ref=src, dst_ref=dst, send_sem=ssem, recv_sem=rsem,
            device_id={axis: index}, device_id_type=MESH,
        )

    barrier = pltpu.get_barrier_semaphore()
    for d in range(1, NF):
        pl.semaphore_signal(barrier, inc=1, device_id={"fsdp": (z + d) % NF}, device_id_type=MESH)
    for d in range(1, NC):
        pl.semaphore_signal(barrier, inc=1, device_id={"context": (x + d) % NC}, device_id_type=MESH)
    for d in range(1, NT4):
        pl.semaphore_signal(barrier, inc=1, device_id={"tensor": (t + d) % NT4}, device_id_type=MESH)

    def moment_load(k, i):
        return pltpu.make_async_copy(
            moments[2 * k + i].at[0], stages[k].at[i], in_sem.at[k, i]
        )

    cot_copy = pltpu.make_async_copy(
        cot.at[:, pl.ds(pl.multiple_of(t * TS, TS), TS), :], cot_v, loc_sem.at[0]
    )
    cot_copy.start()
    if adam:
        for k in range(4):
            for i in range(2):
                moment_load(k, i).start()

    def own_rows(index):
        return pl.ds(pl.multiple_of(index * DB, DB), DB)

    def pad_cols(values, left, right):
        parts = []
        if left:
            parts.append(jnp.zeros((values.shape[0], left), values.dtype))
        parts.append(values)
        if right:
            parts.append(jnp.zeros((values.shape[0], right), values.dtype))
        return jnp.concatenate(parts, axis=1)

    wq[own_rows(z), :] = jnp.concatenate(
        [
            pad_cols(wq_in[0], 0, QW - C),
            jnp.concatenate([wq_in[1], wq_in[2]], axis=1),
        ],
        axis=1,
    ).astype(BF16)

    pl.semaphore_wait(barrier, NF - 1 + NC - 1 + NT4 - 1)

    def gather(buffer, slot):
        copies = []
        for d in range(1, NF):
            copies.append(
                remote(
                    buffer.at[own_rows(z), :], buffer.at[own_rows(z), :],
                    w_ss.at[slot, d - 1], w_rs.at[slot, d - 1], "fsdp", (z + d) % NF,
                )
            )
        for c in copies:
            c.start()
        return copies

    def wait_recv(copies):
        for c in copies:
            c.wait_recv()

    def wait_send(copies):
        for c in copies:
            c.wait_send()

    wq_copies = gather(wq, 0)

    ids_all[x] = ids_in[...]
    id_copies = []
    for d in range(1, NC):
        c = remote(
            ids_all.at[x], ids_all.at[x], id_ss.at[d - 1], id_rs.at[d - 1],
            "context", (x + d) % NC,
        )
        c.start()
        id_copies.append(c)

    def eye(n):
        return (
            lax.broadcasted_iota(jnp.int32, (n, n), 0)
            == lax.broadcasted_iota(jnp.int32, (n, n), 1)
        ).astype(F32).astype(BF16)

    wo_t = jnp.transpose(wo_in[...])
    wo[own_rows(z), :] = pad_cols(wo_t, HD, 0).astype(BF16)
    wd[own_rows(z), :] = wd_in[...].astype(BF16)
    wg[own_rows(z), 0:F] = wg_in[:, 0, :].astype(BF16)
    wg[own_rows(z), F : 2 * F] = wg_in[:, 1, :].astype(BF16)

    wait_recv(wq_copies)
    wo_copies = gather(wo, 1)

    def rotate_pair(values, rows, sign):
        cosine, sine_rows = cos_t[rows, :], sin_t[rows, :] * sign
        lane = lax.broadcasted_iota(jnp.int32, cosine.shape, 1)
        head = lane < HD
        first, second = values[:, 0:128], values[:, 128:256]
        first = first * cosine + swap_halves(first) * sine_rows
        second = second * jnp.where(head, cosine, 1.0) + swap_halves(second) * jnp.where(
            head, sine_rows, 0.0
        )
        return first, second

    TR = min(256, T)

    def project(s):
        def tile(i, carry):
            rows = pl.ds(pl.multiple_of(i * TR, TR), TR)
            p = mm(tok[s, rows, :], wq[...], NN)
            q0, q1 = rotate_pair(p[:, 0:QW], rows, 1.0)
            q_ref[s, rows, 0:128] = q0.astype(BF16)
            q_ref[s, rows, 128:256] = q1.astype(BF16)
            k0, k1 = rotate_pair(p[:, QW : QW + 256], rows, 1.0)
            kv[x, s, rows, 0:128] = k0.astype(BF16)
            kv[x, s, rows, 128:256] = k1.astype(BF16)
            kv[x, s, rows, 256:384] = p[:, QW + 256 : QW + 384].astype(BF16)
            return carry

        lax.fori_loop(0, T // TR, tile, 0)
        for d in range(1, NC):
            kv_copy(s, d).start()

    def kv_copy(s, d):
        return remote(
            kv.at[x, s], kv.at[x, s], kv_ss.at[s, d - 1], kv_rs.at[s, d - 1],
            "context", (x + d) % NC,
        )

    def head_mask(h, offset):
        lane = lax.broadcasted_iota(jnp.int32, (1, 256), 1)
        return jnp.logical_and(lane >= offset + h * HD, lane < offset + (h + 1) * HD)

    def keep(values, mask):
        return jnp.where(mask, values, jnp.zeros_like(values))

    def doc_bias(j, s):
        key_ids = jnp.broadcast_to(ids_all[j, pl.ds(s, 1), :].astype(F32), (128, T))
        key_col = jnp.transpose(key_ids)[:, 0:1]
        query_row = ids_all[x, pl.ds(s, 1), :].astype(F32)
        bias_ref[...] = jnp.where(key_col == query_row, 0.0, NEGATIVE)

    eye256 = eye(256)

    def attend(s):
        am[...] = jnp.full(am.shape, NEGATIVE, F32)
        al[...] = jnp.zeros(al.shape, F32)
        acc[...] = jnp.zeros(acc.shape, F32)

        def block(d, carry):
            j = (x + NC - d) % NC
            doc_bias(j, s)
            vt[...] = mm(eye256, kv[j, s, :, 128:384], NT).astype(BF16)

            def head(h, inner):
                keys = keep(kv[j, s, :, 0:256], head_mask(h, 0))
                scores = mm(keys, q_ref[s], NT) * scale + bias_ref[...]
                row = pl.ds(h, 1)
                before = am[row, :]
                newest = jnp.maximum(before, jnp.max(scores, axis=0, keepdims=True))
                shrink = jnp.exp(before - newest)
                weights = jnp.exp(scores - newest)
                al[row, :] = al[row, :] * shrink + jnp.sum(weights, axis=0, keepdims=True)
                am[row, :] = newest
                rows = pl.ds(pl.multiple_of(h * HD, HD), HD)
                vrows = pl.ds(pl.multiple_of(HD + h * HD, HD), HD)
                acc[vrows, :] = acc[vrows, :] * shrink + mm(
                    vt[vrows, :], weights.astype(BF16), NN
                )
                return inner

            lax.fori_loop(0, H, head, 0)
            return carry

        block(0, 0)
        if NC > 1:
            for d in range(1, NC):
                kv_copy(s, d).wait_recv()
            if s == 0:
                wait_recv(id_copies)
            lax.fori_loop(1, NC, block, 0)
        for h in range(H):
            rows = slice(HD + h * HD, HD + (h + 1) * HD)
            acc[rows, :] = acc[rows, :] / al[h : h + 1, :]
        tot[s] = am[...] + jnp.log(jnp.maximum(al[...], 1e-37))
        att[s] = jnp.transpose(acc[...]).astype(BF16)

    def rs_copy(rnd, s, part):
        if part < 2:
            chip = 1 - yy if part == 0 else yy
            return remote(
                rsend.at[s, chip, 1 - core], rsb.at[s, chip],
                rs_ss.at[rnd, s, part], rs_rs.at[rnd, s, part], "tensor", t_core,
            )
        return remote(
            rs2.at[s], rs2r.at[s], rs_ss.at[rnd, s, 2], rs_rs.at[rnd, s, 2], "tensor", t_y
        )

    def rs_produce(rnd, s, product):
        if rnd > 0:
            for part in range(3):
                rs_copy(rnd - 1, s, part).wait_send()

        def tile(i, carry):
            chip = jnp.where(i < 2, 1 - yy, yy)
            other = jnp.where(i % 2 == 0, 1 - core, core)
            start = pl.multiple_of((chip * 2 + other) * TS, TS)
            rsend[s, chip, other] = product(s, pl.ds(start, TS)).astype(BF16)
            return carry

        lax.fori_loop(0, 2, tile, 0)
        rs_copy(rnd, s, 0).start()
        lax.fori_loop(2, 4, tile, 0)
        rs_copy(rnd, s, 1).start()

    def rs_middle(rnd, s):
        rs_copy(rnd, s, 0).wait_recv()
        rs2[s] = (
            rsend[s, 1 - yy, core].astype(F32) + rsb[s, 1 - yy].astype(F32)
        ).astype(BF16)
        rs_copy(rnd, s, 2).start()

    def rs_finish(rnd, s):
        rs_copy(rnd, s, 1).wait_recv()
        rs_copy(rnd, s, 2).wait_recv()
        return rsend[s, yy, core].astype(F32) + rsb[s, yy].astype(F32) + rs2r[s].astype(F32)

    def ag_copy(rnd, buffer, s, part):
        if part == 0:
            return remote(
                buffer.at[s, t], buffer.at[s, t],
                ag_ss.at[rnd, s, 0], ag_rs.at[rnd, s, 0], "tensor", t_core,
            )
        if part == 1:
            return remote(
                buffer.at[s, t], buffer.at[s, t],
                ag_ss.at[rnd, s, 1], ag_rs.at[rnd, s, 1], "tensor", t_y,
            )
        return remote(
            buffer.at[s, t_y], buffer.at[s, t_y],
            ag_ss.at[rnd, s, 2], ag_rs.at[rnd, s, 2], "tensor", t_core,
        )

    def ag_start(rnd, buffer, s):
        ag_copy(rnd, buffer, s, 1).start()
        ag_copy(rnd, buffer, s, 0).start()

    def ag_middle(rnd, buffer, s):
        ag_copy(rnd, buffer, s, 1).wait_recv()
        ag_copy(rnd, buffer, s, 2).start()

    def ag_finish(rnd, buffer, s):
        ag_copy(rnd, buffer, s, 0).wait_recv()
        ag_copy(rnd, buffer, s, 2).wait_recv()

    def out_product(s, rows):
        return mm(att[s, rows, :], wo[...], NT)

    def first_norm(s):
        share = pl.ds(pl.multiple_of(t * TS, TS), TS)
        values = tok[s, share, :].astype(F32) + rs_finish(0, s)
        normed, unit, inverse = normalize(values, gains[0:1, :], biases[0:1, :])
        n1[s] = normed
        unit1[s] = unit
        inv1[s] = jnp.broadcast_to(inverse, (TS, 128))
        ag1[s, t] = normed.astype(BF16)
        ag_start(0, ag1, s)

    def sigmoid(v):
        return 1.0 / (1.0 + jnp.exp(-v))

    def gate_up(s):
        def tile(i, carry):
            rows = pl.ds(pl.multiple_of(i * TS, TS), TS)
            both = mm(ag1[s, i], wg[...], NN)
            gate, up = both[:, 0:F], both[:, F : 2 * F]
            gb[s, rows, 0:F] = gate.astype(BF16)
            gb[s, rows, F : 2 * F] = up.astype(BF16)
            hid[s, rows, :] = (gate * sigmoid(gate) * up).astype(BF16)
            return carry

        lax.fori_loop(0, NT4, tile, 0)

    def down_product(s, rows):
        return mm(hid[s, rows, :], wd[...], NT)

    def second_norm(s):
        values = n1[s] + rs_finish(1, s)
        out, unit, inverse = normalize(values, gains[1:2, :], biases[1:2, :])
        layer_out[s] = out.astype(BF16)
        grad = cot_v[s].astype(F32)
        sums = (jnp.sum(grad * unit, axis=0, keepdims=True), jnp.sum(grad, axis=0, keepdims=True))
        add_sums(s, 1, sums)
        back = norm_back(grad, unit, inverse, gains[1:2, :])
        n1[s] = back
        ag2[s, t] = back.astype(BF16)
        ag_start(1, ag2, s)

    def add_sums(s, row, sums):
        for k in range(2):
            at = slice(row + 2 * k, row + 2 * k + 1)
            if s == 0:
                nsum_t[t, at, :] = sums[k]
            else:
                nsum_t[t, at, :] = nsum_t[t, at, :] + sums[k]

    def hidden_back(s):
        def tile(i, carry):
            rows = pl.ds(pl.multiple_of(i * TS, TS), TS)
            grad = mm(ag2[s, i], wd[...], NN)
            gate = gb[s, rows, 0:F].astype(F32)
            up = gb[s, rows, F : 2 * F].astype(F32)
            sig = sigmoid(gate)
            act = gate * sig
            gb[s, rows, 0:F] = (grad * up * (sig + act * (1.0 - sig))).astype(BF16)
            gb[s, rows, F : 2 * F] = (grad * act).astype(BF16)
            return carry

        lax.fori_loop(0, NT4, tile, 0)

    def gate_product(s, rows):
        return mm(gb[s, rows, :], wg[...], NT)

    def first_norm_back(s):
        grad = n1[s] + rs_finish(2, s)
        unit = unit1[s]
        sums = (jnp.sum(grad * unit, axis=0, keepdims=True), jnp.sum(grad, axis=0, keepdims=True))
        add_sums(s, 0, sums)
        back = norm_back(grad, unit, inv1[s, :, 0:1], gains[0:1, :])
        n1[s] = back
        ag3[s, t] = back.astype(BF16)
        ag_start(2, ag3, s)

    def weight_grad(dest, left_of, right):
        def tile(i, carry):
            columns = pl.ds(pl.multiple_of(i * 128, 128), 128)
            dest[columns, :] = mm(left_of(columns), right, TN).astype(BF16)
            return carry

        lax.fori_loop(0, D // 128, tile, 0)

    def reduce_start(slot, source, landing):
        for d in range(1, NF):
            reduce_copy(slot, source, landing, d).start()

    def reduce_copy(slot, source, landing, d):
        to = (z + d) % NF
        return remote(
            source.at[own_rows(to), :], landing.at[d - 1],
            gr_ss.at[slot, d - 1], gr_rs.at[slot, d - 1], "fsdp", to,
        )

    def reduce_middle(slot, source, landing, crossing):
        for d in range(1, NF):
            reduce_copy(slot, source, landing, d).wait_recv()
        total = source[own_rows(z), :].astype(F32)
        for d in range(1, NF):
            total = total + landing[d - 1].astype(F32)
        source[own_rows(z), :] = total.astype(BF16)
        for d in range(1, NC):
            cross_copy(slot, source, crossing, d).start()
        own_copy(slot, source).start()

    def cross_copy(slot, source, crossing, d):
        return remote(
            source.at[own_rows(z), :], crossing.at[d - 1],
            x_ss.at[slot, d - 1], x_rs.at[slot, d - 1], "context", (x + d) % NC,
        )

    def own_copy(slot, source):
        return pltpu.make_async_copy(
            source.at[own_rows(z), :], own_out[slot], own_sem.at[slot]
        )

    def reduce_finish(slot, source, landing, crossing):
        for d in range(1, NC):
            cross_copy(slot, source, crossing, d).wait()
        own_copy(slot, source).wait()
        for d in range(1, NF):
            reduce_copy(slot, source, landing, d).wait_send()

    def moment_copy(k):
        return remote(
            sends[k], lands[k], m_ss.at[k], m_rs.at[k], "context", (x + 1) % NC
        )

    def moment_send(k):
        for i in range(2):
            moment_load(k, i).wait()
            if k == 2:
                for j in range(2):
                    sends[k][i, :, j * F : (j + 1) * F] = stages[k][i, :, j, :].astype(BF16)
            else:
                sends[k][i] = stages[k][i].astype(BF16)
        moment_copy(k).start()

    def norm_copy(buffer, axis, me, count, base, d):
        return remote(
            buffer.at[me], buffer.at[me], n_ss.at[base + d - 1], n_rs.at[base + d - 1],
            axis, (me + d) % count,
        )

    norm_levels = (
        (nsum_t, "tensor", t, NT4, 0),
        (nsum_c, "context", x, NC, NT4 - 1),
        (nsum_f, "fsdp", z, NF, NT4 - 1 + NC - 1),
    )

    def norm_start(level):
        for d in range(1, norm_levels[level][3]):
            norm_copy(*norm_levels[level], d).start()

    def norm_total(level):
        buffer, count = norm_levels[level][0], norm_levels[level][3]
        for d in range(1, count):
            norm_copy(*norm_levels[level], d).wait_recv()
        total = buffer[0]
        for i in range(1, count):
            total = total + buffer[i]
        return total

    def attended_back(s):
        def tile(i, carry):
            rows = pl.ds(pl.multiple_of(i * TS, TS), TS)
            datt[s, rows, :] = mm(ag3[s, i], wo[...], NN).astype(BF16)
            return carry

        lax.fori_loop(0, NT4, tile, 0)
        both = datt[s].astype(F32) * att[s].astype(F32)
        head_row = lax.broadcasted_iota(jnp.int32, (8, 256), 0)
        lane = lax.broadcasted_iota(jnp.int32, (8, 256), 1)
        chooser = (lane // HD == head_row + 1).astype(F32)
        dlt[s] = lax.dot_general(
            chooser, both, NT, precision=lax.Precision.HIGHEST, preferred_element_type=F32
        )

    def kvg_copy(s, d):
        return remote(
            kvg_s.at[(d - 1) % KS, s], kvg_r.at[d - 1, s],
            kvg_ss.at[d - 1, s], kvg_rs.at[d - 1, s], "context", (x + NC - d) % NC,
        )

    def attend_back(s):
        dqt[...] = jnp.zeros(dqt.shape, F32)

        def block(d):
            j = (x + NC - d) % NC
            doc_bias(j, s)
            vt[...] = mm(eye256, kv[j, s, :, 0:256], NT).astype(BF16)
            dk[...] = jnp.zeros(dk.shape, F32)
            dv[...] = jnp.zeros(dv.shape, F32)

            def head(h, inner):
                key_mask, value_mask = head_mask(h, 0), head_mask(h, HD)
                keys = keep(kv[j, s, :, 0:256], key_mask)
                row = pl.ds(h, 1)
                scores = mm(keys, q_ref[s], NT) * scale + bias_ref[...]
                probs = jnp.exp(scores - tot[s, row, :])
                dv[...] += mm(probs.astype(BF16), keep(datt[s], value_mask), NN)
                grad_probs = mm(keep(kv[j, s, :, 128:384], value_mask), datt[s], NT)
                grads = (probs * (grad_probs - dlt[s, row, :])).astype(BF16)
                dk[...] += mm(grads, keep(q_ref[s], key_mask), NN)
                rows = pl.ds(pl.multiple_of(h * HD, HD), HD)
                dqt[rows, :] += mm(vt[rows, :], grads, NN)
                return inner

            lax.fori_loop(0, H, head, 0)
            first = dk[:, 0:128] * scale
            second = dk[:, 128:256] * scale + dv[:, 0:128]
            return first, second, dv[:, 128:256]

        def far(d, carry):
            parts = block(d)
            if NC - 1 > KS:

                @pl.when(d > KS)
                def _():
                    kvg_copy(s, d - KS).wait_send()

            for k in range(3):
                kvg_s[(d - 1) % KS, s, :, k * 128 : (k + 1) * 128] = parts[k].astype(BF16)
            kvg_copy(s, d).start()
            return carry

        if NC > 1:
            lax.fori_loop(1, NC, far, 0)
        parts = block(0)
        for k in range(3):
            kv_own[s, :, k * 128 : (k + 1) * 128] = parts[k].astype(BF16)
        grad = jnp.transpose(dqt[...]) * scale
        q0, q1 = rotate_pair(grad, slice(0, T), -1.0)
        qb[s, :, 0:128] = q0.astype(BF16)
        qb[s, :, 128:256] = q1.astype(BF16)

    def keys_back(s):
        for d in range(1, NC):
            kvg_copy(s, d).wait_recv()

        def column(k):
            cols = slice(k * 128, (k + 1) * 128)
            total = kv_own[s, :, cols].astype(F32)
            for d in range(1, NC):
                total = total + kvg_r[d - 1, s, :, cols].astype(F32)
            return total

        k0, k1 = rotate_pair(
            jnp.concatenate([column(0), column(1)], axis=1), slice(0, T), -1.0
        )
        qb[s, :, QW : QW + 128] = k0.astype(BF16)
        qb[s, :, QW + 128 : QW + 256] = k1.astype(BF16)
        qb[s, :, QW + 256 : QW + 384] = column(2).astype(BF16)

    def input_product(s, rows):
        return mm(qb[s, rows, :], wq[...], NT)

    def input_out(s):
        n1[s] = n1[s] + rs_finish(3, s)
        input_copy(s).start()

    def input_copy(s):
        return pltpu.make_async_copy(n1.at[s], input_grad.at[s], loc_sem.at[1 + s])

    seqs = range(S)
    R = S * T

    for s in seqs:
        project(s)
    if adam:
        for k in (2, 0, 3, 1):
            moment_send(k)
    wait_recv(wo_copies)
    wg_copies = gather(wg, 2)
    wd_copies = gather(wd, 3)
    for s in seqs:
        attend(s)
        if s > 0:
            rs_middle(0, s - 1)
        rs_produce(0, s, out_product)
        if s > 0:
            first_norm(s - 1)
    rs_middle(0, S - 1)
    first_norm(S - 1)
    wait_recv(wg_copies)
    for s in seqs:
        ag_middle(0, ag1, s)
    for s in seqs:
        ag_finish(0, ag1, s)
        gate_up(s)
        if s == 0:
            wait_recv(wd_copies)
        rs_produce(1, s, down_product)
        if s > 0:
            rs_middle(1, s - 1)
    rs_middle(1, S - 1)
    cot_copy.wait()
    nsum_t[t] = jnp.zeros(nsum_t.shape[1:], F32)
    for s in seqs:
        second_norm(s)
    for s in seqs:
        ag_middle(1, ag2, s)
    for s in seqs:
        ag_finish(1, ag2, s)
        hidden_back(s)
        rs_produce(2, s, gate_product)
        if s > 0:
            rs_middle(2, s - 1)
    rs_middle(2, S - 1)
    flat_hid = hid[...].reshape(R, F)
    weight_grad(gsd, lambda c: ag2[:, :, :, c].reshape(R, 128), flat_hid)
    reduce_start(3, gsd, grd)
    for s in seqs:
        first_norm_back(s)
    norm_start(0)
    weight_grad(gsg, lambda c: ag1[:, :, :, c].reshape(R, 128), gb[...].reshape(R, 2 * F))
    reduce_start(2, gsg, grg)
    for s in seqs:
        ag_middle(2, ag3, s)
    for s in seqs:
        ag_finish(2, ag3, s)
        attended_back(s)
        if s == 0:
            nsum_c[x] = norm_total(0)
            norm_start(1)
        attend_back(s)
    nsum_f[z] = norm_total(1)
    norm_start(2)
    weight_grad(gso, lambda c: ag3[:, :, :, c].reshape(R, 128), att[...].reshape(R, 256))
    reduce_start(1, gso, gro)
    for s in seqs:
        keys_back(s)
        rs_produce(3, s, input_product)
        if s > 0:
            rs_middle(3, s - 1)
    rs_middle(3, S - 1)
    weight_grad(gsq, lambda c: tok[:, :, c].reshape(R, 128), qb[...].reshape(R, QW + KW))
    reduce_start(0, gsq, grq)
    norm_out[...] = norm_total(2)
    reduce_middle(3, gsd, grd, xd)
    reduce_middle(2, gsg, grg, xg)
    reduce_middle(1, gso, gro, xo)
    for s in seqs:
        input_out(s)
    reduce_middle(0, gsq, grq, xq)
    reduce_finish(3, gsd, grd, xd)
    reduce_finish(2, gsg, grg, xg)
    reduce_finish(1, gso, gro, xo)
    reduce_finish(0, gsq, grq, xq)

    for s in seqs:
        input_copy(s).wait()
    for copies in (wq_copies, wo_copies, wg_copies, wd_copies, id_copies):
        wait_send(copies)
    for s in seqs:
        for d in range(1, NC):
            kv_copy(s, d).wait_send()
            if d > NC - 1 - KS:
                kvg_copy(s, d).wait_send()
        for part in range(3):
            rs_copy(3, s, part).wait_send()
        for rnd, buffer in ((0, ag1), (1, ag2), (2, ag3)):
            for part in range(3):
                ag_copy(rnd, buffer, s, part).wait_send()
    for level in range(3):
        for d in range(1, norm_levels[level][3]):
            norm_copy(*norm_levels[level], d).wait_send()
    if adam:
        for k in range(4):
            moment_copy(k).wait()


def finish_kernel(dims, *refs):
    S, T, D, C, F, NF, NC, NT4 = dims
    DB, QW = D // NF, 256
    refs = list(refs)

    def take(count):
        taken, refs[:] = refs[:count], refs[count:]
        return taken

    owner, norm_sums, norm_m, norm_v = take(4)
    layer_in, input_in = take(2)
    own_in, cross_in, masters_in, moments_in, lands_in = take(4), take(4), take(4), take(8), take(4)
    layer_out, input_out = take(2)
    grads_out, states_out = take(4), take(4)
    norm_out, norm_state, norm_flat, updates = take(4)
    layer_v, input_v = take(2)
    own_g, cross_g, masters, lands = take(4), take(4), take(4), take(4)
    states, grads, flats = take(4), take(4), take(4)
    row_a, row_b, in_sem, out_sem, pass_sem = take(5)
    z, x, t = lax.axis_index("fsdp"), lax.axis_index("context"), lax.axis_index("tensor")
    order = (2, 3, 1, 0)

    def loads(k):
        pairs = [
            (own_in[k], own_g[k]), (cross_in[k], cross_g[k]), (masters_in[k], masters[k]),
            (lands_in[k], lands[k]),
            (moments_in[2 * k].at[0], states[k].at[0]),
            (moments_in[2 * k + 1].at[0], states[k].at[1]),
        ]
        return [
            pltpu.make_async_copy(src, dst, in_sem.at[k, i]) for i, (src, dst) in enumerate(pairs)
        ]

    def passing(k, stage):
        src, mid, dst = ((layer_in, layer_v, layer_out), (input_in, input_v, input_out))[k]
        if stage == 0:
            return pltpu.make_async_copy(src, mid, pass_sem.at[k, 0])
        return pltpu.make_async_copy(mid, dst, pass_sem.at[k, 1])

    for k in order:
        for c in loads(k):
            c.start()
    for k in range(2):
        passing(k, 0).start()

    def adam_parts(g, m, v, w, decay):
        m_new = BETA_ONE * m + (1.0 - BETA_ONE) * g
        v_new = BETA_TWO * v + (1.0 - BETA_TWO) * g * g
        corrected = m_new / (1.0 - BETA_ONE**ADAM_STEP)
        scaled = v_new / (1.0 - BETA_TWO**ADAM_STEP)
        step = corrected / (jnp.sqrt(scaled) + ADAM_EPS)
        if decay:
            step = step + decay * w
        return m_new, v_new, -RATE * step

    def rows_to_flat(flat, count, width):
        block = math.lcm(width, 128)
        period, lines = block // width, block // 128
        many = count // period
        halves = (row_a, row_b)
        for line in range(lines):
            parts, at = [], line * 128
            while at < (line + 1) * 128:
                row, column = divmod(at, width)
                half, lane = divmod(column, 128)
                length = min((line + 1) * 128 - at, width - column, 128 - lane)
                rows = halves[half][pl.ds(row, many, stride=period), :]
                parts.append(rows[:, lane : lane + length])
                at += length
            whole = parts[0] if len(parts) == 1 else jnp.concatenate(parts, axis=1)
            flat[pl.ds(line, many, stride=lines), :] = whole

    def to_rows(values, rows):
        width = values.shape[1]
        for half, place in enumerate((row_a, row_b)):
            part = values[:, half * 128 : min(width, (half + 1) * 128)]
            if part.shape[1] == 0:
                continue
            if part.shape[1] < 128:
                rest = jnp.zeros((part.shape[0], 128 - part.shape[1]), F32)
                part = jnp.concatenate([part, rest], axis=1)
            place[rows, :] = part

    sizes = (DB * 3 * C, C * DB, DB * 2 * F, F * DB)

    def out_copies(k):
        first = sum(sizes[:k])
        return (
            pltpu.make_async_copy(grads[k], grads_out[k], out_sem.at[k, 0]),
            pltpu.make_async_copy(states[k], states_out[k], out_sem.at[k, 1]),
            pltpu.make_async_copy(
                flats[k].reshape(1, sizes[k]),
                updates.at[0, :, pl.ds(first, sizes[k])],
                out_sem.at[k, 2],
            ),
        )

    for k in order:
        for c in loads(k):
            c.wait()
        own = own_g[k][...].astype(F32)
        if NC == 2:
            total = own + cross_g[k][0].astype(F32)
        else:
            total = jnp.zeros_like(own)
            for i in range(NC):
                other = cross_g[k][jnp.maximum((x - i + NC) % NC, 1) - 1].astype(F32)
                total = total + jnp.where(x == i, own, other)
        if k == 0:
            parts = [total[:, 0:C], total[:, QW : QW + C], total[:, QW + C : QW + 2 * C]]
        elif k == 1:
            parts = [jnp.transpose(total)[HD : HD + C, :]]
        elif k == 2:
            parts = [total[:, 0:F], total[:, F : 2 * F]]
        else:
            parts = [total]
        mine = owner[0:1, k : k + 1] == x
        for j, g in enumerate(parts):
            at = (j,) if k == 0 else (slice(None), j) if k == 2 else (slice(None),)
            land_at = (slice(None), slice(j * F, (j + 1) * F)) if k == 2 else at
            grads[k][at] = g
            kept = [
                jnp.where(
                    mine, states[k][(i, *at)].astype(BF16).astype(F32),
                    lands[k][(i, *land_at)].astype(F32),
                )
                for i in range(2)
            ]
            m_new, v_new, step = adam_parts(g, *kept, masters[k][at], DECAY)
            states[k][(0, *at)] = m_new
            states[k][(1, *at)] = v_new
            if k == 0:
                to_rows(step, pl.ds(j, DB, stride=3))
            elif k == 1:
                to_rows(step, pl.ds(0, C))
            elif k == 2:
                for c in range(F // 128):
                    flats[2][pl.ds(j * (F // 128) + c, DB, stride=2 * F // 128), :] = step[
                        :, c * 128 : (c + 1) * 128
                    ]
            else:
                to_rows(jnp.transpose(step), pl.ds(0, F))
        if k != 2:
            rows_to_flat(flats[k], (3 * DB, C, 0, F)[k], (C, DB, 0, DB)[k])
        for c in out_copies(k):
            c.start()
        if k == 2:
            for i in range(2):
                passing(i, 0).wait()
                passing(i, 1).start()

    g = norm_sums[0:4, :]
    m_new, v_new, step = adam_parts(g, norm_m[...], norm_v[...], None, 0.0)
    norm_out[...] = g
    norm_state[0] = m_new
    norm_state[1] = v_new
    count = 4 * D // (NF * NT4)
    per_row = D // count
    place = z * NT4 + t
    row = lax.broadcasted_iota(jnp.int32, (4, count), 0)
    chosen = jnp.zeros((4, count), F32)
    for c in range(per_row):
        hit = row * per_row + c == place
        chosen = chosen + jnp.where(hit, step[:, c * count : (c + 1) * count], 0.0)
    norm_flat[...] = jnp.sum(chosen, axis=0, keepdims=True)
    for k in order:
        for c in out_copies(k):
            c.wait()
    for k in range(2):
        passing(k, 1).wait()


def run_layer(
    tokens, cotangent, segment_ids, owner, weights, norm_gains, norm_biases, moments,
    norm_moments, cosine, sine_rows,
):
    S, T, D = tokens.shape
    C, F = weights[0].shape[2], weights[2].shape[2]
    NF, NC, NT4 = lax.axis_size("fsdp"), lax.axis_size("context"), lax.axis_size("tensor")
    TS, DB, KW, W = T // NT4, D // NF, 384, 640
    adam = NC == 2
    assert NT4 == 4 and C == 192
    vmem = pl.BlockSpec(memory_space=pltpu.VMEM)
    far = pl.BlockSpec(memory_space=pl.ANY)
    VM = pltpu.VMEM
    DMA = pltpu.SemaphoreType.DMA
    NX = max(NC - 1, 1)
    scratch = [
        VM((D, W), BF16), VM((D, 256), BF16), VM((D, 2 * F), BF16), VM((D, F), BF16),
        VM((NC, S, T), jnp.int32), VM((S, T, 256), BF16), VM((NC, S, T, KW), BF16),
        VM((S, T, 256), BF16), VM((S, 8, T), F32), VM((8, T), F32), VM((8, T), F32),
        VM((256, T), F32), VM((T, T), F32), VM((256, T), BF16),
        VM((S, 2, 2, TS, D), BF16), VM((S, 2, TS, D), BF16), VM((S, TS, D), BF16), VM((S, TS, D), BF16),
        VM((S, 4, TS, D), BF16), VM((S, 4, TS, D), BF16), VM((S, 4, TS, D), BF16),
        VM((S, T, F), BF16), VM((S, T, 2 * F), BF16),
        VM((S, TS, D), F32), VM((S, TS, D), F32), VM((S, TS, 128), F32),
        VM((S, T, 256), BF16), VM((S, 8, T), F32),
        VM((T, 256), F32), VM((T, 256), F32), VM((min(NX, 2), S, T, KW), BF16), VM((NX, S, T, KW), BF16),
        VM((S, T, KW), BF16), VM((S, T, W), BF16),
        VM((D, W), BF16), VM((D, 256), BF16), VM((D, 2 * F), BF16), VM((D, F), BF16),
        VM((NF - 1, DB, W), BF16), VM((NF - 1, DB, 256), BF16), VM((NF - 1, DB, 2 * F), BF16),
        VM((NF - 1, DB, F), BF16),
        VM((NT4, 8, D), F32), VM((NC, 8, D), F32), VM((NF, 8, D), F32), VM((S, TS, D), BF16),
        DMA((4, NF - 1)), DMA((4, NF - 1)), DMA((S, NX)), DMA((S, NX)), DMA((NX,)), DMA((NX,)),
        DMA((4, S, 3)), DMA((4, S, 3)), DMA((3, S, 3)), DMA((3, S, 3)),
        DMA((NX, S)), DMA((NX, S)), DMA((4, NF - 1)), DMA((4, NF - 1)), DMA((4, NX)), DMA((4, NX)),
        DMA((NT4 + NC + NF,)), DMA((NT4 + NC + NF,)), DMA((1 + S,)), DMA((4,)),
    ]
    shapes = ((3, DB, C), (C, DB), (DB, 2, F), (DB, F))
    flat_shapes = ((DB, W), (DB, 256), (DB, 2 * F), (DB, F))
    low_shapes = ((2, 3, DB, C), (2, C, DB), (2, DB, 2 * F), (2, DB, F))
    dims = (S, T, D, C, F, NF, NC, NT4)
    outs = [
        jax.ShapeDtypeStruct((S, TS, D), BF16),
        jax.ShapeDtypeStruct((S, TS, D), F32),
        *(jax.ShapeDtypeStruct(shape, BF16) for shape in flat_shapes),
        *(jax.ShapeDtypeStruct((NX, *shape), BF16) for shape in flat_shapes),
        jax.ShapeDtypeStruct((8, D), F32),
    ]
    out_specs = [vmem] + [far] * 9 + [vmem]
    args = [
        tokens, cotangent, segment_ids, *weights, norm_gains, norm_biases, cosine, sine_rows,
    ]
    in_specs = [vmem, far] + [vmem] * 9
    flat_moments = [m for pair in moments for m in pair]
    if adam:
        outs += [jax.ShapeDtypeStruct(shape, BF16) for shape in low_shapes]
        out_specs += [far] * 4
        args += flat_moments
        in_specs += [far] * 8
        scratch += [VM((2, *shape), F32) for shape in shapes]
        scratch += [VM(shape, BF16) for shape in low_shapes]
        scratch += [DMA((4,)), DMA((4,)), DMA((4, 2))]
    results = pl.pallas_call(
        functools.partial(layer_kernel, dims),
        out_shape=outs,
        in_specs=in_specs,
        out_specs=out_specs,
        scratch_shapes=scratch,
        compiler_params=pltpu.CompilerParams(
            collective_id=0, has_side_effects=True, vmem_limit_bytes=67043328
        ),
        name="layer",
    )(*args)
    layer_out, input_grad = results[:2]
    own_grads, cross_grads, norm_sums = results[2:6], results[6:10], results[10]
    if adam:
        lands = results[11:]
    else:
        lands = []
        for k in range(4):
            pair = jnp.concatenate(moments[k], axis=0).astype(BF16).reshape(low_shapes[k])
            lands.append(from_root(pair, "context", owner[k]))
        owner = jnp.full_like(owner, -1)

    total = sum(math.prod(shape) for shape in shapes)
    count = 4 * D // (NF * NT4)
    out_shape = [
        jax.ShapeDtypeStruct((S, TS, D), BF16),
        jax.ShapeDtypeStruct((S, TS, D), F32),
        *(jax.ShapeDtypeStruct(shape, F32) for shape in shapes),
        *(jax.ShapeDtypeStruct((2, *shape), F32) for shape in shapes),
        jax.ShapeDtypeStruct((4, D), F32),
        jax.ShapeDtypeStruct((2, 4, D), F32),
        jax.ShapeDtypeStruct((1, count), F32),
        jax.ShapeDtypeStruct((1, 1, total + count), F32),
    ]
    rows = max(3 * DB, F)
    return pl.pallas_call(
        functools.partial(finish_kernel, dims),
        out_shape=out_shape,
        in_specs=[vmem] * 4 + [far] * 26,
        out_specs=[far] * 10 + [vmem] * 3 + [far],
        scratch_shapes=[
            VM((S, TS, D), BF16), VM((S, TS, D), F32),
            *(VM(shape, BF16) for shape in flat_shapes),
            *(VM((NX, *shape), BF16) for shape in flat_shapes),
            *(VM(shape, F32) for shape in shapes),
            *(VM(shape, BF16) for shape in low_shapes),
            *(VM((2, *shape), F32) for shape in shapes),
            *(VM(shape, F32) for shape in shapes),
            *(VM((math.prod(shape) // 128, 128), F32) for shape in shapes),
            VM((rows, 128), F32), VM((rows, 128), F32),
            DMA((4, 6)), DMA((4, 3)), DMA((2, 2)),
        ],
        compiler_params=pltpu.CompilerParams(vmem_limit_bytes=67043328),
        name="finish",
    )(
        owner.reshape(1, 4), norm_sums, *norm_moments, layer_out, input_grad, *own_grads,
        *cross_grads, *weights, *flat_moments, *lands,
    )


def from_root(block, axis, owner):
    block = jnp.where(lax.axis_index(axis) == owner, block, jnp.zeros_like(block))
    return lax.psum(block, axis)


def shards(
    tokens, cotangent, segment_ids, owner, qkv_weight, out_weight, gate_up_weight, down_weight,
    norm_gains, norm_biases, qkv_moment, qkv_square, out_moment, out_square, gate_moment,
    gate_square, down_moment, down_square, norm_moment, norm_square,
):
    tok_here = tokens.shape[1]
    moments = (
        (qkv_moment, qkv_square), (out_moment, out_square),
        (gate_moment, gate_square), (down_moment, down_square),
    )
    positions = (
        lax.axis_index("context") * tok_here + jnp.arange(tok_here, dtype=jnp.int32)
    ).astype(F32)
    frequency = jnp.power(F32(ROPE_BASE), -jnp.arange(0, HD, 2, dtype=F32) / HD)
    angles = positions[:, None] * frequency[None, :]
    cosine, sine_rows = jnp.cos(angles), jnp.sin(angles)
    cosine = jnp.concatenate([cosine] * 4, axis=1)
    sine_rows = jnp.concatenate([-sine_rows, sine_rows] * 2, axis=1)

    columns_last = (0, 2, 1, 3)
    weights = (
        jnp.transpose(qkv_weight, (1, 0, 2)), out_weight, gate_up_weight, jnp.transpose(down_weight),
    )
    turned = (
        [jnp.transpose(m, columns_last) for m in moments[0]],
        moments[1],
        moments[2],
        [jnp.transpose(m, (0, 2, 1)) for m in moments[3]],
    )
    results = run_layer(
        tokens, cotangent, segment_ids, owner, weights, norm_gains, norm_biases, turned,
        (norm_moment, norm_square), cosine, sine_rows,
    )
    layer_out, input_grad, grad_q, grad_o, grad_g, grad_d = results[:6]
    state_q, state_o, state_g, state_d = results[6:10]
    norm_grad, norm_state, piece, weight_updates = results[10:]
    weight_updates = lax.dynamic_update_slice(
        weight_updates, piece[None], (0, 0, weight_updates.shape[2] - piece.shape[1])
    )
    return (
        layer_out, input_grad,
        jnp.transpose(grad_q, (1, 0, 2)), grad_o, grad_g, jnp.transpose(grad_d),
        norm_grad,
        jnp.transpose(state_q, columns_last), state_o, state_g, jnp.transpose(state_d, (0, 2, 1)),
        norm_state, weight_updates,
    )


def solution(mesh):
    return jax.shard_map(
        shards,
        mesh=mesh,
        in_specs=(
            P("fsdp", "context", None),
            P("fsdp", "context", None),
            P("fsdp", "context"),
            P(),
            P("fsdp", None, "tensor"),
            P("tensor", "fsdp"),
            P("fsdp", None, "tensor"),
            P("tensor", "fsdp"),
            P(),
            P(),
            P("context", "fsdp", None, "tensor"),
            P("context", "fsdp", None, "tensor"),
            P("context", "tensor", "fsdp"),
            P("context", "tensor", "fsdp"),
            P("context", "fsdp", None, "tensor"),
            P("context", "fsdp", None, "tensor"),
            P("context", "tensor", "fsdp"),
            P("context", "tensor", "fsdp"),
            P(),
            P(),
        ),
        out_specs=(
            P("fsdp", ("context", "tensor"), None),
            P("fsdp", ("context", "tensor"), None),
            P("fsdp", None, "tensor"),
            P("tensor", "fsdp"),
            P("fsdp", None, "tensor"),
            P("tensor", "fsdp"),
            P(),
            P(None, "fsdp", None, "tensor"),
            P(None, "tensor", "fsdp"),
            P(None, "fsdp", None, "tensor"),
            P(None, "tensor", "fsdp"),
            P(),
            P("fsdp", "tensor", None),
        ),
        check_vma=False,
    )
```

```python
import functools
import math

import jax
import jax.numpy as jnp
from jax import lax
from jax.experimental import pallas as pl
from jax.experimental.pallas import tpu as pltpu
from jax.sharding import PartitionSpec as P

HD = 64

NEGATIVE = -1e30
EPSILON = 1e-05
ROPE_BASE = 1000.0
BETA_ONE = 0.9
BETA_TWO = 0.999
ADAM_EPS = 1e-08
ADAM_STEP = 3.0
RATE = 0.03
DECAY = 0.1

F32 = jnp.float32
BF16 = jnp.bfloat16
MESH = pl.DeviceIdType.MESH
NN = (((1,), (0,)), ((), ()))
NT = (((1,), (1,)), ((), ()))
TN = (((0,), (0,)), ((), ()))


def mm(left, right, dims):
    return lax.dot_general(left, right, dims, preferred_element_type=F32)


def swap_halves(values):
    lane = lax.broadcasted_iota(jnp.int32, values.shape, 1)
    low_half = lane % HD < HD // 2
    return jnp.where(
        low_half,
        pltpu.roll(values, 128 - HD // 2, 1),
        pltpu.roll(values, HD // 2, 1),
    )


def mean_of(values):
    return jnp.sum(values, axis=-1, keepdims=True) * (1.0 / values.shape[-1])


def normalize(values, gain_row, bias_row):
    center = values - mean_of(values)
    inverse_std = lax.rsqrt(mean_of(center * center) + EPSILON)
    unit = center * inverse_std
    return unit * gain_row + bias_row, unit, inverse_std


def norm_back(gradient, unit, inverse_std, gain_row):
    scaled = gradient * gain_row
    return inverse_std * (scaled - mean_of(scaled) - unit * mean_of(scaled * unit))


class Pack:
    pass


def layer_kernel(dims, *refs):
    S, T, D, C, F, NF, NC, NT4 = dims
    TS = T // NT4
    DB = D // NF
    adam = NC == 2
    pair = NC == 2
    HB = DB // 2
    refs = list(refs)
    QW, KW = 256, 384
    H = C // HD
    KS = min(max(NC - 1, 1), 2)
    scale = HD ** (-0.5)
    def take(count):
        taken, refs[:] = refs[:count], refs[count:]
        return taken

    tok, cot, ids_in, wq_in, wo_in, wg_in, wd_in, gains, biases, cos_t, sin_t = take(11)
    if adam:
        moments = take(8)
    layer_out, input_grad = take(2)
    own_out, crosses = take(5), take(5)
    norm_out = take(1)[0]
    if adam:
        lands = take(4)
    wq, wo, wg, wd, ids_all, q_ref, kv, att, tot, am, al, acc, bias_ref, vt = take(14)
    rsend, rsb, rs2, rs2r, ag1, ag2, ag3, hid, gb = take(9)
    n1, unit1, inv1, datt, dlt, dk, dv, kvg_s, kvg_r, kv_own, qb = take(11)
    dqt = acc
    sources, landings, meets = take(5), take(5), take(2)
    nsum_t, nsum_c, nsum_f, cot_v = take(4)
    w_ss, w_rs, kv_ss, kv_rs, id_ss, id_rs, rs_ss, rs_rs, ag_ss, ag_rs = take(10)
    kvg_ss, kvg_rs, gr_ss, gr_rs, x_ss, x_rs, n_ss, n_rs, loc_sem = take(9)
    own_sem, f_ss, f_rs, h_ss, h_rs, l_ss, l_rs = take(7)
    if adam:
        stages, sends = take(4), take(4)
        m_ss, m_rs, in_sem = take(3)

    z, x, t = lax.axis_index("fsdp"), lax.axis_index("context"), lax.axis_index("tensor")
    core, yy = t % 2, t // 2
    t_core = yy * 2 + (1 - core)
    t_y = (1 - yy) * 2 + core
    t_diag = (1 - yy) * 2 + (1 - core)

    def remote(src, dst, ssem, rsem, axis, index):
        return pltpu.make_async_remote_copy(
            src_ref=src, dst_ref=dst, send_sem=ssem, recv_sem=rsem,
            device_id={axis: index}, device_id_type=MESH,
        )

    barrier = pltpu.get_barrier_semaphore()
    for d in range(1, NF):
        pl.semaphore_signal(barrier, inc=1, device_id={"fsdp": (z + d) % NF}, device_id_type=MESH)
    for d in range(1, NC):
        pl.semaphore_signal(barrier, inc=1, device_id={"context": (x + d) % NC}, device_id_type=MESH)
    for d in range(1, NT4):
        pl.semaphore_signal(barrier, inc=1, device_id={"tensor": (t + d) % NT4}, device_id_type=MESH)

    def moment_load(k, i):
        return pltpu.make_async_copy(
            moments[2 * k + i].at[0], stages[k].at[i], in_sem.at[k, i]
        )

    cot_copy = pltpu.make_async_copy(
        cot.at[:, pl.ds(pl.multiple_of(t * TS, TS), TS), :], cot_v, loc_sem.at[0]
    )
    cot_copy.start()
    if adam:
        for k in range(4):
            for i in range(2):
                moment_load(k, i).start()

    def own_rows(index):
        return pl.ds(pl.multiple_of(index * DB, DB), DB)

    def pad_cols(values, left, right):
        parts = []
        if left:
            parts.append(jnp.zeros((values.shape[0], left), values.dtype))
        parts.append(values)
        if right:
            parts.append(jnp.zeros((values.shape[0], right), values.dtype))
        return jnp.concatenate(parts, axis=1)

    wq[own_rows(z), :] = jnp.concatenate(
        [
            pad_cols(wq_in[0], 0, QW - C),
            jnp.concatenate([wq_in[1], wq_in[2]], axis=1),
        ],
        axis=1,
    ).astype(BF16)

    pl.semaphore_wait(barrier, NF - 1 + NC - 1 + NT4 - 1)

    def half_rows(block, half):
        return pl.ds(pl.multiple_of(block * DB + half * HB, HB), HB)

    def fetch_copy(buffer, slot, d):
        rows = half_rows(z, x) if pair else own_rows(z)
        return remote(
            buffer.at[rows, :], buffer.at[rows, :],
            w_ss.at[slot, d - 1], w_rs.at[slot, d - 1], "fsdp", (z + d) % NF,
        )

    def hand_copy(buffer, slot, d):
        rows = half_rows((z + NF - d) % NF, x)
        return remote(
            buffer.at[rows, :], buffer.at[rows, :],
            f_ss.at[slot, d - 1], f_rs.at[slot, d - 1], "context", 1 - x,
        )

    def gather_start(slot):
        for d in range(1, NF):
            fetch_copy(gathered[slot], slot, d).start()

    def gather_hand(slot):
        for d in range(1, NF):
            fetch_copy(gathered[slot], slot, d).wait_recv()
            if pair:
                hand_copy(gathered[slot], slot, d).start()

    def gather_finish(slot):
        if pair:
            for d in range(1, NF):
                hand_copy(gathered[slot], slot, d).wait_recv()

    gathered = (wq, wo, wg, wd)

    def wait_recv(copies):
        for c in copies:
            c.wait_recv()

    def wait_send(copies):
        for c in copies:
            c.wait_send()

    gather_start(0)

    ids_all[x] = ids_in[...]
    id_copies = []
    for d in range(1, NC):
        c = remote(
            ids_all.at[x], ids_all.at[x], id_ss.at[d - 1], id_rs.at[d - 1],
            "context", (x + d) % NC,
        )
        c.start()
        id_copies.append(c)

    def eye(n):
        return (
            lax.broadcasted_iota(jnp.int32, (n, n), 0)
            == lax.broadcasted_iota(jnp.int32, (n, n), 1)
        ).astype(F32).astype(BF16)

    wo_t = jnp.transpose(wo_in[...])
    wo[own_rows(z), :] = pad_cols(wo_t, HD, 0).astype(BF16)
    wd[own_rows(z), :] = wd_in[...].astype(BF16)
    wg[own_rows(z), 0:F] = wg_in[:, 0, :].astype(BF16)
    wg[own_rows(z), F : 2 * F] = wg_in[:, 1, :].astype(BF16)

    gather_hand(0)
    gather_start(1)
    gather_start(2)
    gather_start(3)
    gather_finish(0)

    def rotate_pair(values, rows, sign):
        cosine, sine_rows = cos_t[rows, :], sin_t[rows, :] * sign
        lane = lax.broadcasted_iota(jnp.int32, cosine.shape, 1)
        head = lane < HD
        first, second = values[:, 0:128], values[:, 128:256]
        first = first * cosine + swap_halves(first) * sine_rows
        second = second * jnp.where(head, cosine, 1.0) + swap_halves(second) * jnp.where(
            head, sine_rows, 0.0
        )
        return first, second

    TR = min(256, T)

    def project(s):
        def tile(i, carry):
            rows = pl.ds(pl.multiple_of(i * TR, TR), TR)
            p = mm(tok[s, rows, :], wq[...], NN)
            q0, q1 = rotate_pair(p[:, 0:QW], rows, 1.0)
            q_ref[s, rows, 0:128] = q0.astype(BF16)
            q_ref[s, rows, 128:256] = q1.astype(BF16)
            k0, k1 = rotate_pair(p[:, QW : QW + 256], rows, 1.0)
            kv[x, s, rows, 0:128] = k0.astype(BF16)
            kv[x, s, rows, 128:256] = k1.astype(BF16)
            kv[x, s, rows, 256:384] = p[:, QW + 256 : QW + 384].astype(BF16)
            return carry

        lax.fori_loop(0, T // TR, tile, 0)
        for d in range(1, NC):
            kv_copy(s, d).start()

    def kv_copy(s, d):
        return remote(
            kv.at[x, s], kv.at[x, s], kv_ss.at[s, d - 1], kv_rs.at[s, d - 1],
            "context", (x + d) % NC,
        )

    def head_mask(h, offset):
        lane = lax.broadcasted_iota(jnp.int32, (1, 256), 1)
        return jnp.logical_and(lane >= offset + h * HD, lane < offset + (h + 1) * HD)

    def keep(values, mask):
        return jnp.where(mask, values, jnp.zeros_like(values))

    def doc_bias(j, s):
        key_ids = jnp.broadcast_to(ids_all[j, pl.ds(s, 1), :].astype(F32), (128, T))
        key_col = jnp.transpose(key_ids)[:, 0:1]
        query_row = ids_all[x, pl.ds(s, 1), :].astype(F32)
        bias_ref[...] = jnp.where(key_col == query_row, 0.0, NEGATIVE)

    eye256 = eye(256)

    def attend(s):
        am[...] = jnp.full(am.shape, NEGATIVE, F32)
        al[...] = jnp.zeros(al.shape, F32)
        acc[...] = jnp.zeros(acc.shape, F32)

        def block(d, carry):
            j = (x + NC - d) % NC
            doc_bias(j, s)
            vt[...] = mm(eye256, kv[j, s, :, 128:384], NT).astype(BF16)

            def head(h, inner):
                keys = keep(kv[j, s, :, 0:256], head_mask(h, 0))
                scores = mm(keys, q_ref[s], NT) * scale + bias_ref[...]
                row = pl.ds(h, 1)
                before = am[row, :]
                newest = jnp.maximum(before, jnp.max(scores, axis=0, keepdims=True))
                shrink = jnp.exp(before - newest)
                weights = jnp.exp(scores - newest)
                al[row, :] = al[row, :] * shrink + jnp.sum(weights, axis=0, keepdims=True)
                am[row, :] = newest
                rows = pl.ds(pl.multiple_of(h * HD, HD), HD)
                vrows = pl.ds(pl.multiple_of(HD + h * HD, HD), HD)
                acc[vrows, :] = acc[vrows, :] * shrink + mm(
                    vt[vrows, :], weights.astype(BF16), NN
                )
                return inner

            lax.fori_loop(0, H, head, 0)
            return carry

        block(0, 0)
        if NC > 1:
            for d in range(1, NC):
                kv_copy(s, d).wait_recv()
            if s == 0:
                wait_recv(id_copies)
            lax.fori_loop(1, NC, block, 0)
        for h in range(H):
            rows = slice(HD + h * HD, HD + (h + 1) * HD)
            acc[rows, :] = acc[rows, :] / al[h : h + 1, :]
        tot[s] = am[...] + jnp.log(jnp.maximum(al[...], 1e-37))
        att[s] = jnp.transpose(acc[...]).astype(BF16)

    def rs_copy(rnd, s, part):
        if part < 2:
            chip = 1 - yy if part == 0 else yy
            return remote(
                rsend.at[s, chip, 1 - core], rsb.at[s, chip],
                rs_ss.at[rnd, s, part], rs_rs.at[rnd, s, part], "tensor", t_core,
            )
        return remote(
            rs2.at[s], rs2r.at[s], rs_ss.at[rnd, s, 2], rs_rs.at[rnd, s, 2], "tensor", t_y
        )

    def rs_produce(rnd, s, product):
        if rnd > 0:
            for part in range(3):
                rs_copy(rnd - 1, s, part).wait_send()

        def tile(i, carry):
            chip = jnp.where(i < 2, 1 - yy, yy)
            other = jnp.where(i % 2 == 0, 1 - core, core)
            start = pl.multiple_of((chip * 2 + other) * TS, TS)
            rsend[s, chip, other] = product(s, pl.ds(start, TS)).astype(BF16)
            return carry

        lax.fori_loop(0, 2, tile, 0)
        rs_copy(rnd, s, 0).start()
        lax.fori_loop(2, 4, tile, 0)
        rs_copy(rnd, s, 1).start()

    def rs_middle(rnd, s):
        rs_copy(rnd, s, 0).wait_recv()
        rs2[s] = (
            rsend[s, 1 - yy, core].astype(F32) + rsb[s, 1 - yy].astype(F32)
        ).astype(BF16)
        rs_copy(rnd, s, 2).start()

    def rs_finish(rnd, s):
        rs_copy(rnd, s, 1).wait_recv()
        rs_copy(rnd, s, 2).wait_recv()
        return rsend[s, yy, core].astype(F32) + rsb[s, yy].astype(F32) + rs2r[s].astype(F32)

    def ag_copy(rnd, buffer, s, part):
        if part == 0:
            return remote(
                buffer.at[s, t], buffer.at[s, t],
                ag_ss.at[rnd, s, 0], ag_rs.at[rnd, s, 0], "tensor", t_core,
            )
        if part == 1:
            return remote(
                buffer.at[s, t], buffer.at[s, t],
                ag_ss.at[rnd, s, 1], ag_rs.at[rnd, s, 1], "tensor", t_y,
            )
        return remote(
            buffer.at[s, t_y], buffer.at[s, t_y],
            ag_ss.at[rnd, s, 2], ag_rs.at[rnd, s, 2], "tensor", t_core,
        )

    def ag_start(rnd, buffer, s):
        ag_copy(rnd, buffer, s, 1).start()
        ag_copy(rnd, buffer, s, 0).start()

    def ag_middle(rnd, buffer, s):
        ag_copy(rnd, buffer, s, 1).wait_recv()
        ag_copy(rnd, buffer, s, 2).start()

    def ag_finish(rnd, buffer, s):
        ag_copy(rnd, buffer, s, 0).wait_recv()
        ag_copy(rnd, buffer, s, 2).wait_recv()

    def out_product(s, rows):
        return mm(att[s, rows, :], wo[...], NT)

    def first_norm(s):
        share = pl.ds(pl.multiple_of(t * TS, TS), TS)
        values = tok[s, share, :].astype(F32) + rs_finish(0, s)
        normed, unit, inverse = normalize(values, gains[0:1, :], biases[0:1, :])
        n1[s] = normed
        unit1[s] = unit
        inv1[s] = jnp.broadcast_to(inverse, (TS, 128))
        ag1[s, t] = normed.astype(BF16)
        ag_start(0, ag1, s)

    def sigmoid(v):
        return 1.0 / (1.0 + jnp.exp(-v))

    def gate_up(s):
        def tile(i, carry):
            rows = pl.ds(pl.multiple_of(i * TS, TS), TS)
            both = mm(ag1[s, i], wg[...], NN)
            gate, up = both[:, 0:F], both[:, F : 2 * F]
            gb[s, rows, 0:F] = gate.astype(BF16)
            gb[s, rows, F : 2 * F] = up.astype(BF16)
            hid[s, rows, :] = (gate * sigmoid(gate) * up).astype(BF16)
            return carry

        lax.fori_loop(0, NT4, tile, 0)

    def down_product(s, rows):
        return mm(hid[s, rows, :], wd[...], NT)

    def second_norm(s):
        values = n1[s] + rs_finish(1, s)
        out, unit, inverse = normalize(values, gains[1:2, :], biases[1:2, :])
        layer_out[s] = out.astype(BF16)
        grad = cot_v[s].astype(F32)
        sums = (jnp.sum(grad * unit, axis=0, keepdims=True), jnp.sum(grad, axis=0, keepdims=True))
        add_sums(s, 1, sums)
        back = norm_back(grad, unit, inverse, gains[1:2, :])
        n1[s] = back
        ag2[s, t] = back.astype(BF16)
        ag_start(1, ag2, s)

    def add_sums(s, row, sums):
        for k in range(2):
            at = slice(row + 2 * k, row + 2 * k + 1)
            if s == 0:
                nsum_t[t, at, :] = sums[k]
            else:
                nsum_t[t, at, :] = nsum_t[t, at, :] + sums[k]

    def hidden_back(s):
        def tile(i, carry):
            rows = pl.ds(pl.multiple_of(i * TS, TS), TS)
            grad = mm(ag2[s, i], wd[...], NN)
            gate = gb[s, rows, 0:F].astype(F32)
            up = gb[s, rows, F : 2 * F].astype(F32)
            sig = sigmoid(gate)
            act = gate * sig
            gb[s, rows, 0:F] = (grad * up * (sig + act * (1.0 - sig))).astype(BF16)
            gb[s, rows, F : 2 * F] = (grad * act).astype(BF16)
            return carry

        lax.fori_loop(0, NT4, tile, 0)

    def gate_product(s, rows):
        return mm(gb[s, rows, :], wg[...], NT)

    def first_norm_back(s):
        grad = n1[s] + rs_finish(2, s)
        unit = unit1[s]
        sums = (jnp.sum(grad * unit, axis=0, keepdims=True), jnp.sum(grad, axis=0, keepdims=True))
        add_sums(s, 0, sums)
        back = norm_back(grad, unit, inv1[s, :, 0:1], gains[0:1, :])
        n1[s] = back
        ag3[s, t] = back.astype(BF16)
        ag_start(2, ag3, s)

    def weight_grad(dest, left_of, right):
        def tile(i, carry):
            columns = pl.ds(pl.multiple_of(i * 128, 128), 128)
            dest[columns, :] = mm(left_of(columns), right, TN).astype(BF16)
            return carry

        lax.fori_loop(0, D // 128, tile, 0)

    def reduce_copy(slot, d):
        to = (z + d) % NF
        rows = half_rows(to, x) if two_level(slot) else own_rows(to)
        return remote(
            sources[slot].at[rows, :], landings[slot].at[d - 1],
            gr_ss.at[slot, d - 1], gr_rs.at[slot, d - 1], "fsdp", to,
        )

    def two_level(slot):
        return pair and slot in (2, 3)

    def meet_copy(slot, block):
        return remote(
            sources[slot].at[half_rows(block, 1 - x), :], meets[slot - 2].at[block],
            h_ss.at[slot - 2, block], h_rs.at[slot - 2, block], "context", 1 - x,
        )

    def reduce_start(slot):
        for d in range(1, NF):
            if two_level(slot):
                meet_copy(slot, (z + d) % NF).start()
            else:
                reduce_copy(slot, d).start()
        if two_level(slot):
            meet_copy(slot, z).start()

    def reduce_meet(slot):
        if not two_level(slot):
            return
        for d in range(1, NF + 1):
            block = (z + d) % NF
            meet_copy(slot, block).wait_recv()
            rows = half_rows(block, x)
            sources[slot][rows, :] = (
                sources[slot][rows, :].astype(F32) + meets[slot - 2][block].astype(F32)
            ).astype(BF16)
            if d < NF:
                reduce_copy(slot, d).start()

    def reduce_middle(slot):
        rows = half_rows(z, x) if two_level(slot) else own_rows(z)
        total = sources[slot][rows, :].astype(F32)
        for d in range(1, NF):
            reduce_copy(slot, d).wait_recv()
            total = total + landings[slot][d - 1].astype(F32)
        sources[slot][rows, :] = total.astype(BF16)
        if two_level(slot):
            last_copy(slot).start()
        else:
            for d in range(1, NC):
                cross_copy(slot, d).start()
        own_copy(slot).start()

    def last_copy(slot):
        place = pl.ds(pl.multiple_of(x * HB, HB), HB)
        return remote(
            sources[slot].at[half_rows(z, x), :], own_out[slot].at[place, :],
            l_ss.at[slot - 2], l_rs.at[slot - 2], "context", 1 - x,
        )

    def cross_copy(slot, d):
        return remote(
            sources[slot].at[own_rows(z), :], crosses[slot].at[d - 1],
            x_ss.at[slot, d - 1], x_rs.at[slot, d - 1], "context", (x + d) % NC,
        )

    def own_copy(slot):
        if two_level(slot):
            place = pl.ds(pl.multiple_of(x * HB, HB), HB)
            return pltpu.make_async_copy(
                sources[slot].at[half_rows(z, x), :], own_out[slot].at[place, :],
                own_sem.at[slot],
            )
        return pltpu.make_async_copy(
            sources[slot].at[own_rows(z), :], own_out[slot], own_sem.at[slot]
        )

    def reduce_finish(slot):
        if two_level(slot):
            last_copy(slot).wait()
            for block in range(NF):
                meet_copy(slot, block).wait_send()
        else:
            for d in range(1, NC):
                cross_copy(slot, d).wait()
        own_copy(slot).wait()
        for d in range(1, NF):
            reduce_copy(slot, d).wait_send()

    def moment_copy(k):
        return remote(
            sends[k], lands[k], m_ss.at[k], m_rs.at[k], "context", (x + 1) % NC
        )

    def moment_cast(k):
        for i in range(2):
            moment_load(k, i).wait()
            if k == 2:
                for j in range(2):
                    sends[k][i, :, j * F : (j + 1) * F] = stages[k][i, :, j, :].astype(BF16)
            else:
                sends[k][i] = stages[k][i].astype(BF16)

    def norm_copy(buffer, axis, me, count, base, d):
        return remote(
            buffer.at[me], buffer.at[me], n_ss.at[base + d - 1], n_rs.at[base + d - 1],
            axis, (me + d) % count,
        )

    norm_levels = (
        (nsum_t, "tensor", t, NT4, 0),
        (nsum_c, "context", x, NC, NT4 - 1),
        (nsum_f, "fsdp", z, NF, NT4 - 1 + NC - 1),
    )

    def norm_start(level):
        for d in range(1, norm_levels[level][3]):
            norm_copy(*norm_levels[level], d).start()

    def norm_total(level):
        buffer, count = norm_levels[level][0], norm_levels[level][3]
        for d in range(1, count):
            norm_copy(*norm_levels[level], d).wait_recv()
        total = buffer[0]
        for i in range(1, count):
            total = total + buffer[i]
        return total

    def attended_back(s):
        def tile(i, carry):
            rows = pl.ds(pl.multiple_of(i * TS, TS), TS)
            datt[s, rows, :] = mm(ag3[s, i], wo[...], NN).astype(BF16)
            return carry

        lax.fori_loop(0, NT4, tile, 0)
        both = datt[s].astype(F32) * att[s].astype(F32)
        head_row = lax.broadcasted_iota(jnp.int32, (8, 256), 0)
        lane = lax.broadcasted_iota(jnp.int32, (8, 256), 1)
        chooser = (lane // HD == head_row + 1).astype(F32)
        dlt[s] = lax.dot_general(
            chooser, both, NT, precision=lax.Precision.HIGHEST, preferred_element_type=F32
        )

    def kvg_copy(s, d):
        return remote(
            kvg_s.at[(d - 1) % KS, s], kvg_r.at[d - 1, s],
            kvg_ss.at[d - 1, s], kvg_rs.at[d - 1, s], "context", (x + NC - d) % NC,
        )

    def attend_back(s):
        dqt[...] = jnp.zeros(dqt.shape, F32)

        def block(d):
            j = (x + NC - d) % NC
            doc_bias(j, s)
            vt[...] = mm(eye256, kv[j, s, :, 0:256], NT).astype(BF16)
            dk[...] = jnp.zeros(dk.shape, F32)
            dv[...] = jnp.zeros(dv.shape, F32)

            def head(h, inner):
                key_mask, value_mask = head_mask(h, 0), head_mask(h, HD)
                keys = keep(kv[j, s, :, 0:256], key_mask)
                row = pl.ds(h, 1)
                scores = mm(keys, q_ref[s], NT) * scale + bias_ref[...]
                probs = jnp.exp(scores - tot[s, row, :])
                dv[...] += mm(probs.astype(BF16), keep(datt[s], value_mask), NN)
                grad_probs = mm(keep(kv[j, s, :, 128:384], value_mask), datt[s], NT)
                grads = (probs * (grad_probs - dlt[s, row, :])).astype(BF16)
                dk[...] += mm(grads, keep(q_ref[s], key_mask), NN)
                rows = pl.ds(pl.multiple_of(h * HD, HD), HD)
                dqt[rows, :] += mm(vt[rows, :], grads, NN)
                return inner

            lax.fori_loop(0, H, head, 0)
            first = dk[:, 0:128] * scale
            second = dk[:, 128:256] * scale + dv[:, 0:128]
            return first, second, dv[:, 128:256]

        def far(d, carry):
            parts = block(d)
            if NC - 1 > KS:

                @pl.when(d > KS)
                def _():
                    kvg_copy(s, d - KS).wait_send()

            for k in range(3):
                kvg_s[(d - 1) % KS, s, :, k * 128 : (k + 1) * 128] = parts[k].astype(BF16)
            kvg_copy(s, d).start()
            return carry

        if NC > 1:
            lax.fori_loop(1, NC, far, 0)
        parts = block(0)
        for k in range(3):
            kv_own[s, :, k * 128 : (k + 1) * 128] = parts[k].astype(BF16)
        grad = jnp.transpose(dqt[...]) * scale
        q0, q1 = rotate_pair(grad, slice(0, T), -1.0)
        qb[s, :, 0:128] = q0.astype(BF16)
        qb[s, :, 128:256] = q1.astype(BF16)

    def keys_back(s):
        for d in range(1, NC):
            kvg_copy(s, d).wait_recv()

        def column(k):
            cols = slice(k * 128, (k + 1) * 128)
            total = kv_own[s, :, cols].astype(F32)
            for d in range(1, NC):
                total = total + kvg_r[d - 1, s, :, cols].astype(F32)
            return total

        k0, k1 = rotate_pair(
            jnp.concatenate([column(0), column(1)], axis=1), slice(0, T), -1.0
        )
        qb[s, :, QW : QW + 128] = k0.astype(BF16)
        qb[s, :, QW + 128 : QW + 256] = k1.astype(BF16)
        qb[s, :, QW + 256 : QW + 384] = column(2).astype(BF16)

    def input_product(s, rows):
        return mm(qb[s, rows, :], wq[...], NT)

    def input_out(s):
        n1[s] = n1[s] + rs_finish(3, s)
        input_copy(s).start()

    def input_copy(s):
        return pltpu.make_async_copy(n1.at[s], input_grad.at[s], loc_sem.at[1 + s])

    seqs = range(S)
    R = S * T

    for s in seqs:
        project(s)
    gather_hand(1)
    if adam:
        for k in (2, 0, 3, 1):
            moment_cast(k)
    attend(0)
    gather_finish(1)
    rs_produce(0, 0, out_product)
    for s in range(1, S):
        attend(s)
        rs_middle(0, s - 1)
        rs_produce(0, s, out_product)
        first_norm(s - 1)
    gather_hand(2)
    rs_middle(0, S - 1)
    first_norm(S - 1)
    gather_hand(3)
    for s in seqs:
        ag_middle(0, ag1, s)
    gather_finish(2)
    if adam:
        for k in (2, 0, 3, 1):
            moment_copy(k).start()
    for s in seqs:
        ag_finish(0, ag1, s)
        gate_up(s)
        if s == 0:
            gather_finish(3)
        rs_produce(1, s, down_product)
        if s > 0:
            rs_middle(1, s - 1)
    rs_middle(1, S - 1)
    cot_copy.wait()
    nsum_t[t] = jnp.zeros(nsum_t.shape[1:], F32)
    for s in seqs:
        second_norm(s)
    for s in seqs:
        ag_middle(1, ag2, s)
    for s in seqs:
        ag_finish(1, ag2, s)
        hidden_back(s)
        rs_produce(2, s, gate_product)
        if s > 0:
            rs_middle(2, s - 1)
    rs_middle(2, S - 1)
    weight_grad(sources[3], lambda c: ag2[:, :, :, c].reshape(R, 128), hid[...].reshape(R, F))
    reduce_start(3)
    for s in seqs:
        first_norm_back(s)
    norm_start(0)
    weight_grad(
        sources[2], lambda c: ag1[:, :, :, c].reshape(R, 128), gb[...].reshape(R, 2 * F)
    )
    reduce_start(2)
    for s in seqs:
        ag_middle(2, ag3, s)
    reduce_meet(3)
    for s in seqs:
        ag_finish(2, ag3, s)
        attended_back(s)
        if s == 0:
            nsum_c[x] = norm_total(0)
            norm_start(1)
        attend_back(s)
    reduce_meet(2)
    nsum_f[z] = norm_total(1)
    norm_start(2)
    weight_grad(
        sources[4], lambda c: tok[:, :, c].reshape(R, 128), qb[:, :, 0:QW].reshape(R, QW)
    )
    reduce_start(4)
    weight_grad(sources[1], lambda c: ag3[:, :, :, c].reshape(R, 128), att[...].reshape(R, 256))
    reduce_start(1)
    reduce_middle(3)
    for s in seqs:
        keys_back(s)
        if s == S - 1:
            weight_grad(
                sources[0], lambda c: tok[:, :, c].reshape(R, 128),
                qb[:, :, QW : QW + KW].reshape(R, KW),
            )
            reduce_start(0)
        rs_produce(3, s, input_product)
        if s > 0:
            rs_middle(3, s - 1)
    rs_middle(3, S - 1)
    norm_out[...] = norm_total(2)
    reduce_middle(2)
    reduce_middle(4)
    reduce_middle(1)
    for s in seqs:
        input_out(s)
    reduce_middle(0)
    for slot in (3, 2, 4, 1, 0):
        reduce_finish(slot)

    for s in seqs:
        input_copy(s).wait()
    wait_send(id_copies)
    for slot in range(4):
        for d in range(1, NF):
            fetch_copy(gathered[slot], slot, d).wait_send()
            if pair:
                hand_copy(gathered[slot], slot, d).wait_send()
    for s in seqs:
        for d in range(1, NC):
            kv_copy(s, d).wait_send()
            if d > NC - 1 - KS:
                kvg_copy(s, d).wait_send()
        for part in range(3):
            rs_copy(3, s, part).wait_send()
        for rnd, buffer in ((0, ag1), (1, ag2), (2, ag3)):
            for part in range(3):
                ag_copy(rnd, buffer, s, part).wait_send()
    for level in range(3):
        for d in range(1, norm_levels[level][3]):
            norm_copy(*norm_levels[level], d).wait_send()
    if adam:
        for k in range(4):
            moment_copy(k).wait()


def finish_kernel(dims, *refs):
    S, T, D, C, F, NF, NC, NT4 = dims
    DB = D // NF
    refs = list(refs)

    def take(count):
        taken, refs[:] = refs[:count], refs[count:]
        return taken

    owner, norm_sums, norm_m, norm_v = take(4)
    layer_in, input_in = take(2)
    own_in, cross_in, masters_in, moments_in, lands_in = take(5), take(5), take(4), take(8), take(4)
    layer_out, input_out = take(2)
    grads_out, states_out = take(4), take(4)
    norm_out, norm_state, norm_flat, updates = take(4)
    layer_v, input_v = take(2)
    own_g, cross_g, masters, lands = take(5), take(5), take(4), take(4)
    pair = NC == 2
    states, grads, flats = take(4), take(4), take(4)
    row_a, row_b, in_sem, out_sem, pass_sem = take(5)
    z, x, t = lax.axis_index("fsdp"), lax.axis_index("context"), lax.axis_index("tensor")
    order = (2, 3, 1, 0)

    def loads(k):
        pairs = [
            (masters_in[k], masters[k]), (lands_in[k], lands[k]),
            (moments_in[2 * k].at[0], states[k].at[0]),
            (moments_in[2 * k + 1].at[0], states[k].at[1]),
        ]
        for slot in ((0, 4) if k == 0 else (k,)):
            pairs.append((own_in[slot], own_g[slot]))
            if not (pair and slot in (2, 3)):
                pairs.append((cross_in[slot], cross_g[slot]))
        return [
            pltpu.make_async_copy(src, dst, in_sem.at[k, i]) for i, (src, dst) in enumerate(pairs)
        ]

    def passing(k, stage):
        src, mid, dst = ((layer_in, layer_v, layer_out), (input_in, input_v, input_out))[k]
        if stage == 0:
            return pltpu.make_async_copy(src, mid, pass_sem.at[k, 0])
        return pltpu.make_async_copy(mid, dst, pass_sem.at[k, 1])

    for k in order:
        for c in loads(k):
            c.start()
    for k in range(2):
        passing(k, 0).start()

    def adam_parts(g, m, v, w, decay):
        m_new = BETA_ONE * m + (1.0 - BETA_ONE) * g
        v_new = BETA_TWO * v + (1.0 - BETA_TWO) * g * g
        corrected = m_new / (1.0 - BETA_ONE**ADAM_STEP)
        scaled = v_new / (1.0 - BETA_TWO**ADAM_STEP)
        step = corrected / (jnp.sqrt(scaled) + ADAM_EPS)
        if decay:
            step = step + decay * w
        return m_new, v_new, -RATE * step

    def rows_to_flat(flat, count, width):
        block = math.lcm(width, 128)
        period, lines = block // width, block // 128
        many = count // period
        halves = (row_a, row_b)
        for line in range(lines):
            parts, at = [], line * 128
            while at < (line + 1) * 128:
                row, column = divmod(at, width)
                half, lane = divmod(column, 128)
                length = min((line + 1) * 128 - at, width - column, 128 - lane)
                rows = halves[half][pl.ds(row, many, stride=period), :]
                parts.append(rows[:, lane : lane + length])
                at += length
            whole = parts[0] if len(parts) == 1 else jnp.concatenate(parts, axis=1)
            flat[pl.ds(line, many, stride=lines), :] = whole

    def to_rows(values, rows):
        width = values.shape[1]
        for half, place in enumerate((row_a, row_b)):
            part = values[:, half * 128 : min(width, (half + 1) * 128)]
            if part.shape[1] == 0:
                continue
            if part.shape[1] < 128:
                rest = jnp.zeros((part.shape[0], 128 - part.shape[1]), F32)
                part = jnp.concatenate([part, rest], axis=1)
            place[rows, :] = part

    sizes = (DB * 3 * C, C * DB, DB * 2 * F, F * DB)

    def out_copies(k):
        first = sum(sizes[:k])
        return (
            pltpu.make_async_copy(grads[k], grads_out[k], out_sem.at[k, 0]),
            pltpu.make_async_copy(states[k], states_out[k], out_sem.at[k, 1]),
            pltpu.make_async_copy(
                flats[k].reshape(1, sizes[k]),
                updates.at[0, :, pl.ds(first, sizes[k])],
                out_sem.at[k, 2],
            ),
        )

    def summed(slot):
        own = own_g[slot][...].astype(F32)
        if pair:
            return own if slot in (2, 3) else own + cross_g[slot][0].astype(F32)
        total = jnp.zeros_like(own)
        for i in range(NC):
            other = cross_g[slot][jnp.maximum((x - i + NC) % NC, 1) - 1].astype(F32)
            total = total + jnp.where(x == i, own, other)
        return total

    for k in order:
        for c in loads(k):
            c.wait()
        total = summed(k)
        if k == 0:
            parts = [summed(4)[:, 0:C], total[:, 0:C], total[:, C : 2 * C]]
        elif k == 1:
            parts = [jnp.transpose(total)[HD : HD + C, :]]
        elif k == 2:
            parts = [total[:, 0:F], total[:, F : 2 * F]]
        else:
            parts = [total]
        mine = owner[0:1, k : k + 1] == x
        for j, g in enumerate(parts):
            at = (j,) if k == 0 else (slice(None), j) if k == 2 else (slice(None),)
            land_at = (slice(None), slice(j * F, (j + 1) * F)) if k == 2 else at
            grads[k][at] = g
            kept = [
                jnp.where(
                    mine, states[k][(i, *at)].astype(BF16).astype(F32),
                    lands[k][(i, *land_at)].astype(F32),
                )
                for i in range(2)
            ]
            m_new, v_new, step = adam_parts(g, *kept, masters[k][at], DECAY)
            states[k][(0, *at)] = m_new
            states[k][(1, *at)] = v_new
            if k == 0:
                to_rows(step, pl.ds(j, DB, stride=3))
            elif k == 1:
                to_rows(step, pl.ds(0, C))
            elif k == 2:
                for c in range(F // 128):
                    flats[2][pl.ds(j * (F // 128) + c, DB, stride=2 * F // 128), :] = step[
                        :, c * 128 : (c + 1) * 128
                    ]
            else:
                to_rows(jnp.transpose(step), pl.ds(0, F))
        if k != 2:
            rows_to_flat(flats[k], (3 * DB, C, 0, F)[k], (C, DB, 0, DB)[k])
        for c in out_copies(k):
            c.start()
        if k == 2:
            for i in range(2):
                passing(i, 0).wait()
                passing(i, 1).start()

    g = norm_sums[0:4, :]
    m_new, v_new, step = adam_parts(g, norm_m[...], norm_v[...], None, 0.0)
    norm_out[...] = g
    norm_state[0] = m_new
    norm_state[1] = v_new
    count = 4 * D // (NF * NT4)
    per_row = D // count
    place = z * NT4 + t
    row = lax.broadcasted_iota(jnp.int32, (4, count), 0)
    chosen = jnp.zeros((4, count), F32)
    for c in range(per_row):
        hit = row * per_row + c == place
        chosen = chosen + jnp.where(hit, step[:, c * count : (c + 1) * count], 0.0)
    norm_flat[...] = jnp.sum(chosen, axis=0, keepdims=True)
    for k in order:
        for c in out_copies(k):
            c.wait()
    for k in range(2):
        passing(k, 1).wait()


def run_layer(
    tokens, cotangent, segment_ids, owner, weights, norm_gains, norm_biases, moments,
    norm_moments, cosine, sine_rows,
):
    S, T, D = tokens.shape
    C, F = weights[0].shape[2], weights[2].shape[2]
    NF, NC, NT4 = lax.axis_size("fsdp"), lax.axis_size("context"), lax.axis_size("tensor")
    TS, DB, KW, W = T // NT4, D // NF, 384, 640
    adam = NC == 2
    assert NT4 == 4 and C == 192
    vmem = pl.BlockSpec(memory_space=pltpu.VMEM)
    far = pl.BlockSpec(memory_space=pl.ANY)
    VM = pltpu.VMEM
    DMA = pltpu.SemaphoreType.DMA
    NX = max(NC - 1, 1)
    grad_columns = (KW, 256, 2 * F, F, 256)
    scratch = [
        VM((D, W), BF16), VM((D, 256), BF16), VM((D, 2 * F), BF16), VM((D, F), BF16),
        VM((NC, S, T), jnp.int32), VM((S, T, 256), BF16), VM((NC, S, T, KW), BF16),
        VM((S, T, 256), BF16), VM((S, 8, T), F32), VM((8, T), F32), VM((8, T), F32),
        VM((256, T), F32), VM((T, T), F32), VM((256, T), BF16),
        VM((S, 2, 2, TS, D), BF16), VM((S, 2, TS, D), BF16), VM((S, TS, D), BF16), VM((S, TS, D), BF16),
        VM((S, 4, TS, D), BF16), VM((S, 4, TS, D), BF16), VM((S, 4, TS, D), BF16),
        VM((S, T, F), BF16), VM((S, T, 2 * F), BF16),
        VM((S, TS, D), F32), VM((S, TS, D), F32), VM((S, TS, 128), F32),
        VM((S, T, 256), BF16), VM((S, 8, T), F32),
        VM((T, 256), F32), VM((T, 256), F32), VM((min(NX, 2), S, T, KW), BF16), VM((NX, S, T, KW), BF16),
        VM((S, T, KW), BF16), VM((S, T, W), BF16),
        *(VM((D, columns), BF16) for columns in grad_columns),
        *(
            VM((NF - 1, DB // 2 if NC == 2 and slot in (2, 3) else DB, grad_columns[slot]), BF16)
            for slot in range(5)
        ),
        *(
            VM((NF, DB // 2, columns) if NC == 2 else (1, 16, 128), BF16)
            for columns in grad_columns[2:4]
        ),
        VM((NT4, 8, D), F32), VM((NC, 8, D), F32), VM((NF, 8, D), F32), VM((S, TS, D), BF16),
        DMA((4, NF - 1)), DMA((4, NF - 1)), DMA((S, NX)), DMA((S, NX)), DMA((NX,)), DMA((NX,)),
        DMA((4, S, 3)), DMA((4, S, 3)), DMA((3, S, 3)), DMA((3, S, 3)),
        DMA((NX, S)), DMA((NX, S)), DMA((5, NF - 1)), DMA((5, NF - 1)), DMA((5, NX)), DMA((5, NX)),
        DMA((NT4 + NC + NF,)), DMA((NT4 + NC + NF,)), DMA((1 + S,)), DMA((5,)),
        DMA((4, NF - 1)), DMA((4, NF - 1)), DMA((2, NF)), DMA((2, NF)), DMA((2,)), DMA((2,)),
    ]
    shapes = ((3, DB, C), (C, DB), (DB, 2, F), (DB, F))
    flat_shapes = tuple((DB, columns) for columns in grad_columns)
    low_shapes = ((2, 3, DB, C), (2, C, DB), (2, DB, 2 * F), (2, DB, F))
    dims = (S, T, D, C, F, NF, NC, NT4)
    outs = [
        jax.ShapeDtypeStruct((S, TS, D), BF16),
        jax.ShapeDtypeStruct((S, TS, D), F32),
        *(jax.ShapeDtypeStruct(shape, BF16) for shape in flat_shapes),
        *(jax.ShapeDtypeStruct((NX, *shape), BF16) for shape in flat_shapes),
        jax.ShapeDtypeStruct((8, D), F32),
    ]
    out_specs = [vmem] + [far] * 11 + [vmem]
    args = [
        tokens, cotangent, segment_ids, *weights, norm_gains, norm_biases, cosine, sine_rows,
    ]
    in_specs = [vmem, far] + [vmem] * 9
    flat_moments = [m for pair in moments for m in pair]
    if adam:
        outs += [jax.ShapeDtypeStruct(shape, BF16) for shape in low_shapes]
        out_specs += [far] * 4
        args += flat_moments
        in_specs += [far] * 8
        scratch += [VM((2, *shape), F32) for shape in shapes]
        scratch += [VM(shape, BF16) for shape in low_shapes]
        scratch += [DMA((4,)), DMA((4,)), DMA((4, 2))]
    results = pl.pallas_call(
        functools.partial(layer_kernel, dims),
        out_shape=outs,
        in_specs=in_specs,
        out_specs=out_specs,
        scratch_shapes=scratch,
        compiler_params=pltpu.CompilerParams(
            collective_id=0, has_side_effects=True, vmem_limit_bytes=67043328
        ),
        name="layer",
    )(*args)
    layer_out, input_grad = results[:2]
    own_grads, cross_grads, norm_sums = results[2:7], results[7:12], results[12]
    if adam:
        lands = results[13:]
    else:
        lands = []
        for k in range(4):
            pair = jnp.concatenate(moments[k], axis=0).astype(BF16).reshape(low_shapes[k])
            lands.append(from_root(pair, "context", owner[k]))
        owner = jnp.full_like(owner, -1)

    total = sum(math.prod(shape) for shape in shapes)
    count = 4 * D // (NF * NT4)
    out_shape = [
        jax.ShapeDtypeStruct((S, TS, D), BF16),
        jax.ShapeDtypeStruct((S, TS, D), F32),
        *(jax.ShapeDtypeStruct(shape, F32) for shape in shapes),
        *(jax.ShapeDtypeStruct((2, *shape), F32) for shape in shapes),
        jax.ShapeDtypeStruct((4, D), F32),
        jax.ShapeDtypeStruct((2, 4, D), F32),
        jax.ShapeDtypeStruct((1, count), F32),
        jax.ShapeDtypeStruct((1, 1, total + count), F32),
    ]
    rows = max(3 * DB, F)
    return pl.pallas_call(
        functools.partial(finish_kernel, dims),
        out_shape=out_shape,
        in_specs=[vmem] * 4 + [far] * 28,
        out_specs=[far] * 10 + [vmem] * 3 + [far],
        scratch_shapes=[
            VM((S, TS, D), BF16), VM((S, TS, D), F32),
            *(VM(shape, BF16) for shape in flat_shapes),
            *(VM((NX, *shape), BF16) for shape in flat_shapes),
            *(VM(shape, F32) for shape in shapes),
            *(VM(shape, BF16) for shape in low_shapes),
            *(VM((2, *shape), F32) for shape in shapes),
            *(VM(shape, F32) for shape in shapes),
            *(VM((math.prod(shape) // 128, 128), F32) for shape in shapes),
            VM((rows, 128), F32), VM((rows, 128), F32),
            DMA((4, 8)), DMA((4, 3)), DMA((2, 2)),
        ],
        compiler_params=pltpu.CompilerParams(vmem_limit_bytes=67043328),
        name="finish",
    )(
        owner.reshape(1, 4), norm_sums, *norm_moments, layer_out, input_grad, *own_grads,
        *cross_grads, *weights, *flat_moments, *lands,
    )


def from_root(block, axis, owner):
    block = jnp.where(lax.axis_index(axis) == owner, block, jnp.zeros_like(block))
    return lax.psum(block, axis)


def shards(
    tokens, cotangent, segment_ids, owner, qkv_weight, out_weight, gate_up_weight, down_weight,
    norm_gains, norm_biases, qkv_moment, qkv_square, out_moment, out_square, gate_moment,
    gate_square, down_moment, down_square, norm_moment, norm_square,
):
    tok_here = tokens.shape[1]
    moments = (
        (qkv_moment, qkv_square), (out_moment, out_square),
        (gate_moment, gate_square), (down_moment, down_square),
    )
    positions = (
        lax.axis_index("context") * tok_here + jnp.arange(tok_here, dtype=jnp.int32)
    ).astype(F32)
    frequency = jnp.power(F32(ROPE_BASE), -jnp.arange(0, HD, 2, dtype=F32) / HD)
    angles = positions[:, None] * frequency[None, :]
    cosine, sine_rows = jnp.cos(angles), jnp.sin(angles)
    cosine = jnp.concatenate([cosine] * 4, axis=1)
    sine_rows = jnp.concatenate([-sine_rows, sine_rows] * 2, axis=1)

    columns_last = (0, 2, 1, 3)
    weights = (
        jnp.transpose(qkv_weight, (1, 0, 2)), out_weight, gate_up_weight, jnp.transpose(down_weight),
    )
    turned = (
        [jnp.transpose(m, columns_last) for m in moments[0]],
        moments[1],
        moments[2],
        [jnp.transpose(m, (0, 2, 1)) for m in moments[3]],
    )
    results = run_layer(
        tokens, cotangent, segment_ids, owner, weights, norm_gains, norm_biases, turned,
        (norm_moment, norm_square), cosine, sine_rows,
    )
    layer_out, input_grad, grad_q, grad_o, grad_g, grad_d = results[:6]
    state_q, state_o, state_g, state_d = results[6:10]
    norm_grad, norm_state, piece, weight_updates = results[10:]
    weight_updates = lax.dynamic_update_slice(
        weight_updates, piece[None], (0, 0, weight_updates.shape[2] - piece.shape[1])
    )
    return (
        layer_out, input_grad,
        jnp.transpose(grad_q, (1, 0, 2)), grad_o, grad_g, jnp.transpose(grad_d),
        norm_grad,
        jnp.transpose(state_q, columns_last), state_o, state_g, jnp.transpose(state_d, (0, 2, 1)),
        norm_state, weight_updates,
    )


def solution(mesh):
    return jax.shard_map(
        shards,
        mesh=mesh,
        in_specs=(
            P("fsdp", "context", None),
            P("fsdp", "context", None),
            P("fsdp", "context"),
            P(),
            P("fsdp", None, "tensor"),
            P("tensor", "fsdp"),
            P("fsdp", None, "tensor"),
            P("tensor", "fsdp"),
            P(),
            P(),
            P("context", "fsdp", None, "tensor"),
            P("context", "fsdp", None, "tensor"),
            P("context", "tensor", "fsdp"),
            P("context", "tensor", "fsdp"),
            P("context", "fsdp", None, "tensor"),
            P("context", "fsdp", None, "tensor"),
            P("context", "tensor", "fsdp"),
            P("context", "tensor", "fsdp"),
            P(),
            P(),
        ),
        out_specs=(
            P("fsdp", ("context", "tensor"), None),
            P("fsdp", ("context", "tensor"), None),
            P("fsdp", None, "tensor"),
            P("tensor", "fsdp"),
            P("fsdp", None, "tensor"),
            P("tensor", "fsdp"),
            P(),
            P(None, "fsdp", None, "tensor"),
            P(None, "tensor", "fsdp"),
            P(None, "fsdp", None, "tensor"),
            P(None, "tensor", "fsdp"),
            P(),
            P("fsdp", "tensor", None),
        ),
        check_vma=False,
    )
```

```python
import functools
import math

import jax
import jax.numpy as jnp
from jax import lax
from jax.experimental import pallas as pl
from jax.experimental.pallas import tpu as pltpu
from jax.sharding import PartitionSpec as P

HD = 64

NEGATIVE = -1e30
EPSILON = 1e-05
ROPE_BASE = 1000.0
BETA_ONE = 0.9
BETA_TWO = 0.999
ADAM_EPS = 1e-08
ADAM_STEP = 3.0
RATE = 0.03
DECAY = 0.1

F32 = jnp.float32
BF16 = jnp.bfloat16
MESH = pl.DeviceIdType.MESH
NN = (((1,), (0,)), ((), ()))
NT = (((1,), (1,)), ((), ()))
TN = (((0,), (0,)), ((), ()))


FETCH_HALVES = (0, 2)
SUM_HALVES = (2, 4)
RELAYED = (1, 2, 3, 4)


def mm(left, right, dims):
    return lax.dot_general(left, right, dims, preferred_element_type=F32)


def swap_halves(values):
    lane = lax.broadcasted_iota(jnp.int32, values.shape, 1)
    low_half = lane % HD < HD // 2
    return jnp.where(
        low_half,
        pltpu.roll(values, 128 - HD // 2, 1),
        pltpu.roll(values, HD // 2, 1),
    )


def mean_of(values):
    return jnp.sum(values, axis=-1, keepdims=True) * (1.0 / values.shape[-1])


def normalize(values, gain_row, bias_row):
    center = values - mean_of(values)
    inverse_std = lax.rsqrt(mean_of(center * center) + EPSILON)
    unit = center * inverse_std
    return unit * gain_row + bias_row, unit, inverse_std


def norm_back(gradient, unit, inverse_std, gain_row):
    scaled = gradient * gain_row
    return inverse_std * (scaled - mean_of(scaled) - unit * mean_of(scaled * unit))


class Pack:
    pass


def layer_kernel(dims, *refs):
    S, T, D, C, F, NF, NC, NT4 = dims
    TS = T // NT4
    DB = D // NF
    adam = NC == 2
    pair = NC == 2
    HB = DB // 2
    refs = list(refs)
    QW, KW = 256, 384
    H = C // HD
    KS = min(max(NC - 1, 1), 2)
    scale = HD ** (-0.5)
    def take(count):
        taken, refs[:] = refs[:count], refs[count:]
        return taken

    tok, cot, ids_in, wq_in, wo_in, wg_in, wd_in, gains, biases, cos_t, sin_t = take(11)
    if adam:
        moments = take(8)
    layer_out, input_grad = take(2)
    own_out, crosses = take(5), take(5)
    norm_out = take(1)[0]
    if adam:
        lands = take(4)
    wq, wo, wg, wd, ids_all, q_ref, kv, att, tot, am, al, acc, bias_ref, vt = take(14)
    rsend, rsb, rs2, rs2r, ag1, ag2, ag3, hid, gb = take(9)
    n1, unit1, inv1, datt, dlt, dqt, dk, dv, kvg_s, kvg_r, kv_own, qb = take(12)
    sources, landings, meets = take(5), take(5), take(2)
    nsum_t, nsum_c, nsum_f, cot_v = take(4)
    w_ss, w_rs, kv_ss, kv_rs, id_ss, id_rs, rs_ss, rs_rs, ag_ss, ag_rs = take(10)
    kvg_ss, kvg_rs, gr_ss, gr_rs, x_ss, x_rs, n_ss, n_rs, loc_sem = take(9)
    own_sem, f_ss, f_rs, h_ss, h_rs, l_ss, l_rs = take(7)
    if adam:
        stages, sends = take(4), take(4)
        m_ss, m_rs, in_sem = take(3)

    z, x, t = lax.axis_index("fsdp"), lax.axis_index("context"), lax.axis_index("tensor")
    core, yy = t % 2, t // 2
    t_core = yy * 2 + (1 - core)
    t_y = (1 - yy) * 2 + core
    t_diag = (1 - yy) * 2 + (1 - core)

    def remote(src, dst, ssem, rsem, axis, index):
        return pltpu.make_async_remote_copy(
            src_ref=src, dst_ref=dst, send_sem=ssem, recv_sem=rsem,
            device_id={axis: index}, device_id_type=MESH,
        )

    barrier = pltpu.get_barrier_semaphore()
    for d in range(1, NF):
        pl.semaphore_signal(barrier, inc=1, device_id={"fsdp": (z + d) % NF}, device_id_type=MESH)
    for d in range(1, NC):
        pl.semaphore_signal(barrier, inc=1, device_id={"context": (x + d) % NC}, device_id_type=MESH)
    for d in range(1, NT4):
        pl.semaphore_signal(barrier, inc=1, device_id={"tensor": (t + d) % NT4}, device_id_type=MESH)

    def moment_load(k, i):
        return pltpu.make_async_copy(
            moments[2 * k + i].at[0], stages[k].at[i], in_sem.at[k, i]
        )

    cot_copy = pltpu.make_async_copy(
        cot.at[:, pl.ds(pl.multiple_of(t * TS, TS), TS), :], cot_v, loc_sem.at[0]
    )
    cot_copy.start()
    if adam:
        for k in range(4):
            for i in range(2):
                moment_load(k, i).start()

    def own_rows(index):
        return pl.ds(pl.multiple_of(index * DB, DB), DB)

    def pad_cols(values, left, right):
        parts = []
        if left:
            parts.append(jnp.zeros((values.shape[0], left), values.dtype))
        parts.append(values)
        if right:
            parts.append(jnp.zeros((values.shape[0], right), values.dtype))
        return jnp.concatenate(parts, axis=1)

    wq[own_rows(z), :] = jnp.concatenate(
        [
            pad_cols(wq_in[0], 0, QW - C),
            jnp.concatenate([wq_in[1], wq_in[2]], axis=1),
        ],
        axis=1,
    ).astype(BF16)

    pl.semaphore_wait(barrier, NF - 1 + NC - 1 + NT4 - 1)

    def half_rows(block, half):
        return pl.ds(pl.multiple_of(block * DB + half * HB, HB), HB)

    def fetch_copy(buffer, slot, d):
        rows = half_rows(z, x) if halved(slot) else own_rows(z)
        return remote(
            buffer.at[rows, :], buffer.at[rows, :],
            w_ss.at[slot, d - 1], w_rs.at[slot, d - 1], "fsdp", (z + d) % NF,
        )

    def hand_copy(buffer, slot, d):
        rows = half_rows((z + NF - d) % NF, x)
        return remote(
            buffer.at[rows, :], buffer.at[rows, :],
            f_ss.at[slot, d - 1], f_rs.at[slot, d - 1], "context", 1 - x,
        )

    def halved(slot):
        return pair and slot in FETCH_HALVES

    def gather_start(slot):
        for d in range(1, NF):
            fetch_copy(gathered[slot], slot, d).start()

    def gather_hand(slot):
        for d in range(1, NF):
            fetch_copy(gathered[slot], slot, d).wait_recv()
            if halved(slot):
                hand_copy(gathered[slot], slot, d).start()

    def gather_finish(slot):
        if halved(slot):
            for d in range(1, NF):
                hand_copy(gathered[slot], slot, d).wait_recv()

    gathered = (wq, wo, wg, wd)

    def wait_recv(copies):
        for c in copies:
            c.wait_recv()

    def wait_send(copies):
        for c in copies:
            c.wait_send()

    gather_start(0)

    ids_all[x] = ids_in[...]
    id_copies = []
    for d in range(1, NC):
        c = remote(
            ids_all.at[x], ids_all.at[x], id_ss.at[d - 1], id_rs.at[d - 1],
            "context", (x + d) % NC,
        )
        c.start()
        id_copies.append(c)

    def eye(n):
        return (
            lax.broadcasted_iota(jnp.int32, (n, n), 0)
            == lax.broadcasted_iota(jnp.int32, (n, n), 1)
        ).astype(F32).astype(BF16)

    wo_t = jnp.transpose(wo_in[...])
    wo[own_rows(z), :] = pad_cols(wo_t, HD, 0).astype(BF16)
    wd[own_rows(z), :] = wd_in[...].astype(BF16)
    wg[own_rows(z), 0:F] = wg_in[:, 0, :].astype(BF16)
    wg[own_rows(z), F : 2 * F] = wg_in[:, 1, :].astype(BF16)

    gather_hand(0)
    gather_start(1)
    gather_start(2)
    gather_start(3)
    gather_finish(0)

    def rotate_pair(values, rows, sign):
        cosine, sine_rows = cos_t[rows, :], sin_t[rows, :] * sign
        lane = lax.broadcasted_iota(jnp.int32, cosine.shape, 1)
        head = lane < HD
        first, second = values[:, 0:128], values[:, 128:256]
        first = first * cosine + swap_halves(first) * sine_rows
        second = second * jnp.where(head, cosine, 1.0) + swap_halves(second) * jnp.where(
            head, sine_rows, 0.0
        )
        return first, second

    TR = min(256, T)

    def project(s):
        def tile(i, carry):
            rows = pl.ds(pl.multiple_of(i * TR, TR), TR)
            p = mm(tok[s, rows, :], wq[...], NN)
            q0, q1 = rotate_pair(p[:, 0:QW], rows, 1.0)
            q_ref[s, rows, 0:128] = q0.astype(BF16)
            q_ref[s, rows, 128:256] = q1.astype(BF16)
            k0, k1 = rotate_pair(p[:, QW : QW + 256], rows, 1.0)
            kv[x, s, rows, 0:128] = k0.astype(BF16)
            kv[x, s, rows, 128:256] = k1.astype(BF16)
            kv[x, s, rows, 256:384] = p[:, QW + 256 : QW + 384].astype(BF16)
            return carry

        lax.fori_loop(0, T // TR, tile, 0)
        for d in range(1, NC):
            kv_copy(s, d).start()

    def kv_copy(s, d):
        return remote(
            kv.at[x, s], kv.at[x, s], kv_ss.at[s, d - 1], kv_rs.at[s, d - 1],
            "context", (x + d) % NC,
        )

    def head_mask(h, offset):
        lane = lax.broadcasted_iota(jnp.int32, (1, 256), 1)
        return jnp.logical_and(lane >= offset + h * HD, lane < offset + (h + 1) * HD)

    def keep(values, mask):
        return jnp.where(mask, values, jnp.zeros_like(values))

    def doc_bias(j, s):
        key_ids = jnp.broadcast_to(ids_all[j, pl.ds(s, 1), :].astype(F32), (128, T))
        key_col = jnp.transpose(key_ids)[:, 0:1]
        query_row = ids_all[x, pl.ds(s, 1), :].astype(F32)
        bias_ref[...] = jnp.where(key_col == query_row, 0.0, NEGATIVE)

    eye256 = eye(256)

    def attend(s):
        am[...] = jnp.full(am.shape, NEGATIVE, F32)
        al[...] = jnp.zeros(al.shape, F32)
        acc[...] = jnp.zeros(acc.shape, F32)

        def block(d, carry):
            j = (x + NC - d) % NC
            doc_bias(j, s)
            vt[...] = mm(eye256, kv[j, s, :, 128:384], NT).astype(BF16)

            def head(h, inner):
                keys = keep(kv[j, s, :, 0:256], head_mask(h, 0))
                scores = mm(keys, q_ref[s], NT) * scale + bias_ref[...]
                row = pl.ds(h, 1)
                before = am[row, :]
                newest = jnp.maximum(before, jnp.max(scores, axis=0, keepdims=True))
                shrink = jnp.exp(before - newest)
                weights = jnp.exp(scores - newest)
                al[row, :] = al[row, :] * shrink + jnp.sum(weights, axis=0, keepdims=True)
                am[row, :] = newest
                rows = pl.ds(pl.multiple_of(h * HD, HD), HD)
                vrows = pl.ds(pl.multiple_of(HD + h * HD, HD), HD)
                acc[vrows, :] = acc[vrows, :] * shrink + mm(
                    vt[vrows, :], weights.astype(BF16), NN
                )
                return inner

            lax.fori_loop(0, H, head, 0)
            return carry

        block(0, 0)
        if NC > 1:
            for d in range(1, NC):
                kv_copy(s, d).wait_recv()
            if s == 0:
                wait_recv(id_copies)
            lax.fori_loop(1, NC, block, 0)
        for h in range(H):
            rows = slice(HD + h * HD, HD + (h + 1) * HD)
            acc[rows, :] = acc[rows, :] / al[h : h + 1, :]
        tot[s] = am[...] + jnp.log(jnp.maximum(al[...], 1e-37))
        att[s] = jnp.transpose(acc[...]).astype(BF16)

    def rs_copy(rnd, s, part):
        if part < 2:
            chip = 1 - yy if part == 0 else yy
            return remote(
                rsend.at[s, chip, 1 - core], rsb.at[s, chip],
                rs_ss.at[rnd, s, part], rs_rs.at[rnd, s, part], "tensor", t_core,
            )
        return remote(
            rs2.at[s], rs2r.at[s], rs_ss.at[rnd, s, 2], rs_rs.at[rnd, s, 2], "tensor", t_y
        )

    def rs_produce(rnd, s, product):
        if rnd > 0:
            for part in range(3):
                rs_copy(rnd - 1, s, part).wait_send()

        def tile(i, carry):
            chip = jnp.where(i < 2, 1 - yy, yy)
            other = jnp.where(i % 2 == 0, 1 - core, core)
            start = pl.multiple_of((chip * 2 + other) * TS, TS)
            rsend[s, chip, other] = product(s, pl.ds(start, TS)).astype(BF16)
            return carry

        lax.fori_loop(0, 2, tile, 0)
        rs_copy(rnd, s, 0).start()
        lax.fori_loop(2, 4, tile, 0)
        rs_copy(rnd, s, 1).start()

    def rs_middle(rnd, s):
        rs_copy(rnd, s, 0).wait_recv()
        rs2[s] = (
            rsend[s, 1 - yy, core].astype(F32) + rsb[s, 1 - yy].astype(F32)
        ).astype(BF16)
        rs_copy(rnd, s, 2).start()

    def rs_finish(rnd, s):
        rs_copy(rnd, s, 1).wait_recv()
        rs_copy(rnd, s, 2).wait_recv()
        return rsend[s, yy, core].astype(F32) + rsb[s, yy].astype(F32) + rs2r[s].astype(F32)

    def ag_copy(rnd, buffer, s, part):
        if part == 0:
            return remote(
                buffer.at[s, t], buffer.at[s, t],
                ag_ss.at[rnd, s, 0], ag_rs.at[rnd, s, 0], "tensor", t_core,
            )
        if part == 1:
            return remote(
                buffer.at[s, t], buffer.at[s, t],
                ag_ss.at[rnd, s, 1], ag_rs.at[rnd, s, 1], "tensor", t_y,
            )
        return remote(
            buffer.at[s, t_y], buffer.at[s, t_y],
            ag_ss.at[rnd, s, 2], ag_rs.at[rnd, s, 2], "tensor", t_core,
        )

    def ag_start(rnd, buffer, s):
        ag_copy(rnd, buffer, s, 1).start()
        ag_copy(rnd, buffer, s, 0).start()

    def ag_middle(rnd, buffer, s):
        ag_copy(rnd, buffer, s, 1).wait_recv()
        ag_copy(rnd, buffer, s, 2).start()

    def ag_finish(rnd, buffer, s):
        ag_copy(rnd, buffer, s, 0).wait_recv()
        ag_copy(rnd, buffer, s, 2).wait_recv()

    def out_product(s, rows):
        return mm(att[s, rows, :], wo[...], NT)

    def first_norm(s):
        share = pl.ds(pl.multiple_of(t * TS, TS), TS)
        values = tok[s, share, :].astype(F32) + rs_finish(0, s)
        normed, unit, inverse = normalize(values, gains[0:1, :], biases[0:1, :])
        n1[s] = normed
        unit1[s] = unit
        inv1[s] = jnp.broadcast_to(inverse, (TS, 128))
        ag1[s, t] = normed.astype(BF16)
        ag_start(0, ag1, s)

    def sigmoid(v):
        return 1.0 / (1.0 + jnp.exp(-v))

    def gate_up(s):
        def tile(i, carry):
            rows = pl.ds(pl.multiple_of(i * TS, TS), TS)
            both = mm(ag1[s, i], wg[...], NN)
            gate, up = both[:, 0:F], both[:, F : 2 * F]
            gb[s, rows, 0:F] = gate.astype(BF16)
            gb[s, rows, F : 2 * F] = up.astype(BF16)
            hid[s, rows, :] = (gate * sigmoid(gate) * up).astype(BF16)
            return carry

        lax.fori_loop(0, NT4, tile, 0)

    def down_product(s, rows):
        return mm(hid[s, rows, :], wd[...], NT)

    def second_norm(s):
        values = n1[s] + rs_finish(1, s)
        out, unit, inverse = normalize(values, gains[1:2, :], biases[1:2, :])
        layer_out[s] = out.astype(BF16)
        grad = cot_v[s].astype(F32)
        sums = (jnp.sum(grad * unit, axis=0, keepdims=True), jnp.sum(grad, axis=0, keepdims=True))
        add_sums(s, 1, sums)
        back = norm_back(grad, unit, inverse, gains[1:2, :])
        n1[s] = back
        ag2[s, t] = back.astype(BF16)
        ag_start(1, ag2, s)

    def add_sums(s, row, sums):
        for k in range(2):
            at = slice(row + 2 * k, row + 2 * k + 1)
            if s == 0:
                nsum_t[t, at, :] = sums[k]
            else:
                nsum_t[t, at, :] = nsum_t[t, at, :] + sums[k]

    def hidden_back(s):
        def tile(i, carry):
            rows = pl.ds(pl.multiple_of(i * TS, TS), TS)
            grad = mm(ag2[s, i], wd[...], NN)
            gate = gb[s, rows, 0:F].astype(F32)
            up = gb[s, rows, F : 2 * F].astype(F32)
            sig = sigmoid(gate)
            act = gate * sig
            gb[s, rows, 0:F] = (grad * up * (sig + act * (1.0 - sig))).astype(BF16)
            gb[s, rows, F : 2 * F] = (grad * act).astype(BF16)
            return carry

        lax.fori_loop(0, NT4, tile, 0)

    def gate_product(s, rows):
        return mm(gb[s, rows, :], wg[...], NT)

    def first_norm_back(s):
        grad = n1[s] + rs_finish(2, s)
        unit = unit1[s]
        sums = (jnp.sum(grad * unit, axis=0, keepdims=True), jnp.sum(grad, axis=0, keepdims=True))
        add_sums(s, 0, sums)
        back = norm_back(grad, unit, inv1[s, :, 0:1], gains[0:1, :])
        n1[s] = back
        ag3[s, t] = back.astype(BF16)
        ag_start(2, ag3, s)

    def weight_grad(dest, left_of, right):
        def tile(i, carry):
            columns = pl.ds(pl.multiple_of(i * 128, 128), 128)
            dest[columns, :] = mm(left_of(columns), right, TN).astype(BF16)
            return carry

        lax.fori_loop(0, D // 128, tile, 0)

    def query_out_grad():
        def tile(i, carry):
            columns = pl.ds(pl.multiple_of(i * 128, 128), 128)
            query = mm(tok[:, :, columns].reshape(R, 128), qb[:, :, 0:QW].reshape(R, QW), TN)
            out = mm(ag3[:, :, :, columns].reshape(R, 128), att[...].reshape(R, 256), TN)
            sources[1][columns, 0:128] = query[:, 0:128].astype(BF16)
            sources[1][columns, 128:256] = (query[:, 128:256] + out[:, 0:128]).astype(BF16)
            sources[1][columns, 256:384] = out[:, 128:256].astype(BF16)
            return carry

        lax.fori_loop(0, D // 128, tile, 0)

    def block_rows(slot, block):
        return half_rows(block, x) if two_level(slot) else own_rows(block)

    def relayed(slot):
        return NF == 4 and slot in RELAYED

    z_near = z + 1 - 2 * (z % 2)
    z_far = (z + 2) % NF

    def reduce_copy(slot, d):
        to = (z + d) % NF
        block = to
        if relayed(slot):
            to = z_far if d == 3 else z_near
            block = (z_near + 2) % NF if d == 1 else to
        return remote(
            sources[slot].at[block_rows(slot, block), :], landings[slot].at[d - 1],
            gr_ss.at[slot, d - 1], gr_rs.at[slot, d - 1], "fsdp", to,
        )

    def reduce_relay(slot):
        if not relayed(slot):
            return
        reduce_copy(slot, 1).wait_recv()
        rows = block_rows(slot, z_far)
        sources[slot][rows, :] = (
            sources[slot][rows, :].astype(F32) + landings[slot][0].astype(F32)
        ).astype(BF16)
        reduce_copy(slot, 3).start()

    def two_level(slot):
        return pair and slot in SUM_HALVES

    def meet_copy(slot, block):
        return remote(
            sources[slot].at[half_rows(block, 1 - x), :], meets[SUM_HALVES.index(slot)].at[block],
            h_ss.at[SUM_HALVES.index(slot), block], h_rs.at[SUM_HALVES.index(slot), block], "context", 1 - x,
        )

    def send_order(slot):
        if relayed(slot):
            return ((z_near + 2) % NF, z_near, z_far, z)
        return [(z + d) % NF for d in range(1, NF + 1)]

    def starts_now(slot, d):
        return d < NF - 1 if relayed(slot) else d < NF

    def reduce_start(slot):
        for d, block in enumerate(send_order(slot), 1):
            if two_level(slot):
                meet_copy(slot, block).start()
            elif starts_now(slot, d):
                reduce_copy(slot, d).start()

    def reduce_meet(slot):
        if not two_level(slot):
            return
        for d, block in enumerate(send_order(slot), 1):
            meet_copy(slot, block).wait_recv()
            rows = half_rows(block, x)
            sources[slot][rows, :] = (
                sources[slot][rows, :].astype(F32)
                + meets[SUM_HALVES.index(slot)][block].astype(F32)
            ).astype(BF16)
            if starts_now(slot, d):
                reduce_copy(slot, d).start()

    def reduce_middle(slot):
        rows = block_rows(slot, z)
        total = sources[slot][rows, :].astype(F32)
        for d in range(2 if relayed(slot) else 1, NF):
            reduce_copy(slot, d).wait_recv()
            total = total + landings[slot][d - 1].astype(F32)
        sources[slot][rows, :] = total.astype(BF16)
        if two_level(slot):
            last_copy(slot).start()
        else:
            for d in range(1, NC):
                cross_copy(slot, d).start()
        own_copy(slot).start()

    def last_copy(slot):
        place = pl.ds(pl.multiple_of(x * HB, HB), HB)
        return remote(
            sources[slot].at[half_rows(z, x), :], own_out[slot].at[place, :],
            l_ss.at[SUM_HALVES.index(slot)], l_rs.at[SUM_HALVES.index(slot)], "context", 1 - x,
        )

    def cross_copy(slot, d):
        return remote(
            sources[slot].at[own_rows(z), :], crosses[slot].at[d - 1],
            x_ss.at[slot, d - 1], x_rs.at[slot, d - 1], "context", (x + d) % NC,
        )

    def own_copy(slot):
        if two_level(slot):
            place = pl.ds(pl.multiple_of(x * HB, HB), HB)
            return pltpu.make_async_copy(
                sources[slot].at[half_rows(z, x), :], own_out[slot].at[place, :],
                own_sem.at[slot],
            )
        return pltpu.make_async_copy(
            sources[slot].at[own_rows(z), :], own_out[slot], own_sem.at[slot]
        )

    def reduce_finish(slot):
        if two_level(slot):
            last_copy(slot).wait()
            for block in range(NF):
                meet_copy(slot, block).wait_send()
        else:
            for d in range(1, NC):
                cross_copy(slot, d).wait()
        own_copy(slot).wait()
        for d in range(1, NF):
            reduce_copy(slot, d).wait_send()

    def moment_copy(k):
        return remote(
            sends[k], lands[k], m_ss.at[k], m_rs.at[k], "context", (x + 1) % NC
        )

    def moment_cast(k):
        for i in range(2):
            moment_load(k, i).wait()
            if k == 2:
                for j in range(2):
                    sends[k][i, :, j * F : (j + 1) * F] = stages[k][i, :, j, :].astype(BF16)
            else:
                sends[k][i] = stages[k][i].astype(BF16)

    def norm_copy(buffer, axis, me, count, base, d):
        return remote(
            buffer.at[me], buffer.at[me], n_ss.at[base + d - 1], n_rs.at[base + d - 1],
            axis, (me + d) % count,
        )

    norm_levels = (
        (nsum_t, "tensor", t, NT4, 0),
        (nsum_c, "context", x, NC, NT4 - 1),
        (nsum_f, "fsdp", z, NF, NT4 - 1 + NC - 1),
    )

    def norm_start(level):
        for d in range(1, norm_levels[level][3]):
            norm_copy(*norm_levels[level], d).start()

    def norm_total(level):
        buffer, count = norm_levels[level][0], norm_levels[level][3]
        for d in range(1, count):
            norm_copy(*norm_levels[level], d).wait_recv()
        total = buffer[0]
        for i in range(1, count):
            total = total + buffer[i]
        return total

    def attended_back(s):
        def tile(i, carry):
            rows = pl.ds(pl.multiple_of(i * TS, TS), TS)
            datt[s, rows, :] = mm(ag3[s, i], wo[...], NN).astype(BF16)
            return carry

        lax.fori_loop(0, NT4, tile, 0)
        both = datt[s].astype(F32) * att[s].astype(F32)
        head_row = lax.broadcasted_iota(jnp.int32, (8, 256), 0)
        lane = lax.broadcasted_iota(jnp.int32, (8, 256), 1)
        chooser = (lane // HD == head_row + 1).astype(F32)
        dlt[s] = lax.dot_general(
            chooser, both, NT, precision=lax.Precision.HIGHEST, preferred_element_type=F32
        )

    def kvg_copy(s, d):
        return remote(
            kvg_s.at[(d - 1) % KS, s], kvg_r.at[d - 1, s],
            kvg_ss.at[d - 1, s], kvg_rs.at[d - 1, s], "context", (x + NC - d) % NC,
        )

    def back_block(s):
        def block(d):
            j = (x + NC - d) % NC
            doc_bias(j, s)
            vt[...] = mm(eye256, kv[j, s, :, 0:256], NT).astype(BF16)
            dk[...] = jnp.zeros(dk.shape, F32)
            dv[...] = jnp.zeros(dv.shape, F32)

            def head(h, inner):
                key_mask, value_mask = head_mask(h, 0), head_mask(h, HD)
                keys = keep(kv[j, s, :, 0:256], key_mask)
                row = pl.ds(h, 1)
                scores = mm(keys, q_ref[s], NT) * scale + bias_ref[...]
                probs = jnp.exp(scores - tot[s, row, :])
                dv[...] += mm(probs.astype(BF16), keep(datt[s], value_mask), NN)
                grad_probs = mm(keep(kv[j, s, :, 128:384], value_mask), datt[s], NT)
                grads = (probs * (grad_probs - dlt[s, row, :])).astype(BF16)
                dk[...] += mm(grads, keep(q_ref[s], key_mask), NN)
                rows = pl.ds(pl.multiple_of(h * HD, HD), HD)
                dqt[s, rows, :] += mm(vt[rows, :], grads, NN)
                return inner

            lax.fori_loop(0, H, head, 0)
            first = dk[:, 0:128] * scale
            second = dk[:, 128:256] * scale + dv[:, 0:128]
            return first, second, dv[:, 128:256]

        return block

    def attend_far(s):
        dqt[s] = jnp.zeros(dqt.shape[1:], F32)
        block = back_block(s)

        def far(d, carry):
            parts = block(d)
            if NC - 1 > KS:

                @pl.when(d > KS)
                def _():
                    kvg_copy(s, d - KS).wait_send()

            for k in range(3):
                kvg_s[(d - 1) % KS, s, :, k * 128 : (k + 1) * 128] = parts[k].astype(BF16)
            kvg_copy(s, d).start()
            return carry

        if NC > 1:
            lax.fori_loop(1, NC, far, 0)

    def attend_near(s):
        parts = back_block(s)(0)
        for k in range(3):
            kv_own[s, :, k * 128 : (k + 1) * 128] = parts[k].astype(BF16)
        grad = jnp.transpose(dqt[s]) * scale
        q0, q1 = rotate_pair(grad, slice(0, T), -1.0)
        qb[s, :, 0:128] = q0.astype(BF16)
        qb[s, :, 128:256] = q1.astype(BF16)

    def keys_back(s):
        for d in range(1, NC):
            kvg_copy(s, d).wait_recv()

        def column(k):
            cols = slice(k * 128, (k + 1) * 128)
            total = kv_own[s, :, cols].astype(F32)
            for d in range(1, NC):
                total = total + kvg_r[d - 1, s, :, cols].astype(F32)
            return total

        k0, k1 = rotate_pair(
            jnp.concatenate([column(0), column(1)], axis=1), slice(0, T), -1.0
        )
        qb[s, :, QW : QW + 128] = k0.astype(BF16)
        qb[s, :, QW + 128 : QW + 256] = k1.astype(BF16)
        qb[s, :, QW + 256 : QW + 384] = column(2).astype(BF16)

    def input_product(s, rows):
        return mm(qb[s, rows, :], wq[...], NT)

    def input_out(s):
        n1[s] = n1[s] + rs_finish(3, s)
        input_copy(s).start()

    def input_copy(s):
        return pltpu.make_async_copy(n1.at[s], input_grad.at[s], loc_sem.at[1 + s])

    seqs = list(range(S))
    R = S * T

    for s in seqs:
        project(s)
    gather_hand(1)
    if adam:
        for k in (2, 0, 3, 1):
            moment_cast(k)
    attend(0)
    gather_finish(1)
    rs_produce(0, 0, out_product)
    for s in range(1, S):
        attend(s)
        rs_middle(0, s - 1)
        rs_produce(0, s, out_product)
        first_norm(s - 1)
    gather_hand(2)
    rs_middle(0, S - 1)
    first_norm(S - 1)
    gather_hand(3)
    for s in seqs:
        ag_middle(0, ag1, s)
    gather_finish(2)
    if adam:
        for k in (2, 0, 3, 1):
            moment_copy(k).start()
    for s in seqs:
        ag_finish(0, ag1, s)
        gate_up(s)
        if s == 0:
            gather_finish(3)
        rs_produce(1, s, down_product)
        if s > 0:
            rs_middle(1, s - 1)
    rs_middle(1, S - 1)
    cot_copy.wait()
    nsum_t[t] = jnp.zeros(nsum_t.shape[1:], F32)
    for s in seqs:
        second_norm(s)
    for s in seqs:
        ag_middle(1, ag2, s)
    for s in seqs:
        ag_finish(1, ag2, s)
        hidden_back(s)
        rs_produce(2, s, gate_product)
        if s > 0:
            rs_middle(2, s - 1)
    weight_grad(
        sources[2], lambda c: ag1[:, :, :, c].reshape(R, 128), gb[:, :, 0:F].reshape(R, F)
    )
    reduce_start(2)
    rs_middle(2, S - 1)
    weight_grad(
        sources[4], lambda c: ag1[:, :, :, c].reshape(R, 128), gb[:, :, F : 2 * F].reshape(R, F)
    )
    reduce_start(4)
    for s in seqs[:-1]:
        first_norm_back(s)
    weight_grad(sources[3], lambda c: ag2[:, :, :, c].reshape(R, 128), hid[...].reshape(R, F))
    reduce_start(3)
    first_norm_back(S - 1)
    norm_start(0)
    reduce_meet(2)
    for s in seqs:
        ag_middle(2, ag3, s)
    for s in seqs:
        ag_finish(2, ag3, s)
        attended_back(s)
        attend_far(s)
        if s == 0:
            nsum_c[x] = norm_total(0)
            norm_start(1)
            reduce_relay(2)
    reduce_meet(4)
    reduce_relay(3)
    for s in seqs:
        attend_near(s)
    nsum_f[z] = norm_total(1)
    norm_start(2)
    query_out_grad()
    reduce_start(1)
    reduce_relay(4)
    for s in seqs:
        keys_back(s)
        if s == S - 1:
            weight_grad(
                sources[0], lambda c: tok[:, :, c].reshape(R, 128),
                qb[:, :, QW : QW + KW].reshape(R, KW),
            )
            reduce_start(0)
        rs_produce(3, s, input_product)
        if s > 0:
            rs_middle(3, s - 1)
        else:
            reduce_relay(1)
    rs_middle(3, S - 1)
    reduce_middle(2)
    norm_out[...] = norm_total(2)
    reduce_middle(3)
    reduce_middle(4)
    for s in seqs:
        input_out(s)
    reduce_middle(1)
    reduce_relay(0)
    reduce_middle(0)
    for slot in (2, 4, 3, 1, 0):
        reduce_finish(slot)

    for s in seqs:
        input_copy(s).wait()
    wait_send(id_copies)
    for slot in range(4):
        for d in range(1, NF):
            fetch_copy(gathered[slot], slot, d).wait_send()
            if halved(slot):
                hand_copy(gathered[slot], slot, d).wait_send()
    for s in seqs:
        for d in range(1, NC):
            kv_copy(s, d).wait_send()
            if d > NC - 1 - KS:
                kvg_copy(s, d).wait_send()
        for part in range(3):
            rs_copy(3, s, part).wait_send()
        for rnd, buffer in ((0, ag1), (1, ag2), (2, ag3)):
            for part in range(3):
                ag_copy(rnd, buffer, s, part).wait_send()
    for level in range(3):
        for d in range(1, norm_levels[level][3]):
            norm_copy(*norm_levels[level], d).wait_send()
    if adam:
        for k in range(4):
            moment_copy(k).wait()


def finish_kernel(dims, *refs):
    S, T, D, C, F, NF, NC, NT4 = dims
    DB = D // NF
    refs = list(refs)

    def take(count):
        taken, refs[:] = refs[:count], refs[count:]
        return taken

    owner, norm_sums, norm_m, norm_v = take(4)
    layer_in, input_in = take(2)
    own_in, cross_in, masters_in, moments_in, lands_in = take(5), take(5), take(4), take(8), take(4)
    layer_out, input_out = take(2)
    grads_out, states_out = take(4), take(4)
    norm_out, norm_state, norm_flat, updates = take(4)
    layer_v, input_v = take(2)
    own_g, cross_g, masters, lands = take(5), take(5), take(4), take(4)
    pair = NC == 2
    states, grads, flats = take(4), take(4), take(4)
    row_a, row_b, in_sem, out_sem, pass_sem = take(5)
    z, x, t = lax.axis_index("fsdp"), lax.axis_index("context"), lax.axis_index("tensor")
    order = (2, 3, 1, 0)

    def loads(k):
        pairs = [
            (masters_in[k], masters[k]), (lands_in[k], lands[k]),
            (moments_in[2 * k].at[0], states[k].at[0]),
            (moments_in[2 * k + 1].at[0], states[k].at[1]),
        ]
        for slot in ((2, 4) if k == 2 else (k,)):
            pairs.append((own_in[slot], own_g[slot]))
            if not (pair and slot in SUM_HALVES):
                pairs.append((cross_in[slot], cross_g[slot]))
        return [
            pltpu.make_async_copy(src, dst, in_sem.at[k, i]) for i, (src, dst) in enumerate(pairs)
        ]

    def passing(k, stage):
        src, mid, dst = ((layer_in, layer_v, layer_out), (input_in, input_v, input_out))[k]
        if stage == 0:
            return pltpu.make_async_copy(src, mid, pass_sem.at[k, 0])
        return pltpu.make_async_copy(mid, dst, pass_sem.at[k, 1])

    for k in order:
        for c in loads(k):
            c.start()
    for k in range(2):
        passing(k, 0).start()

    def adam_parts(g, m, v, w, decay):
        m_new = BETA_ONE * m + (1.0 - BETA_ONE) * g
        v_new = BETA_TWO * v + (1.0 - BETA_TWO) * g * g
        corrected = m_new / (1.0 - BETA_ONE**ADAM_STEP)
        scaled = v_new / (1.0 - BETA_TWO**ADAM_STEP)
        step = corrected / (jnp.sqrt(scaled) + ADAM_EPS)
        if decay:
            step = step + decay * w
        return m_new, v_new, -RATE * step

    def rows_to_flat(flat, count, width):
        block = math.lcm(width, 128)
        period, lines = block // width, block // 128
        many = count // period
        halves = (row_a, row_b)
        for line in range(lines):
            parts, at = [], line * 128
            while at < (line + 1) * 128:
                row, column = divmod(at, width)
                half, lane = divmod(column, 128)
                length = min((line + 1) * 128 - at, width - column, 128 - lane)
                rows = halves[half][pl.ds(row, many, stride=period), :]
                parts.append(rows[:, lane : lane + length])
                at += length
            whole = parts[0] if len(parts) == 1 else jnp.concatenate(parts, axis=1)
            flat[pl.ds(line, many, stride=lines), :] = whole

    def to_rows(values, rows):
        width = values.shape[1]
        for half, place in enumerate((row_a, row_b)):
            part = values[:, half * 128 : min(width, (half + 1) * 128)]
            if part.shape[1] == 0:
                continue
            if part.shape[1] < 128:
                rest = jnp.zeros((part.shape[0], 128 - part.shape[1]), F32)
                part = jnp.concatenate([part, rest], axis=1)
            place[rows, :] = part

    sizes = (DB * 3 * C, C * DB, DB * 2 * F, F * DB)

    def out_copies(k):
        first = sum(sizes[:k])
        return (
            pltpu.make_async_copy(grads[k], grads_out[k], out_sem.at[k, 0]),
            pltpu.make_async_copy(states[k], states_out[k], out_sem.at[k, 1]),
            pltpu.make_async_copy(
                flats[k].reshape(1, sizes[k]),
                updates.at[0, :, pl.ds(first, sizes[k])],
                out_sem.at[k, 2],
            ),
        )

    def summed(slot):
        own = own_g[slot][...].astype(F32)
        if pair:
            return own if slot in SUM_HALVES else own + cross_g[slot][0].astype(F32)
        total = jnp.zeros_like(own)
        for i in range(NC):
            other = cross_g[slot][jnp.maximum((x - i + NC) % NC, 1) - 1].astype(F32)
            total = total + jnp.where(x == i, own, other)
        return total

    for k in order:
        for c in loads(k):
            c.wait()
        total = summed(k)
        if k == 0:
            parts = [summed(1)[:, 0:C], total[:, 0:C], total[:, C : 2 * C]]
        elif k == 1:
            parts = [jnp.transpose(total)[C : 2 * C, :]]
        elif k == 2:
            parts = [total, summed(4)]
        else:
            parts = [total]
        mine = owner[0:1, k : k + 1] == x
        for j, g in enumerate(parts):
            at = (j,) if k == 0 else (slice(None), j) if k == 2 else (slice(None),)
            land_at = (slice(None), slice(j * F, (j + 1) * F)) if k == 2 else at
            grads[k][at] = g
            kept = [
                jnp.where(
                    mine, states[k][(i, *at)].astype(BF16).astype(F32),
                    lands[k][(i, *land_at)].astype(F32),
                )
                for i in range(2)
            ]
            m_new, v_new, step = adam_parts(g, *kept, masters[k][at], DECAY)
            states[k][(0, *at)] = m_new
            states[k][(1, *at)] = v_new
            if k == 0:
                to_rows(step, pl.ds(j, DB, stride=3))
            elif k == 1:
                to_rows(step, pl.ds(0, C))
            elif k == 2:
                for c in range(F // 128):
                    flats[2][pl.ds(j * (F // 128) + c, DB, stride=2 * F // 128), :] = step[
                        :, c * 128 : (c + 1) * 128
                    ]
            else:
                to_rows(jnp.transpose(step), pl.ds(0, F))
        if k != 2:
            rows_to_flat(flats[k], (3 * DB, C, 0, F)[k], (C, DB, 0, DB)[k])
        for c in out_copies(k):
            c.start()
        if k == 2:
            for i in range(2):
                passing(i, 0).wait()
                passing(i, 1).start()

    g = norm_sums[0:4, :]
    m_new, v_new, step = adam_parts(g, norm_m[...], norm_v[...], None, 0.0)
    norm_out[...] = g
    norm_state[0] = m_new
    norm_state[1] = v_new
    count = 4 * D // (NF * NT4)
    per_row = D // count
    place = z * NT4 + t
    row = lax.broadcasted_iota(jnp.int32, (4, count), 0)
    chosen = jnp.zeros((4, count), F32)
    for c in range(per_row):
        hit = row * per_row + c == place
        chosen = chosen + jnp.where(hit, step[:, c * count : (c + 1) * count], 0.0)
    norm_flat[...] = jnp.sum(chosen, axis=0, keepdims=True)
    for k in order:
        for c in out_copies(k):
            c.wait()
    for k in range(2):
        passing(k, 1).wait()


def run_layer(
    tokens, cotangent, segment_ids, owner, weights, norm_gains, norm_biases, moments,
    norm_moments, cosine, sine_rows,
):
    S, T, D = tokens.shape
    C, F = weights[0].shape[2], weights[2].shape[2]
    NF, NC, NT4 = lax.axis_size("fsdp"), lax.axis_size("context"), lax.axis_size("tensor")
    TS, DB, KW, W = T // NT4, D // NF, 384, 640
    adam = NC == 2
    assert NT4 == 4 and C == 192
    vmem = pl.BlockSpec(memory_space=pltpu.VMEM)
    far = pl.BlockSpec(memory_space=pl.ANY)
    VM = pltpu.VMEM
    DMA = pltpu.SemaphoreType.DMA
    NX = max(NC - 1, 1)
    grad_columns = (KW, KW, F, F, F)
    scratch = [
        VM((D, W), BF16), VM((D, 256), BF16), VM((D, 2 * F), BF16), VM((D, F), BF16),
        VM((NC, S, T), jnp.int32), VM((S, T, 256), BF16), VM((NC, S, T, KW), BF16),
        VM((S, T, 256), BF16), VM((S, 8, T), F32), VM((8, T), F32), VM((8, T), F32),
        VM((256, T), F32), VM((T, T), F32), VM((256, T), BF16),
        VM((S, 2, 2, TS, D), BF16), VM((S, 2, TS, D), BF16), VM((S, TS, D), BF16), VM((S, TS, D), BF16),
        VM((S, 4, TS, D), BF16), VM((S, 4, TS, D), BF16), VM((S, 4, TS, D), BF16),
        VM((S, T, F), BF16), VM((S, T, 2 * F), BF16),
        VM((S, TS, D), F32), VM((S, TS, D), F32), VM((S, TS, 128), F32),
        VM((S, T, 256), BF16), VM((S, 8, T), F32), VM((S, 256, T), F32),
        VM((T, 256), F32), VM((T, 256), F32), VM((min(NX, 2), S, T, KW), BF16), VM((NX, S, T, KW), BF16),
        VM((S, T, KW), BF16), VM((S, T, W), BF16),
        *(VM((D, columns), BF16) for columns in grad_columns),
        *(
            VM((NF - 1, DB // 2 if NC == 2 and slot in SUM_HALVES else DB, grad_columns[slot]), BF16)
            for slot in range(5)
        ),
        *(
            VM((NF, DB // 2, grad_columns[slot]) if NC == 2 else (1, 16, 128), BF16)
            for slot in SUM_HALVES
        ),
        VM((NT4, 8, D), F32), VM((NC, 8, D), F32), VM((NF, 8, D), F32), VM((S, TS, D), BF16),
        DMA((4, NF - 1)), DMA((4, NF - 1)), DMA((S, NX)), DMA((S, NX)), DMA((NX,)), DMA((NX,)),
        DMA((4, S, 3)), DMA((4, S, 3)), DMA((3, S, 3)), DMA((3, S, 3)),
        DMA((NX, S)), DMA((NX, S)), DMA((5, NF - 1)), DMA((5, NF - 1)), DMA((5, NX)), DMA((5, NX)),
        DMA((NT4 + NC + NF,)), DMA((NT4 + NC + NF,)), DMA((1 + S,)), DMA((5,)),
        DMA((4, NF - 1)), DMA((4, NF - 1)), DMA((2, NF)), DMA((2, NF)), DMA((2,)), DMA((2,)),
    ]
    shapes = ((3, DB, C), (C, DB), (DB, 2, F), (DB, F))
    flat_shapes = tuple((DB, columns) for columns in grad_columns)
    low_shapes = ((2, 3, DB, C), (2, C, DB), (2, DB, 2 * F), (2, DB, F))
    dims = (S, T, D, C, F, NF, NC, NT4)
    outs = [
        jax.ShapeDtypeStruct((S, TS, D), BF16),
        jax.ShapeDtypeStruct((S, TS, D), F32),
        *(jax.ShapeDtypeStruct(shape, BF16) for shape in flat_shapes),
        *(jax.ShapeDtypeStruct((NX, *shape), BF16) for shape in flat_shapes),
        jax.ShapeDtypeStruct((8, D), F32),
    ]
    out_specs = [vmem] + [far] * 11 + [vmem]
    args = [
        tokens, cotangent, segment_ids, *weights, norm_gains, norm_biases, cosine, sine_rows,
    ]
    in_specs = [vmem, far] + [vmem] * 9
    flat_moments = [m for pair in moments for m in pair]
    if adam:
        outs += [jax.ShapeDtypeStruct(shape, BF16) for shape in low_shapes]
        out_specs += [far] * 4
        args += flat_moments
        in_specs += [far] * 8
        scratch += [VM((2, *shape), F32) for shape in shapes]
        scratch += [VM(shape, BF16) for shape in low_shapes]
        scratch += [DMA((4,)), DMA((4,)), DMA((4, 2))]
    results = pl.pallas_call(
        functools.partial(layer_kernel, dims),
        out_shape=outs,
        in_specs=in_specs,
        out_specs=out_specs,
        scratch_shapes=scratch,
        compiler_params=pltpu.CompilerParams(
            collective_id=0, has_side_effects=True, vmem_limit_bytes=67043328
        ),
        name="layer",
    )(*args)
    layer_out, input_grad = results[:2]
    own_grads, cross_grads, norm_sums = results[2:7], results[7:12], results[12]
    if adam:
        lands = results[13:]
    else:
        lands = []
        for k in range(4):
            pair = jnp.concatenate(moments[k], axis=0).astype(BF16).reshape(low_shapes[k])
            lands.append(from_root(pair, "context", owner[k]))
        owner = jnp.full_like(owner, -1)

    total = sum(math.prod(shape) for shape in shapes)
    count = 4 * D // (NF * NT4)
    out_shape = [
        jax.ShapeDtypeStruct((S, TS, D), BF16),
        jax.ShapeDtypeStruct((S, TS, D), F32),
        *(jax.ShapeDtypeStruct(shape, F32) for shape in shapes),
        *(jax.ShapeDtypeStruct((2, *shape), F32) for shape in shapes),
        jax.ShapeDtypeStruct((4, D), F32),
        jax.ShapeDtypeStruct((2, 4, D), F32),
        jax.ShapeDtypeStruct((1, count), F32),
        jax.ShapeDtypeStruct((1, 1, total + count), F32),
    ]
    rows = max(3 * DB, F)
    return pl.pallas_call(
        functools.partial(finish_kernel, dims),
        out_shape=out_shape,
        in_specs=[vmem] * 4 + [far] * 28,
        out_specs=[far] * 10 + [vmem] * 3 + [far],
        scratch_shapes=[
            VM((S, TS, D), BF16), VM((S, TS, D), F32),
            *(VM(shape, BF16) for shape in flat_shapes),
            *(VM((NX, *shape), BF16) for shape in flat_shapes),
            *(VM(shape, F32) for shape in shapes),
            *(VM(shape, BF16) for shape in low_shapes),
            *(VM((2, *shape), F32) for shape in shapes),
            *(VM(shape, F32) for shape in shapes),
            *(VM((math.prod(shape) // 128, 128), F32) for shape in shapes),
            VM((rows, 128), F32), VM((rows, 128), F32),
            DMA((4, 8)), DMA((4, 3)), DMA((2, 2)),
        ],
        compiler_params=pltpu.CompilerParams(vmem_limit_bytes=67043328),
        name="finish",
    )(
        owner.reshape(1, 4), norm_sums, *norm_moments, layer_out, input_grad, *own_grads,
        *cross_grads, *weights, *flat_moments, *lands,
    )


def from_root(block, axis, owner):
    block = jnp.where(lax.axis_index(axis) == owner, block, jnp.zeros_like(block))
    return lax.psum(block, axis)


def shards(
    tokens, cotangent, segment_ids, owner, qkv_weight, out_weight, gate_up_weight, down_weight,
    norm_gains, norm_biases, qkv_moment, qkv_square, out_moment, out_square, gate_moment,
    gate_square, down_moment, down_square, norm_moment, norm_square,
):
    tok_here = tokens.shape[1]
    moments = (
        (qkv_moment, qkv_square), (out_moment, out_square),
        (gate_moment, gate_square), (down_moment, down_square),
    )
    positions = (
        lax.axis_index("context") * tok_here + jnp.arange(tok_here, dtype=jnp.int32)
    ).astype(F32)
    frequency = jnp.power(F32(ROPE_BASE), -jnp.arange(0, HD, 2, dtype=F32) / HD)
    angles = positions[:, None] * frequency[None, :]
    cosine, sine_rows = jnp.cos(angles), jnp.sin(angles)
    cosine = jnp.concatenate([cosine] * 4, axis=1)
    sine_rows = jnp.concatenate([-sine_rows, sine_rows] * 2, axis=1)

    columns_last = (0, 2, 1, 3)
    weights = (
        jnp.transpose(qkv_weight, (1, 0, 2)), out_weight, gate_up_weight, jnp.transpose(down_weight),
    )
    turned = (
        [jnp.transpose(m, columns_last) for m in moments[0]],
        moments[1],
        moments[2],
        [jnp.transpose(m, (0, 2, 1)) for m in moments[3]],
    )
    results = run_layer(
        tokens, cotangent, segment_ids, owner, weights, norm_gains, norm_biases, turned,
        (norm_moment, norm_square), cosine, sine_rows,
    )
    layer_out, input_grad, grad_q, grad_o, grad_g, grad_d = results[:6]
    state_q, state_o, state_g, state_d = results[6:10]
    norm_grad, norm_state, piece, weight_updates = results[10:]
    weight_updates = lax.dynamic_update_slice(
        weight_updates, piece[None], (0, 0, weight_updates.shape[2] - piece.shape[1])
    )
    return (
        layer_out, input_grad,
        jnp.transpose(grad_q, (1, 0, 2)), grad_o, grad_g, jnp.transpose(grad_d),
        norm_grad,
        jnp.transpose(state_q, columns_last), state_o, state_g, jnp.transpose(state_d, (0, 2, 1)),
        norm_state, weight_updates,
    )


def solution(mesh):
    return jax.shard_map(
        shards,
        mesh=mesh,
        in_specs=(
            P("fsdp", "context", None),
            P("fsdp", "context", None),
            P("fsdp", "context"),
            P(),
            P("fsdp", None, "tensor"),
            P("tensor", "fsdp"),
            P("fsdp", None, "tensor"),
            P("tensor", "fsdp"),
            P(),
            P(),
            P("context", "fsdp", None, "tensor"),
            P("context", "fsdp", None, "tensor"),
            P("context", "tensor", "fsdp"),
            P("context", "tensor", "fsdp"),
            P("context", "fsdp", None, "tensor"),
            P("context", "fsdp", None, "tensor"),
            P("context", "tensor", "fsdp"),
            P("context", "tensor", "fsdp"),
            P(),
            P(),
        ),
        out_specs=(
            P("fsdp", ("context", "tensor"), None),
            P("fsdp", ("context", "tensor"), None),
            P("fsdp", None, "tensor"),
            P("tensor", "fsdp"),
            P("fsdp", None, "tensor"),
            P("tensor", "fsdp"),
            P(),
            P(None, "fsdp", None, "tensor"),
            P(None, "tensor", "fsdp"),
            P(None, "fsdp", None, "tensor"),
            P(None, "tensor", "fsdp"),
            P(),
            P("fsdp", "tensor", None),
        ),
        check_vma=False,
    )
```
